8 devices in a mesh: graphs: 2 (over z, y), nodes: 4 (over x, core).
Axes of the slice: x: 2, y: 2, z: 1, core: 2. Of those that a mesh axis runs over, the one named last changes fastest.
Arguments:
- x_feat: bfloat16 [8192, 512], P(('graphs', 'nodes')), parts along dimension 0
- valid: int32 [8192], P(('graphs', 'nodes')), parts along dimension 0
- halo_slot: int32 [8, 4, 32], P(('graphs', 'nodes')), parts along dimension 0
- edge_src: int32 [8, 14336], P(('graphs', 'nodes')), parts along dimension 0
- edge_dst: int32 [8, 14336], P(('graphs', 'nodes')), parts along dimension 0
- edge_mask: int32 [8, 14336], P(('graphs', 'nodes')), parts along dimension 0
- bal_perm: int32 [8192], P(('graphs', 'nodes')), parts along dimension 0
- pos_enc: bfloat16 [8192, 512], P(('graphs', 'nodes')), parts along dimension 0
- y_cot: bfloat16 [8192, 512], P(('graphs', 'nodes')), parts along dimension 0
- w_msg: bfloat16 [512, 512], replicated
- w_self: bfloat16 [512, 512], replicated
- w_q: bfloat16 [512, 512], replicated
- w_k: bfloat16 [512, 64], replicated
- w_v: bfloat16 [512, 64], replicated
- w_o: bfloat16 [512, 512], replicated
- w_up: bfloat16 [512, 2048], replicated
- w_down: bfloat16 [2048, 512], replicated
Outputs:
- output 1: bfloat16 [8192, 512], P(('graphs', 'nodes')), parts along dimension 0
- output 2: bfloat16 [8192, 512], P(('graphs', 'nodes')), parts along dimension 0
- output 3: float32 [1024, 512], P('graphs'), parts along dimension 0
- output 4: float32 [1024, 512], P('graphs'), parts along dimension 0
- output 5: float32 [1024, 512], P('graphs'), parts along dimension 0
- output 6: float32 [1024, 64], P('graphs'), parts along dimension 0
- output 7: float32 [1024, 64], P('graphs'), parts along dimension 0
- output 8: float32 [1024, 512], P('graphs'), parts along dimension 0
- output 9: float32 [1024, 2048], P('graphs'), parts along dimension 0
- output 10: float32 [4096, 512], P('graphs'), parts along dimension 0
There are 2 independent parts. The reference program is written for one: setup_inputs(seed, part) draws one part's arguments, and reference() takes and returns one part's arrays. A program takes and returns all parts, laid end to end along the dimension named above; an argument that names none is the same for every part.
All inputs are finite; a program needn't handle non-finite values.
Results may differ from the reference program's by a relative error of at most 0.02.
Values are sent between devices in bfloat16 or wider.
A program may use at most 1 GiB of HBM per device.

```python
import math
import functools
import jax
import jax.numpy as jnp
from jax import lax

NODES = 4
ROWS_DEV = 1024
HALO_PAIR = 32
DEG = 14
D = 512
HEADS = 8

HEAD = D // HEADS
HALO = NODES * HALO_PAIR
EDGES = DEG * ROWS_DEV
TOTAL = NODES * ROWS_DEV
QUERY_BLOCK = math.gcd(TOTAL * HEADS, 2 ** max(3, 22 - int(math.log2(TOTAL))))


def draw_perm(key_off, key_rows, key_pos):
    base_count = ROWS_DEV // NODES
    shift_count = base_count // 2
    key_plus, key_gap = jax.random.split(key_off)
    plus_off = jax.random.randint(key_plus, (), 0, NODES)
    minus_off = (plus_off + 1 + jax.random.randint(key_gap, (), 0, NODES - 1)) % NODES
    diagonal = (jnp.arange(NODES)[None, :] - jnp.arange(NODES)[:, None]) % NODES
    counts = base_count + shift_count * (diagonal == plus_off).astype(jnp.int32) - shift_count * (diagonal == minus_off).astype(jnp.int32)
    row_start = jnp.cumsum(counts, axis=1) - counts
    col_end = jnp.cumsum(counts, axis=0)
    col_start = col_end - counts
    row_order = jax.vmap(lambda k: jax.random.permutation(k, ROWS_DEV))(jax.random.split(key_rows, NODES))
    place_ix = jnp.arange(ROWS_DEV)
    owner_ix = jax.vmap(lambda ends: jnp.searchsorted(ends, place_ix, side='right'))(col_end.T)
    dest_ix = jnp.arange(NODES)[:, None]
    offset = place_ix[None, :] - col_start[owner_ix, dest_ix]
    slot_ix = row_order[owner_ix, row_start[owner_ix, dest_ix] + offset]
    global_ix = owner_ix * ROWS_DEV + slot_ix
    shuffle = jax.vmap(lambda k: jax.random.permutation(k, ROWS_DEV))(jax.random.split(key_pos, NODES))
    return jnp.take_along_axis(global_ix, shuffle, axis=1).reshape(TOTAL).astype(jnp.int32)


def draw_layout(key):
    subkeys = jax.random.split(key, 11)
    drop = jax.random.randint(subkeys[0], (NODES,), 0, ROWS_DEV // 32 + 1)
    full_dev = jax.random.randint(subkeys[1], (), 0, NODES)
    n_valid = ROWS_DEV - jnp.where(jnp.arange(NODES) == full_dev, 0, drop)
    valid = (jnp.arange(ROWS_DEV)[None, :] < n_valid[:, None]).astype(jnp.int32).reshape(TOTAL)
    halo_slot = jax.random.randint(subkeys[2], (NODES, NODES, HALO_PAIR), 0, n_valid[None, :, None]).astype(jnp.int32)
    local_src = jax.random.randint(subkeys[3], (NODES, EDGES), 0, n_valid[:, None])
    remote_src = ROWS_DEV + jax.random.randint(subkeys[4], (NODES, EDGES), 0, HALO)
    crosses = jax.random.randint(subkeys[5], (NODES, EDGES), 0, 4) == 0
    edge_src = jnp.where(crosses, remote_src, local_src).astype(jnp.int32)
    edge_dst = jax.random.randint(subkeys[6], (NODES, EDGES), 0, n_valid[:, None]).astype(jnp.int32)
    edge_mask = (jax.random.randint(subkeys[7], (NODES, EDGES), 0, 10) < 9).astype(jnp.int32)
    bal_perm = draw_perm(subkeys[8], subkeys[9], subkeys[10])
    return valid, halo_slot, edge_src, edge_dst, edge_mask, bal_perm


def draw_weight(key, fan_in, fan_out, gain):
    return (jax.random.normal(key, (fan_in, fan_out), jnp.float32) * (gain / math.sqrt(fan_in))).astype(jnp.bfloat16)


def setup_inputs(seed: int = 0, part: int = 0) -> dict:
    root = jax.random.key(seed)
    part_key = jax.random.fold_in(root, part)
    valid, halo_slot, edge_src, edge_dst, edge_mask, bal_perm = draw_layout(jax.random.fold_in(part_key, 1))
    feat_keys = jax.random.split(jax.random.fold_in(part_key, 2), 3)
    weight_keys = jax.random.split(jax.random.fold_in(root, 3), 8)
    score_gain = math.sqrt(0.75 * math.log(TOTAL))
    out_gain = TOTAL ** 0.125
    msg_gain = (0.9 * DEG) ** -0.5
    return {
        'x_feat': jax.random.normal(feat_keys[0], (TOTAL, D), jnp.float32).astype(jnp.bfloat16),
        'valid': valid,
        'halo_slot': halo_slot,
        'edge_src': edge_src,
        'edge_dst': edge_dst,
        'edge_mask': edge_mask,
        'bal_perm': bal_perm,
        'pos_enc': jax.random.normal(feat_keys[1], (TOTAL, D), jnp.float32).astype(jnp.bfloat16),
        'y_cot': jax.random.normal(feat_keys[2], (TOTAL, D), jnp.float32).astype(jnp.bfloat16),
        'w_msg': draw_weight(weight_keys[0], D, D, msg_gain),
        'w_self': draw_weight(weight_keys[1], D, D, 1.0),
        'w_q': draw_weight(weight_keys[2], D, D, score_gain),
        'w_k': draw_weight(weight_keys[3], D, HEAD, 1.0),
        'w_v': draw_weight(weight_keys[4], D, HEAD, 1.0),
        'w_o': draw_weight(weight_keys[5], D, D, out_gain),
        'w_up': draw_weight(weight_keys[6], D, 4 * D, 1.0),
        'w_down': draw_weight(weight_keys[7], 4 * D, D, 1.0),
    }


def to_bf16(a):
    return a.astype(jnp.bfloat16).astype(jnp.float32)


def aggregate(operands):
    table, edge_src, edge_dst, edge_on = operands
    messages = table[edge_src] * edge_on[:, None].astype(jnp.float32)
    return jax.ops.segment_sum(messages, edge_dst, num_segments=ROWS_DEV)


def attend(q_block, keys, values, key_ok):
    scores = jnp.dot(q_block, keys.T, preferred_element_type=jnp.float32) * (HEAD ** -0.5)
    scores = jnp.where(key_ok[None, :], scores, -jnp.inf)
    return jnp.dot(jax.nn.softmax(scores, axis=-1), values, preferred_element_type=jnp.float32)


def layer(x_in, weights, valid, halo_slot, edge_src, edge_dst, edge_mask, bal_perm, pos_enc):
    w_msg, w_self, w_q, w_k, w_v, w_o, w_up, w_down = weights
    owner_base = jnp.arange(NODES)[None, :, None] * ROWS_DEV
    halo_feat = x_in[(halo_slot + owner_base).reshape(NODES, HALO)]
    table = jnp.concatenate([x_in.reshape(NODES, ROWS_DEV, D), halo_feat], axis=1)
    agg_msg = to_bf16(lax.map(aggregate, (table, edge_src, edge_dst, edge_mask)).reshape(TOTAL, D))
    pre_act = jnp.dot(agg_msg, w_msg, preferred_element_type=jnp.float32) + jnp.dot(x_in, w_self, preferred_element_type=jnp.float32)
    hidden_in = to_bf16(x_in[bal_perm] + pos_enc.astype(jnp.float32))
    queries = to_bf16(jnp.dot(hidden_in, w_q, preferred_element_type=jnp.float32)).reshape(TOTAL * HEADS // QUERY_BLOCK, QUERY_BLOCK, HEAD)
    keys = to_bf16(jnp.dot(hidden_in, w_k, preferred_element_type=jnp.float32))
    values = to_bf16(jnp.dot(hidden_in, w_v, preferred_element_type=jnp.float32))
    attend_rows = jax.checkpoint(functools.partial(attend, keys=keys, values=values, key_ok=valid[bal_perm] > 0))
    mixed = to_bf16(lax.map(attend_rows, queries).reshape(TOTAL, D))
    u_bal = to_bf16(jnp.dot(mixed, w_o, preferred_element_type=jnp.float32))
    u_part = jnp.zeros((TOTAL, D), jnp.float32).at[bal_perm].set(u_bal)
    z_mid = to_bf16(x_in + jax.nn.relu(pre_act) + x_in + u_part)
    hidden = to_bf16(jax.nn.gelu(jnp.dot(z_mid, w_up, preferred_element_type=jnp.float32)))
    return jnp.where(valid[:, None] > 0, z_mid + jnp.dot(hidden, w_down, preferred_element_type=jnp.float32), 0.0)


def reference(x_feat, valid, halo_slot, edge_src, edge_dst, edge_mask, bal_perm, pos_enc, y_cot, w_msg, w_self, w_q, w_k, w_v, w_o, w_up, w_down):
    weights = tuple(w.astype(jnp.float32) for w in (w_msg, w_self, w_q, w_k, w_v, w_o, w_up, w_down))
    forward = functools.partial(layer, valid=valid, halo_slot=halo_slot, edge_src=edge_src, edge_dst=edge_dst, edge_mask=edge_mask, bal_perm=bal_perm, pos_enc=pos_enc)
    y_out, pullback = jax.vjp(forward, x_feat.astype(jnp.float32), weights)
    dx_feat, grads = pullback(y_cot.astype(jnp.float32))
    grad_msg, grad_self, grad_q, grad_k, grad_v, grad_o, grad_up, grad_down = grads
    return (y_out.astype(jnp.bfloat16), dx_feat.astype(jnp.bfloat16), grad_msg, grad_self, grad_q, grad_k, grad_v, grad_o, grad_up, grad_down)
```

```python
import functools
import math

import jax
import jax.numpy as jnp
from jax import lax
from jax.experimental import pallas as pl
from jax.experimental.pallas import tpu as pltpu
from jax.sharding import PartitionSpec as P

NEG_FILL = -1e30
LOG2E = math.log2(math.e)
TAIL = 32
F32 = jnp.float32
BF16 = jnp.bfloat16
NN = (((1,), (0,)), ((), ()))
NT = (((1,), (1,)), ((), ()))
TN = (((0,), (0,)), ((), ()))
TT = (((0,), (1,)), ((), ()))


def dot(a, b, dims=NN):
    return lax.dot_general(a, b, dims, preferred_element_type=F32)


def adjacency_kernel(rows_dev, chunks, steps, width, src_ref, dst_ref, on_ref, out_ref, acc):
    half = rows_dev // 2
    table_rows = out_ref.shape[0]

    def step_block(index):
        cols = pl.ds(pl.multiple_of(index * width, width), width)
        src, dst, on = src_ref[:, cols], dst_ref[:, cols], on_ref[:, cols]
        upper = dst >= half
        place = jnp.where(upper, dst - half, dst)
        weight = jnp.where(on > 0, jnp.where(upper, 4096.0, 1.0), 0.0)
        src_hot = jnp.where(lax.broadcasted_iota(jnp.int32, (table_rows, width), 0) == src, 1.0, 0.0).astype(BF16)
        dst_hot = jnp.where(lax.broadcasted_iota(jnp.int32, (half, width), 0) == place, weight, 0.0).astype(BF16)
        return dot(src_hot, dst_hot, NT)

    for chunk in range(chunks):
        acc[...] = step_block(chunk * steps)

        def body(step, carry, chunk=chunk):
            acc[...] += step_block(chunk * steps + step)
            return carry

        lax.fori_loop(1, steps, body, 0)
        total = acc[...]
        high = jnp.floor(total * (1.0 / 4096.0))
        low = total - high * 4096.0
        if chunk == 0:
            out_ref[:, :half] = low
            out_ref[:, half:] = high
        else:
            out_ref[:, :half] += low
            out_ref[:, half:] += high


def build_adjacency(edge_src, edge_dst, edge_mask, rows_dev, table_rows):
    edges = edge_src.shape[1]
    width = 512
    chunks = 4
    steps = edges // (chunks * width)
    assert chunks * steps * width == edges and steps * width < 4096
    return pl.pallas_call(
        functools.partial(adjacency_kernel, rows_dev, chunks, steps, width),
        out_shape=jax.ShapeDtypeStruct((table_rows, rows_dev), F32),
        in_specs=[pl.BlockSpec(memory_space=pltpu.VMEM)] * 3,
        out_specs=pl.BlockSpec(memory_space=pltpu.VMEM),
        scratch_shapes=[pltpu.VMEM((table_rows, rows_dev // 2), F32)],
        compiler_params=pltpu.CompilerParams(vmem_limit_bytes=40 << 20),
        cost_estimate=pl.CostEstimate(flops=edges * table_rows * rows_dev, bytes_accessed=6 << 20, transcendentals=0),
        name='adjacency',
    )(edge_src, edge_dst, edge_mask)


def mask_tail(scores, chunk, key_chunk, part_rows, count_ref):
    start = chunk * key_chunk
    part = start // part_rows
    first = start - part * part_rows + key_chunk - TAIL
    row_ix = first + lax.broadcasted_iota(jnp.int32, (TAIL, scores.shape[1]), 0)
    tail = jnp.where(row_ix < count_ref[part], scores[key_chunk - TAIL:, :], NEG_FILL)
    return jnp.concatenate([scores[:key_chunk - TAIL, :], tail], axis=0)


def attention_fwd_kernel(head_dim, q_block, key_chunk, part_rows, count_ref, q_ref, kv_ref, kvt_ref, out_ref, lse_ref, w_q, s_buf, stat):
    heads = q_ref.shape[0] // head_dim
    blocks = q_ref.shape[1] // q_block
    units = heads * blocks
    keys = kv_ref.shape[0]
    chunks = keys // key_chunk
    factor = head_dim ** -0.5 * LOG2E
    groups = key_chunk // 8

    def load_weights(unit):
        head, block = unit // blocks, lax.rem(unit, blocks)
        w_q[:head_dim, :] = q_ref[pl.ds(pl.multiple_of(head * head_dim, head_dim), head_dim), pl.ds(pl.multiple_of(block * q_block, q_block), q_block)]

    def score_stage(slot, chunk, run_max):
        rows = pl.ds(pl.multiple_of(chunk * key_chunk, key_chunk), key_chunk)
        scores = mask_tail(dot(kv_ref[rows, :], w_q[...]), chunk, key_chunk, part_rows, count_ref)
        s_buf[slot, rows, :] = scores
        return jnp.maximum(run_max, jnp.max(scores.reshape(groups, 8, q_block), axis=0))

    w_q[head_dim:, :] = jnp.zeros((w_q.shape[0] - head_dim, q_block), BF16)
    floor = jnp.full((8, q_block), -jnp.inf, F32)
    load_weights(0)
    stat[...] = lax.fori_loop(0, chunks, lambda chunk, run_max: score_stage(0, chunk, run_max), floor)

    def unit_body(unit, carry):
        slot = lax.rem(unit, 2)
        load_weights(jnp.minimum(unit + 1, units - 1))
        top = jnp.max(stat[...], axis=0, keepdims=True) * factor

        def chunk_body(chunk, state):
            run_max, run_sum, weighted = state
            cols = pl.ds(pl.multiple_of(chunk * key_chunk, key_chunk), key_chunk)
            prob = jnp.exp2(s_buf[slot, cols, :] * factor - top)
            run_sum = run_sum + jnp.sum(prob.reshape(groups, 8, q_block), axis=0)
            weighted = weighted + dot(kvt_ref[head_dim:2 * head_dim, cols], prob.astype(BF16))
            return score_stage(1 - slot, chunk, run_max), run_sum, weighted

        run_max, run_sum, weighted = lax.fori_loop(0, chunks, chunk_body, (floor, jnp.zeros((8, q_block), F32), jnp.zeros((head_dim, q_block), F32)))
        stat[...] = run_max
        total = jnp.sum(run_sum, axis=0, keepdims=True)
        head, block = unit // blocks, lax.rem(unit, blocks)
        cols = pl.ds(pl.multiple_of(block * q_block, q_block), q_block)
        out_ref[pl.ds(pl.multiple_of(head * head_dim, head_dim), head_dim), cols] = (weighted / total).astype(BF16)
        lse_ref[pl.ds(head, 1), cols] = top + jnp.log2(total)
        return carry

    lax.fori_loop(0, units, unit_body, 0)


def attention_forward(counts, q_t, kv, kv_t, head_dim, part_rows):
    width, rows = q_t.shape
    keys = kv.shape[0]
    heads = width // head_dim
    q_block, key_chunk = 256, 1024
    vmem = pl.BlockSpec(memory_space=pltpu.VMEM)
    return pl.pallas_call(
        functools.partial(attention_fwd_kernel, head_dim, q_block, key_chunk, part_rows),
        out_shape=[jax.ShapeDtypeStruct((width, rows), BF16), jax.ShapeDtypeStruct((heads, rows), F32)],
        in_specs=[pl.BlockSpec(memory_space=pltpu.SMEM), vmem, vmem, vmem],
        out_specs=[vmem, vmem],
        scratch_shapes=[pltpu.VMEM((2 * head_dim, q_block), BF16), pltpu.VMEM((2, keys, q_block), F32), pltpu.VMEM((8, q_block), F32)],
        compiler_params=pltpu.CompilerParams(vmem_limit_bytes=48 << 20),
        cost_estimate=pl.CostEstimate(flops=4 * heads * rows * keys * head_dim, bytes_accessed=4 << 20, transcendentals=heads * rows * keys),
        name='attention_fwd',
    )(counts, q_t, kv, kv_t)


def backward_kernel(head_dim, q_block, key_chunk, part_rows, pieces, count_ref, q_ref, do_ref, o_ref, lse_ref, kv_ref, kvt_ref, *rest):
    grads = len(pieces)
    grad_refs, rest = rest[:grads], rest[grads:]
    (dq_ref, dkv_ref), rest = rest[:2], rest[2:]
    sum_refs, rest = rest[:grads], rest[grads:]
    w_q, w_do, lse_buf, delta_buf, p_buf, ds_buf, dq_acc, dkv_acc, dkv_in, dkv_sum, own, from_mate, from_cross, own_sem, send_sem, recv_sem, dkv_send, dkv_recv = rest
    heads = q_ref.shape[0] // head_dim
    blocks = q_ref.shape[1] // q_block
    units = heads * blocks
    chunks = kv_ref.shape[0] // key_chunk
    steps = units * chunks
    per_group = steps // 4
    halves = part_rows // key_chunk
    scale = head_dim ** -0.5
    factor = scale * LOG2E
    total = own.shape[0]

    me = lax.axis_index('nodes')
    chip, side = me // 2, lax.rem(me, 2)
    mate = chip * 2 + 1 - side
    cross = (1 - chip) * 2 + side

    spots = [(array, j) for array in range(grads) for j in range(pieces[array])]

    def block(refs, spot, half):
        array, j = spot
        rows, cols = own.shape[1:]
        ref = refs[array]
        if ref.shape[1] > cols:
            return ref.at[pl.ds(half * rows, rows), pl.ds(j * cols, cols)]
        return ref.at[pl.ds((half * pieces[array] + j) * rows, rows), :]

    def to_peer(src, dst, kind, index, peer):
        return pltpu.make_async_remote_copy(src_ref=src, dst_ref=dst, send_sem=send_sem.at[kind, index], recv_sem=recv_sem.at[kind, index], device_id={'nodes': peer}, device_id_type=pl.DeviceIdType.MESH)

    def mate_copy(index):
        return to_peer(block(grad_refs, spots[index], 1 - side), from_mate.at[index], 0, index, mate)

    def own_copy(index):
        return pltpu.make_async_copy(block(grad_refs, spots[index], side), own.at[index], own_sem.at[0, index])

    def cross_copy(index):
        return to_peer(own.at[index], from_cross.at[index], 1, index, cross)

    def back_copy(index):
        return to_peer(from_mate.at[index], block(sum_refs, spots[index], side), 2, index, mate)

    def keep_copy(index):
        return pltpu.make_async_copy(from_mate.at[index], block(sum_refs, spots[index], side), own_sem.at[1, index])

    def chip_sum(index):
        to_peer(own.at[index], from_mate.at[index], 0, index, mate).wait_recv()
        pltpu.make_async_copy(own.at[index], own.at[index], own_sem.at[0, index]).wait()
        own[index] = own[index] + from_mate[index]

    def group_sum(index):
        cross_copy(index).wait_recv()
        from_mate[index] = own[index] + from_cross[index]

    def start_out(index):
        for k in range(total):
            @pl.when(index == k)
            def start_piece(k=k):
                keep_copy(k).start()
                back_copy(k).start()

    def dkv_copy(src, slot, peer):
        return pltpu.make_async_remote_copy(src_ref=src, dst_ref=dkv_in.at[slot], send_sem=dkv_send.at[slot], recv_sem=dkv_recv.at[slot], device_id={'nodes': peer}, device_id_type=pl.DeviceIdType.MESH)

    dkv_copies = [dkv_copy(dkv_acc.at[0], 0, mate), dkv_copy(dkv_sum, 1, cross), dkv_copy(dkv_acc.at[2], 2, mate)]

    barrier = pltpu.get_barrier_semaphore()
    for peer in (mate, cross):
        pl.semaphore_signal(barrier, inc=1, device_id={'nodes': peer}, device_id_type=pl.DeviceIdType.MESH)
    pl.semaphore_wait(barrier, 2)
    for index in range(total):
        mate_copy(index).start()
        own_copy(index).start()

    def unit_spots(unit):
        head, place = unit // blocks, lax.rem(unit, blocks)
        return head, pl.ds(pl.multiple_of(head * head_dim, head_dim), head_dim), pl.ds(pl.multiple_of(place * q_block, q_block), q_block)

    def prepare(unit, carry):
        head, rows, cols = unit_spots(unit)
        delta_buf[unit] = jnp.sum(do_ref[rows, cols].astype(F32) * o_ref[rows, cols].astype(F32), axis=0, keepdims=True)
        lse_buf[unit] = lse_ref[pl.ds(head, 1), cols]
        dq_acc[unit] = jnp.zeros((head_dim, q_block), F32)
        return carry

    lax.fori_loop(0, units, prepare, 0)
    for slot in range(2):
        w_q[slot, head_dim:, :] = jnp.zeros((head_dim, q_block), BF16)
        w_do[slot, :head_dim, :] = jnp.zeros((head_dim, q_block), BF16)
    dkv_acc[...] = jnp.zeros_like(dkv_acc)

    def place_of(step):
        group = step // per_group
        chunk = step // units
        owner = lax.rem(chip + 1 - group // 2, 2) * 2 + lax.rem(side + 1 - lax.rem(group, 2), 2)
        offset = lax.rem(chunk, halves) * key_chunk
        rows = pl.ds(pl.multiple_of(owner * part_rows + offset, key_chunk), key_chunk)
        return group, owner, offset, rows, lax.rem(step, units), lax.rem(step, 2)

    def first_stage(step):
        group, owner, offset, rows, unit, slot = place_of(step)
        head, unit_rows, cols = unit_spots(unit)
        w_q[slot, :head_dim, :] = q_ref[unit_rows, cols]
        w_do[slot, head_dim:, :] = do_ref[unit_rows, cols]
        kv = kv_ref[rows, :]
        scores = dot(kv, w_q[slot])
        row_ix = offset + key_chunk - TAIL + lax.broadcasted_iota(jnp.int32, (TAIL, q_block), 0)
        tail = jnp.where(row_ix < count_ref[owner], scores[key_chunk - TAIL:, :], NEG_FILL)
        scores = jnp.concatenate([scores[:key_chunk - TAIL, :], tail], axis=0)
        prob = jnp.exp2(scores * factor - lse_buf[unit])
        p_buf[slot] = prob.astype(BF16)
        ds_buf[slot] = (prob * (dot(kv, w_do[slot]) - delta_buf[unit])).astype(BF16)

    def second_stage(step):
        group, owner, offset, rows, unit, slot = place_of(step)
        d_scores = ds_buf[slot]
        spot = pl.ds(pl.multiple_of(offset, key_chunk), key_chunk)
        dkv_acc[group, spot, :] += dot(d_scores, w_q[slot], NT) + dot(p_buf[slot], w_do[slot], NT)
        dq_acc[unit] += dot(kvt_ref[:head_dim, rows], d_scores)

    def exchange(step):
        turn, phase = step // 4, lax.rem(step, 4)

        @pl.when(jnp.logical_and(turn < total, phase == 1))
        def sum_chip():
            chip_sum(turn)

        @pl.when(jnp.logical_and(turn < total, phase == 2))
        def send_cross():
            cross_copy(turn).start()

        lap, beat = step // FINAL_STEPS - FINAL_LAG, lax.rem(step, FINAL_STEPS)

        @pl.when(jnp.logical_and(lap >= 0, beat == 0))
        def sum_group():
            group_sum(lap)

        @pl.when(jnp.logical_and(lap >= 0, beat == 1))
        def send_back():
            start_out(lap)

        @pl.when(step == per_group + 1)
        def first_group():
            dkv_copies[0].start()

        @pl.when(step == 2 * per_group + 1)
        def second_group():
            dkv_copies[0].wait_recv()
            dkv_sum[...] = dkv_acc[1] + dkv_in[0]

        @pl.when(step == 2 * per_group + 2)
        def send_second():
            dkv_copies[1].start()

        @pl.when(step == 3 * per_group + 1)
        def third_group():
            dkv_copies[2].start()

    first_stage(0)

    def body(step, carry):
        exchange(step)
        second_stage(step - 1)
        first_stage(step)
        return carry

    lax.fori_loop(1, steps, body, 0)
    second_stage(steps - 1)
    done = (steps - 1) // FINAL_STEPS - FINAL_LAG + 1
    assert (steps - 1) % FINAL_STEPS >= 1 and 0 < done <= total

    def finish(unit, carry):
        head, rows, cols = unit_spots(unit)
        dq_ref[rows, cols] = (dq_acc[unit] * scale).astype(BF16)
        return carry

    lax.fori_loop(0, units, finish, 0)
    for index in range(done, total):
        group_sum(index)
        if index > done:
            start_out(index - 1)
    dkv_copies[2].wait_recv()
    dkv_copies[1].wait_recv()
    dkv_ref[...] = dkv_acc[3] + dkv_in[2] + dkv_in[1]
    start_out(total - 1)
    for copy in dkv_copies:
        copy.wait_send()
    for index in range(total):
        mate_copy(index).wait_send()
        cross_copy(index).wait_send()
        keep_copy(index).wait()
        back_copy(index).wait_send()
        to_peer(from_mate.at[index], block(sum_refs, spots[index], 1 - side), 2, index, mate).wait_recv()


FINAL_STEPS, FINAL_LAG = 14, 2


def attention_backward(counts, q_t, do_t, o_t, lse, kv, kv_t, grads, head_dim, part_rows):
    width, rows = q_t.shape
    keys = kv.shape[0]
    heads = width // head_dim
    q_block, key_chunk = 512, 512
    units = heads * rows // q_block
    piece_rows, piece_cols = width // 2, width
    pieces = [g.shape[0] * g.shape[1] // (2 * piece_rows * piece_cols) for g in grads]
    total = sum(pieces)
    vmem = pl.BlockSpec(memory_space=pltpu.VMEM)
    anywhere = pl.BlockSpec(memory_space=pl.ANY)
    return pl.pallas_call(
        functools.partial(backward_kernel, head_dim, q_block, key_chunk, part_rows, pieces),
        out_shape=[jax.ShapeDtypeStruct((width, rows), BF16), jax.ShapeDtypeStruct((part_rows, 2 * head_dim), F32)] + [jax.ShapeDtypeStruct(g.shape, F32) for g in grads],
        in_specs=[pl.BlockSpec(memory_space=pltpu.SMEM)] + [vmem] * 6 + [anywhere] * len(grads),
        out_specs=[vmem, vmem] + [anywhere] * len(grads),
        scratch_shapes=[
            pltpu.VMEM((2, 2 * head_dim, q_block), BF16),
            pltpu.VMEM((2, 2 * head_dim, q_block), BF16),
            pltpu.VMEM((units, 1, q_block), F32),
            pltpu.VMEM((units, 1, q_block), F32),
            pltpu.VMEM((2, key_chunk, q_block), BF16),
            pltpu.VMEM((2, key_chunk, q_block), BF16),
            pltpu.VMEM((units, head_dim, q_block), F32),
            pltpu.VMEM((4, part_rows, 2 * head_dim), F32),
            pltpu.VMEM((3, part_rows, 2 * head_dim), F32),
            pltpu.VMEM((part_rows, 2 * head_dim), F32),
            pltpu.VMEM((total, piece_rows, piece_cols), F32),
            pltpu.VMEM((total, piece_rows, piece_cols), F32),
            pltpu.VMEM((total, piece_rows, piece_cols), F32),
            pltpu.SemaphoreType.DMA((2, total)),
            pltpu.SemaphoreType.DMA((3, total)),
            pltpu.SemaphoreType.DMA((3, total)),
            pltpu.SemaphoreType.DMA((3,)),
            pltpu.SemaphoreType.DMA((3,)),
        ],
        compiler_params=pltpu.CompilerParams(vmem_limit_bytes=56 << 20, collective_id=1, has_side_effects=True),
        cost_estimate=pl.CostEstimate(flops=10 * heads * rows * keys * head_dim, bytes_accessed=40 << 20, transcendentals=heads * rows * keys),
        name='attention_bwd',
    )(counts, q_t, do_t, o_t, lse, kv, kv_t, *grads)


def solution(mesh):
    nodes = mesh.shape['nodes']
    row_spec = P(('graphs', 'nodes'), None)
    flat_spec = P(('graphs', 'nodes'))
    halo_spec = P(('graphs', 'nodes'), None, None)
    grad_spec = P('graphs', None)

    def device_step(x_feat, valid, halo_slot, edge_src, edge_dst, edge_mask, bal_perm, pos_enc, y_cot, w_msg, w_self, w_q, w_k, w_v, w_o, w_up, w_down):
        rows_dev, width = x_feat.shape
        head_dim = w_k.shape[1]
        rows_all = rows_dev * nodes
        me = lax.axis_index('nodes')

        pos_all = lax.all_gather(pos_enc, 'nodes', tiled=True)
        count = jnp.sum(valid)
        meta = lax.all_gather(jnp.concatenate([bal_perm, jnp.full((128,), count, jnp.int32)]), 'nodes')
        perm_all = meta[:, :rows_dev].reshape(1, rows_all)
        counts = meta[:, rows_dev]

        halo_req = halo_slot.reshape(nodes, -1)
        halo_rows = halo_req.size
        halo_got = lax.all_to_all(halo_req, 'nodes', 0, 0, tiled=True)
        halo_sent = jnp.take(x_feat, halo_got.reshape(-1), axis=0, mode='clip').reshape(nodes, -1, width)
        halo_feat = lax.all_to_all(halo_sent, 'nodes', 0, 0, tiled=True).reshape(halo_rows, width)
        adjacency_t = build_adjacency(edge_src, edge_dst, edge_mask, rows_dev, rows_dev + halo_rows).astype(BF16)
        table = jnp.concatenate([x_feat, halo_feat], axis=0)
        agg_msg = dot(adjacency_t, table, TN).astype(BF16)
        pre_act = dot(agg_msg, w_msg) + dot(x_feat, w_self)

        own_rows = me * rows_dev + lax.broadcasted_iota(jnp.int32, (rows_dev, 1), 0)
        pos_part = dot(jnp.where(perm_all == own_rows, 1.0, 0.0).astype(BF16), pos_all)
        hidden_in = (x_feat.astype(F32) + pos_part).astype(BF16)
        kv_loc = dot(hidden_in, jnp.concatenate([w_k, w_v], axis=1)).astype(BF16)
        kv_all = lax.all_gather(kv_loc, 'nodes', tiled=True)
        kv_all_t = kv_all.T
        q_t = dot(w_q, hidden_in, TT).astype(BF16)
        mixed_t, lse = attention_forward(counts, q_t, kv_all, kv_all_t, head_dim, rows_dev)
        u_part = dot(mixed_t, w_o, TN).astype(BF16).astype(F32)
        x_wide = x_feat.astype(F32)
        z_mid = (x_wide + jax.nn.relu(pre_act) + x_wide + u_part).astype(BF16)
        h_pre = dot(z_mid, w_up)
        hidden, gelu_pull = jax.vjp(jax.nn.gelu, h_pre)
        hidden = hidden.astype(BF16)
        keep_row = valid[:, None] > 0
        y_out = jnp.where(keep_row, z_mid.astype(F32) + dot(hidden, w_down), 0.0).astype(BF16)

        g_out = jnp.where(keep_row, y_cot, jnp.zeros_like(y_cot))
        grad_down = dot(hidden, g_out, TN)
        d_hidden = dot(g_out, w_down, NT).astype(BF16)
        d_hpre = gelu_pull(d_hidden.astype(F32))[0].astype(BF16)
        grad_up = dot(z_mid, d_hpre, TN)
        d_z = (g_out.astype(F32) + dot(d_hpre, w_up, NT)).astype(BF16)
        d_pre = jnp.where(pre_act > 0, d_z, jnp.zeros_like(d_z))
        grad_self = dot(x_feat, d_pre, TN)
        grad_msg = dot(agg_msg, d_pre, TN)
        grad_o = dot(mixed_t, d_z)
        do_t = dot(w_o, d_z, NT).astype(BF16)
        dq_t, dkv, grad_up, grad_down, grad_self, grad_msg, grad_o = attention_backward(counts, q_t, do_t, mixed_t, lse, kv_all, kv_all_t, (grad_up, grad_down, grad_self, grad_msg, grad_o), head_dim, rows_dev)

        d_agg = dot(d_pre, w_msg, NT).astype(BF16)
        d_table = dot(adjacency_t, d_agg)
        halo_landed = lax.all_to_all(d_table[rows_dev:].astype(BF16).reshape(nodes, -1, width), 'nodes', 0, 0, tiled=True)
        slot_hot = jnp.where(lax.broadcasted_iota(jnp.int32, (rows_dev, 1), 0) == halo_got.reshape(1, -1), 1.0, 0.0).astype(BF16)
        dx_base = 2.0 * d_z.astype(F32) + dot(d_pre, w_self, NT) + d_table[:rows_dev] + dot(slot_hot, halo_landed.reshape(-1, width))

        d_key = (dkv[:, :head_dim] * head_dim ** -0.5).astype(BF16)
        d_value = dkv[:, head_dim:].astype(BF16)
        grad_q = dot(hidden_in, dq_t, TT)
        grad_k = dot(hidden_in, d_key, TN)
        grad_v = dot(hidden_in, d_value, TN)
        attn_back = (dot(dq_t, w_q, TT) + dot(d_key, w_k, NT) + dot(d_value, w_v, NT)).astype(BF16)
        dx_feat = (dx_base + attn_back.astype(F32)).astype(BF16)
        grad_q, grad_k, grad_v = lax.psum((grad_q, grad_k, grad_v), 'nodes')
        return (y_out, dx_feat, grad_msg, grad_self, grad_q, grad_k, grad_v, grad_o, grad_up, grad_down)

    return jax.shard_map(device_step, mesh=mesh, in_specs=(row_spec, flat_spec, halo_spec, row_spec, row_spec, row_spec, flat_spec, row_spec, row_spec) + (P(),) * 8, out_specs=(row_spec, row_spec) + (grad_spec,) * 8, check_vma=False)
```

```python
import functools
import math

import jax
import jax.numpy as jnp
from jax import lax
from jax.experimental import pallas as pl
from jax.experimental.pallas import tpu as pltpu
from jax.sharding import PartitionSpec as P

NEG_FILL = -1e30
LOG2E = math.log2(math.e)
TAIL = 32
F32 = jnp.float32
BF16 = jnp.bfloat16
NN = (((1,), (0,)), ((), ()))
NT = (((1,), (1,)), ((), ()))
TN = (((0,), (0,)), ((), ()))
TT = (((0,), (1,)), ((), ()))


def dot(a, b, dims=NN):
    return lax.dot_general(a, b, dims, preferred_element_type=F32)


def adjacency_kernel(rows_dev, chunks, steps, width, src_ref, dst_ref, on_ref, out_ref, acc):
    half = rows_dev // 2
    table_rows = out_ref.shape[0]

    def step_block(index):
        cols = pl.ds(pl.multiple_of(index * width, width), width)
        src, dst, on = src_ref[:, cols], dst_ref[:, cols], on_ref[:, cols]
        upper = dst >= half
        place = jnp.where(upper, dst - half, dst)
        weight = jnp.where(on > 0, jnp.where(upper, 4096.0, 1.0), 0.0)
        src_hot = jnp.where(lax.broadcasted_iota(jnp.int32, (table_rows, width), 0) == src, 1.0, 0.0).astype(BF16)
        dst_hot = jnp.where(lax.broadcasted_iota(jnp.int32, (half, width), 0) == place, weight, 0.0).astype(BF16)
        return dot(src_hot, dst_hot, NT)

    for chunk in range(chunks):
        acc[...] = step_block(chunk * steps)

        def body(step, carry, chunk=chunk):
            acc[...] += step_block(chunk * steps + step)
            return carry

        lax.fori_loop(1, steps, body, 0)
        total = acc[...]
        high = jnp.floor(total * (1.0 / 4096.0))
        low = total - high * 4096.0
        if chunk == 0:
            out_ref[:, :half] = low
            out_ref[:, half:] = high
        else:
            out_ref[:, :half] += low
            out_ref[:, half:] += high


def build_adjacency(edge_src, edge_dst, edge_mask, rows_dev, table_rows):
    edges = edge_src.shape[1]
    width = 512
    chunks = 4
    steps = edges // (chunks * width)
    assert chunks * steps * width == edges and steps * width < 4096
    return pl.pallas_call(
        functools.partial(adjacency_kernel, rows_dev, chunks, steps, width),
        out_shape=jax.ShapeDtypeStruct((table_rows, rows_dev), F32),
        in_specs=[pl.BlockSpec(memory_space=pltpu.VMEM)] * 3,
        out_specs=pl.BlockSpec(memory_space=pltpu.VMEM),
        scratch_shapes=[pltpu.VMEM((table_rows, rows_dev // 2), F32)],
        compiler_params=pltpu.CompilerParams(vmem_limit_bytes=40 << 20),
        cost_estimate=pl.CostEstimate(flops=edges * table_rows * rows_dev, bytes_accessed=6 << 20, transcendentals=0),
        name='adjacency',
    )(edge_src, edge_dst, edge_mask)


def mask_tail(scores, chunk, key_chunk, part_rows, count_ref):
    start = chunk * key_chunk
    part = start // part_rows
    first = start - part * part_rows + key_chunk - TAIL
    row_ix = first + lax.broadcasted_iota(jnp.int32, (TAIL, scores.shape[1]), 0)
    tail = jnp.where(row_ix < count_ref[part], scores[key_chunk - TAIL:, :], NEG_FILL)
    return jnp.concatenate([scores[:key_chunk - TAIL, :], tail], axis=0)


def attention_fwd_kernel(head_dim, q_block, key_chunk, part_rows, count_ref, q_ref, kv_ref, kvt_ref, out_ref, lse_ref, w_q, s_buf, stat):
    heads = q_ref.shape[0] // head_dim
    blocks = q_ref.shape[1] // q_block
    units = heads * blocks
    keys = kv_ref.shape[0]
    chunks = keys // key_chunk
    factor = head_dim ** -0.5 * LOG2E
    groups = key_chunk // 8

    def load_weights(unit):
        head, block = unit // blocks, lax.rem(unit, blocks)
        w_q[:head_dim, :] = q_ref[pl.ds(pl.multiple_of(head * head_dim, head_dim), head_dim), pl.ds(pl.multiple_of(block * q_block, q_block), q_block)]

    def score_stage(slot, chunk, run_max):
        rows = pl.ds(pl.multiple_of(chunk * key_chunk, key_chunk), key_chunk)
        scores = mask_tail(dot(kv_ref[rows, :], w_q[...]), chunk, key_chunk, part_rows, count_ref)
        s_buf[slot, rows, :] = scores
        return jnp.maximum(run_max, jnp.max(scores.reshape(groups, 8, q_block), axis=0))

    w_q[head_dim:, :] = jnp.zeros((w_q.shape[0] - head_dim, q_block), BF16)
    floor = jnp.full((8, q_block), -jnp.inf, F32)
    load_weights(0)
    stat[...] = lax.fori_loop(0, chunks, lambda chunk, run_max: score_stage(0, chunk, run_max), floor)

    def unit_body(unit, carry):
        slot = lax.rem(unit, 2)
        load_weights(jnp.minimum(unit + 1, units - 1))
        top = jnp.max(stat[...], axis=0, keepdims=True) * factor

        def chunk_body(chunk, state):
            run_max, run_sum, weighted = state
            cols = pl.ds(pl.multiple_of(chunk * key_chunk, key_chunk), key_chunk)
            prob = jnp.exp2(s_buf[slot, cols, :] * factor - top)
            run_sum = run_sum + jnp.sum(prob.reshape(groups, 8, q_block), axis=0)
            weighted = weighted + dot(kvt_ref[head_dim:2 * head_dim, cols], prob.astype(BF16))
            return score_stage(1 - slot, chunk, run_max), run_sum, weighted

        run_max, run_sum, weighted = lax.fori_loop(0, chunks, chunk_body, (floor, jnp.zeros((8, q_block), F32), jnp.zeros((head_dim, q_block), F32)))
        stat[...] = run_max
        total = jnp.sum(run_sum, axis=0, keepdims=True)
        head, block = unit // blocks, lax.rem(unit, blocks)
        cols = pl.ds(pl.multiple_of(block * q_block, q_block), q_block)
        out_ref[pl.ds(pl.multiple_of(head * head_dim, head_dim), head_dim), cols] = (weighted / total).astype(BF16)
        lse_ref[pl.ds(head, 1), cols] = top + jnp.log2(total)
        return carry

    lax.fori_loop(0, units, unit_body, 0)


def attention_forward(counts, q_t, kv, kv_t, head_dim, part_rows):
    width, rows = q_t.shape
    keys = kv.shape[0]
    heads = width // head_dim
    q_block, key_chunk = 256, 1024
    vmem = pl.BlockSpec(memory_space=pltpu.VMEM)
    return pl.pallas_call(
        functools.partial(attention_fwd_kernel, head_dim, q_block, key_chunk, part_rows),
        out_shape=[jax.ShapeDtypeStruct((width, rows), BF16), jax.ShapeDtypeStruct((heads, rows), F32)],
        in_specs=[pl.BlockSpec(memory_space=pltpu.SMEM), vmem, vmem, vmem],
        out_specs=[vmem, vmem],
        scratch_shapes=[pltpu.VMEM((2 * head_dim, q_block), BF16), pltpu.VMEM((2, keys, q_block), F32), pltpu.VMEM((8, q_block), F32)],
        compiler_params=pltpu.CompilerParams(vmem_limit_bytes=48 << 20),
        cost_estimate=pl.CostEstimate(flops=4 * heads * rows * keys * head_dim, bytes_accessed=4 << 20, transcendentals=heads * rows * keys),
        name='attention_fwd',
    )(counts, q_t, kv, kv_t)


FINAL_STEPS, FINAL_LAG = 14, 2
FIRST_PIECES, HOLD_PIECES, HOLD_STEP = 2, 7, 68


def backward_kernel(head_dim, q_block, key_chunk, part_rows, pieces, count_ref, q_ref, do_ref, o_ref, lse_ref, kv_ref, kvt_ref, hid_ref, x_ref, agg_ref, dz_ref, dpre_ref, adj_ref, slot_ref, w_msg_ref, w_self_ref, w_qt_ref, w_kv_ref, up_ref, down_ref, *rest):
    arrays = len(pieces)
    dx_ref, rest = rest[0], rest[1:]
    sum_refs, rest = rest[:arrays], rest[arrays:]
    kv_sum_ref, rest = rest[0], rest[1:]
    w_q, w_do, lse_buf, delta_buf, p_buf, ds_buf, dq_acc, dq_all, dkv_acc, dkv_in, dkv_sum, local, own, from_mate, from_cross, kv_local, kv_own, kv_in, halo_out, halo_in, dx_acc, own_sem, send_sem, recv_sem, dkv_send, dkv_recv, kv_sem, kv_send, kv_recv, halo_send, halo_recv = rest
    heads = q_ref.shape[0] // head_dim
    blocks = q_ref.shape[1] // q_block
    units = heads * blocks
    chunks = kv_ref.shape[0] // key_chunk
    steps = units * chunks
    per_group = steps // 4
    halves = part_rows // key_chunk
    scale = head_dim ** -0.5
    factor = scale * LOG2E
    total = own.shape[0]
    first_small = total - 4
    half_rows, width = own.shape[1:]

    me = lax.axis_index('nodes')
    chip, side = me // 2, lax.rem(me, 2)
    mate = chip * 2 + 1 - side
    cross = (1 - chip) * 2 + side
    other = (1 - chip) * 2 + 1 - side

    spots = [(array, j) for array in range(arrays) for j in range(pieces[array])]

    def block(refs, spot, half):
        array, j = spot
        ref = refs[array]
        if ref.shape[1] > width:
            return ref.at[pl.ds(half * half_rows, half_rows), pl.ds(j * width, width)]
        return ref.at[pl.ds((half * pieces[array] + j) * half_rows, half_rows), :]

    def source(index, half):
        if index < first_small:
            return block((up_ref, down_ref), spots[index], half)
        return local.at[index - first_small, pl.ds(half * half_rows, half_rows), :]

    def remote(src, dst, send, recv, peer):
        return pltpu.make_async_remote_copy(src_ref=src, dst_ref=dst, send_sem=send, recv_sem=recv, device_id={'nodes': peer}, device_id_type=pl.DeviceIdType.MESH)

    def to_peer(src, dst, kind, index, peer):
        return remote(src, dst, send_sem.at[kind, index], recv_sem.at[kind, index], peer)

    def mate_copy(index):
        return to_peer(source(index, 1 - side), from_mate.at[index], 0, index, mate)

    def own_copy(index):
        return pltpu.make_async_copy(source(index, side), own.at[index], own_sem.at[0, index])

    def cross_copy(index):
        return to_peer(own.at[index], from_cross.at[index], 1, index, cross)

    def back_copy(index, half):
        return to_peer(from_mate.at[index], block(sum_refs, spots[index], half), 2, index, mate)

    def keep_copy(index):
        return pltpu.make_async_copy(from_mate.at[index], block(sum_refs, spots[index], side), own_sem.at[1, index])

    def chip_sum(index):
        to_peer(own.at[index], from_mate.at[index], 0, index, mate).wait_recv()
        pltpu.make_async_copy(own.at[index], own.at[index], own_sem.at[0, index]).wait()
        own[index] = own[index] + from_mate[index]

    def group_sum(index):
        cross_copy(index).wait_recv()
        from_mate[index] = own[index] + from_cross[index]

    def start_out(index):
        keep_copy(index).start()
        back_copy(index, side).start()

    dkv_copies = [remote(src, dkv_in.at[i], dkv_send.at[i], dkv_recv.at[i], peer) for i, (src, peer) in enumerate(((dkv_acc.at[0], mate), (dkv_sum, cross), (dkv_acc.at[2], mate)))]

    def kv_rows(half):
        return pl.ds(half * half_rows, half_rows)

    kv_to_mate = remote(kv_local.at[kv_rows(1 - side), :], kv_in.at[0], kv_send.at[0], kv_recv.at[0], mate)
    kv_to_cross = remote(kv_own.at[0], kv_in.at[1], kv_send.at[1], kv_recv.at[1], cross)
    kv_keep = pltpu.make_async_copy(kv_own.at[1], kv_sum_ref.at[kv_rows(side), :], kv_sem)

    def kv_back(half):
        return remote(kv_own.at[1], kv_sum_ref.at[kv_rows(half), :], kv_send.at[2], kv_recv.at[2], mate)

    halo_pair = halo_out.shape[1]

    def halo_copy(peer, owner):
        return remote(halo_out.at[peer], halo_in.at[owner], halo_send.at[peer], halo_recv.at[owner], peer)

    barrier = pltpu.get_barrier_semaphore()
    for peer in (mate, cross, other):
        pl.semaphore_signal(barrier, inc=1, device_id={'nodes': peer}, device_id_type=pl.DeviceIdType.MESH)
    pl.semaphore_wait(barrier, 3)
    for index in range(first_small):
        mate_copy(index).start()
        own_copy(index).start()

    def unit_spots(unit):
        head, place = unit // blocks, lax.rem(unit, blocks)
        return head, pl.ds(pl.multiple_of(head * head_dim, head_dim), head_dim), pl.ds(pl.multiple_of(place * q_block, q_block), q_block)

    def prepare(unit, carry):
        head, rows, cols = unit_spots(unit)
        delta_buf[unit] = jnp.sum(do_ref[rows, cols].astype(F32) * o_ref[rows, cols].astype(F32), axis=0, keepdims=True)
        lse_buf[unit] = lse_ref[pl.ds(head, 1), cols]
        dq_acc[unit] = jnp.zeros((head_dim, q_block), F32)
        return carry

    lax.fori_loop(0, units, prepare, 0)
    for index in range(FIRST_PIECES):
        chip_sum(index)
    for slot in range(2):
        w_q[slot, head_dim:, :] = jnp.zeros((head_dim, q_block), BF16)
        w_do[slot, :head_dim, :] = jnp.zeros((head_dim, q_block), BF16)
    dkv_acc[...] = jnp.zeros_like(dkv_acc)
    for index in range(FIRST_PIECES):
        cross_copy(index).start()

    d_agg = dot(dpre_ref[...], w_msg_ref[...], NT).astype(BF16)
    halo_out[...] = dot(adj_ref[part_rows:, :], d_agg).astype(BF16).reshape(halo_out.shape)
    dx_acc[...] = 2.0 * dz_ref[...].astype(F32) + dot(dpre_ref[...], w_self_ref[...], NT)
    dx_acc[...] += dot(adj_ref[:part_rows, :], d_agg)
    for peer in (mate, cross, other):
        halo_copy(peer, me).start()
    halo_in[me] = halo_out[me]
    local[0] = dot(x_ref[...], dpre_ref[...], TN)
    local[1] = dot(agg_ref[...], dpre_ref[...], TN)
    local[2] = dot(o_ref[...], dz_ref[...])

    def place_of(step):
        group = step // per_group
        chunk = step // units
        owner = lax.rem(chip + 1 - group // 2, 2) * 2 + lax.rem(side + 1 - lax.rem(group, 2), 2)
        offset = lax.rem(chunk, halves) * key_chunk
        rows = pl.ds(pl.multiple_of(owner * part_rows + offset, key_chunk), key_chunk)
        return group, owner, offset, rows, lax.rem(step, units), lax.rem(step, 2)

    def first_stage(step):
        group, owner, offset, rows, unit, slot = place_of(step)
        head, unit_rows, cols = unit_spots(unit)
        w_q[slot, :head_dim, :] = q_ref[unit_rows, cols]
        w_do[slot, head_dim:, :] = do_ref[unit_rows, cols]
        kv = kv_ref[rows, :]
        scores = dot(kv, w_q[slot])
        row_ix = offset + key_chunk - TAIL + lax.broadcasted_iota(jnp.int32, (TAIL, q_block), 0)
        tail = jnp.where(row_ix < count_ref[owner], scores[key_chunk - TAIL:, :], NEG_FILL)
        scores = jnp.concatenate([scores[:key_chunk - TAIL, :], tail], axis=0)
        prob = jnp.exp2(scores * factor - lse_buf[unit])
        p_buf[slot] = prob.astype(BF16)
        ds_buf[slot] = (prob * (dot(kv, w_do[slot]) - delta_buf[unit])).astype(BF16)

    def second_stage(step):
        group, owner, offset, rows, unit, slot = place_of(step)
        d_scores = ds_buf[slot]
        spot = pl.ds(pl.multiple_of(offset, key_chunk), key_chunk)
        dkv_acc[group, spot, :] += dot(d_scores, w_q[slot], NT) + dot(p_buf[slot], w_do[slot], NT)
        dq_acc[unit] += dot(kvt_ref[:head_dim, rows], d_scores)

    def exchange(step):
        early = jnp.where(step < 4 * (HOLD_PIECES - FIRST_PIECES), 1, 0)
        late = jnp.where(jnp.logical_and(step >= HOLD_STEP, step < HOLD_STEP + 4 * (first_small + 3 - HOLD_PIECES)), 1, 0)
        turn = step // 4 + FIRST_PIECES - late * (HOLD_STEP // 4 + FIRST_PIECES - HOLD_PIECES)
        phase = lax.rem(step, 4)

        @pl.when(jnp.logical_and(early + late == 1, phase == 1))
        def sum_chip():
            chip_sum(turn)

        @pl.when(jnp.logical_and(early + late == 1, phase == 2))
        def send_cross():
            cross_copy(turn).start()

        lap, beat = step // FINAL_STEPS - FINAL_LAG, lax.rem(step, FINAL_STEPS)

        @pl.when(jnp.logical_and(lap >= 0, beat == 0))
        def sum_group():
            group_sum(lap)

        @pl.when(jnp.logical_and(lap >= 0, beat == 1))
        def send_back():
            for k in range(done):
                @pl.when(lap == k)
                def start_piece(k=k):
                    start_out(k)

        @pl.when(step == 3)
        def small_pieces():
            for index in range(first_small, total - 1):
                mate_copy(index).start()
                own_copy(index).start()

        @pl.when(step == per_group + 1)
        def first_group():
            dkv_copies[0].start()

        @pl.when(step == 2 * per_group + 1)
        def second_group():
            dkv_copies[0].wait_recv()
            dkv_sum[...] = dkv_acc[1] + dkv_in[0]

        @pl.when(step == 2 * per_group + 2)
        def send_second():
            dkv_copies[1].start()

        @pl.when(step == 3 * per_group + 1)
        def third_group():
            dkv_copies[2].start()

    done = (steps - 1) // FINAL_STEPS - FINAL_LAG + 1
    assert (steps - 1) % FINAL_STEPS >= 1 and 0 < done <= first_small and HOLD_STEP > 2 * per_group + 2 and HOLD_STEP % 4 == 0

    first_stage(0)

    def body(step, carry):
        exchange(step)
        second_stage(step - 1)
        first_stage(step)
        return carry

    lax.fori_loop(1, steps, body, 0)
    second_stage(steps - 1)

    def gather_dq(unit, carry):
        head, rows, cols = unit_spots(unit)
        dq_all[rows, cols] = (dq_acc[unit] * scale).astype(BF16)
        return carry

    lax.fori_loop(0, units, gather_dq, 0)
    last = total - 1
    local[3] = dot(dq_all[...], hid_ref[...]).T
    dkv_copies[2].wait_recv()
    dkv_copies[1].wait_recv()
    dkv = dkv_acc[3] + dkv_in[2] + dkv_in[1]
    lane = lax.broadcasted_iota(jnp.int32, dkv.shape, 1)
    dkv = jnp.where(lane < head_dim, dkv * scale, dkv).astype(BF16)
    mate_copy(last).start()
    own_copy(last).start()
    kv_local[...] = dot(hid_ref[...], dkv, TN)
    dx_acc[...] += dot(dkv, w_kv_ref[...], NT)
    kv_to_mate.start()
    chip_sum(last)
    kv_to_mate.wait_recv()
    kv_own[0] = kv_local[kv_rows(side), :] + kv_in[0]
    for peer in (mate, cross, other):
        halo_copy(me, peer).wait_recv()
    slot_hot = jnp.where(lax.broadcasted_iota(jnp.int32, (part_rows, 4 * halo_pair), 0) == slot_ref[...], 1.0, 0.0).astype(BF16)
    dx_acc[...] += dot(slot_hot, halo_in[...].reshape(4 * halo_pair, width))
    cross_copy(last).start()
    kv_to_cross.start()
    dx_ref[...] = (dx_acc[...] + dot(dq_all[...], w_qt_ref[...], TN)).astype(BF16)
    for index in range(done, total):
        group_sum(index)
        if index > done:
            start_out(index - 1)
    kv_to_cross.wait_recv()
    kv_own[1] = kv_own[0] + kv_in[1]
    start_out(last)
    kv_keep.start()
    kv_back(side).start()
    for copy in dkv_copies + [kv_to_mate, kv_to_cross, kv_back(side)] + [halo_copy(peer, me) for peer in (mate, cross, other)]:
        copy.wait_send()
    kv_keep.wait()
    kv_back(1 - side).wait_recv()
    for index in range(total):
        mate_copy(index).wait_send()
        cross_copy(index).wait_send()
        keep_copy(index).wait()
        back_copy(index, side).wait_send()
        back_copy(index, 1 - side).wait_recv()


def backward(counts, q_t, do_t, o_t, lse, kv, kv_t, hidden_in, x_feat, agg_msg, d_z, d_pre, adjacency_t, halo_got, w_msg, w_self, w_q_t, w_kv, grad_up, grad_down):
    width, rows = q_t.shape
    keys = kv.shape[0]
    head_dim = kv.shape[1] // 2
    heads = width // head_dim
    nodes = keys // rows
    q_block, key_chunk = 512, 512
    units = heads * rows // q_block
    piece_rows = width // 2
    shapes = [grad_up.shape, grad_down.shape] + [(width, width)] * 4
    pieces = [r * c // (2 * piece_rows * width) for r, c in shapes]
    total = sum(pieces)
    halo_pair = halo_got.shape[1] // nodes
    vmem = pl.BlockSpec(memory_space=pltpu.VMEM)
    anywhere = pl.BlockSpec(memory_space=pl.ANY)
    dma = pltpu.SemaphoreType.DMA
    return pl.pallas_call(
        functools.partial(backward_kernel, head_dim, q_block, key_chunk, rows, pieces),
        out_shape=[jax.ShapeDtypeStruct((rows, width), BF16)] + [jax.ShapeDtypeStruct(shape, F32) for shape in shapes] + [jax.ShapeDtypeStruct((width, 2 * head_dim), F32)],
        in_specs=[pl.BlockSpec(memory_space=pltpu.SMEM)] + [vmem] * 17 + [anywhere] * 2,
        out_specs=[vmem] + [anywhere] * 7,
        scratch_shapes=[
            pltpu.VMEM((2, 2 * head_dim, q_block), BF16),
            pltpu.VMEM((2, 2 * head_dim, q_block), BF16),
            pltpu.VMEM((units, 1, q_block), F32),
            pltpu.VMEM((units, 1, q_block), F32),
            pltpu.VMEM((2, key_chunk, q_block), BF16),
            pltpu.VMEM((2, key_chunk, q_block), BF16),
            pltpu.VMEM((units, head_dim, q_block), F32),
            pltpu.VMEM((width, rows), BF16),
            pltpu.VMEM((4, rows, 2 * head_dim), F32),
            pltpu.VMEM((3, rows, 2 * head_dim), F32),
            pltpu.VMEM((rows, 2 * head_dim), F32),
            pltpu.VMEM((4, width, width), F32),
            pltpu.VMEM((total, piece_rows, width), F32),
            pltpu.VMEM((total, piece_rows, width), F32),
            pltpu.VMEM((total, piece_rows, width), F32),
            pltpu.VMEM((width, 2 * head_dim), F32),
            pltpu.VMEM((2, piece_rows, 2 * head_dim), F32),
            pltpu.VMEM((2, piece_rows, 2 * head_dim), F32),
            pltpu.VMEM((nodes, halo_pair, width), BF16),
            pltpu.VMEM((nodes, halo_pair, width), BF16),
            pltpu.VMEM((rows, width), F32),
            dma((2, total)), dma((3, total)), dma((3, total)), dma((3,)), dma((3,)), dma, dma((3,)), dma((3,)), dma((nodes,)), dma((nodes,)),
        ],
        compiler_params=pltpu.CompilerParams(vmem_limit_bytes=62 << 20, collective_id=1, has_side_effects=True),
        cost_estimate=pl.CostEstimate(flops=10 * heads * rows * keys * head_dim, bytes_accessed=40 << 20, transcendentals=heads * rows * keys),
        name='backward',
    )(counts, q_t, do_t, o_t, lse, kv, kv_t, hidden_in, x_feat, agg_msg, d_z, d_pre, adjacency_t, halo_got, w_msg, w_self, w_q_t, w_kv, grad_up, grad_down)


def solution(mesh):
    nodes = mesh.shape['nodes']
    row_spec = P(('graphs', 'nodes'), None)
    flat_spec = P(('graphs', 'nodes'))
    halo_spec = P(('graphs', 'nodes'), None, None)
    grad_spec = P('graphs', None)

    def device_step(x_feat, valid, halo_slot, edge_src, edge_dst, edge_mask, bal_perm, pos_enc, y_cot, w_msg, w_self, w_q, w_k, w_v, w_o, w_up, w_down):
        rows_dev, width = x_feat.shape
        head_dim = w_k.shape[1]
        rows_all = rows_dev * nodes
        me = lax.axis_index('nodes')

        pos_all = lax.all_gather(pos_enc, 'nodes', tiled=True)
        count = jnp.sum(valid)
        meta = lax.all_gather(jnp.concatenate([bal_perm, jnp.full((128,), count, jnp.int32)]), 'nodes')
        perm_all = meta[:, :rows_dev].reshape(1, rows_all)
        counts = meta[:, rows_dev]

        halo_req = halo_slot.reshape(nodes, -1)
        halo_rows = halo_req.size
        halo_got = lax.all_to_all(halo_req, 'nodes', 0, 0, tiled=True)
        halo_sent = jnp.take(x_feat, halo_got.reshape(-1), axis=0, mode='clip').reshape(nodes, -1, width)
        halo_feat = lax.all_to_all(halo_sent, 'nodes', 0, 0, tiled=True).reshape(halo_rows, width)
        adjacency_t = build_adjacency(edge_src, edge_dst, edge_mask, rows_dev, rows_dev + halo_rows).astype(BF16)
        table = jnp.concatenate([x_feat, halo_feat], axis=0)
        agg_msg = dot(adjacency_t, table, TN).astype(BF16)
        pre_act = dot(agg_msg, w_msg) + dot(x_feat, w_self)

        own_rows = me * rows_dev + lax.broadcasted_iota(jnp.int32, (rows_dev, 1), 0)
        pos_part = dot(jnp.where(perm_all == own_rows, 1.0, 0.0).astype(BF16), pos_all)
        hidden_in = (x_feat.astype(F32) + pos_part).astype(BF16)
        w_kv = jnp.concatenate([w_k, w_v], axis=1)
        kv_loc = dot(hidden_in, w_kv).astype(BF16)
        kv_all = lax.all_gather(kv_loc, 'nodes', tiled=True)
        kv_all_t = kv_all.T
        q_t = dot(w_q, hidden_in, TT).astype(BF16)
        mixed_t, lse = attention_forward(counts, q_t, kv_all, kv_all_t, head_dim, rows_dev)
        u_part = dot(mixed_t, w_o, TN).astype(BF16).astype(F32)
        x_wide = x_feat.astype(F32)
        z_mid = (x_wide + jax.nn.relu(pre_act) + x_wide + u_part).astype(BF16)
        h_pre = dot(z_mid, w_up)
        hidden, gelu_pull = jax.vjp(jax.nn.gelu, h_pre)
        hidden = hidden.astype(BF16)
        keep_row = valid[:, None] > 0
        y_out = jnp.where(keep_row, z_mid.astype(F32) + dot(hidden, w_down), 0.0).astype(BF16)

        g_out = jnp.where(keep_row, y_cot, jnp.zeros_like(y_cot))
        grad_down = dot(hidden, g_out, TN)
        d_hidden = dot(g_out, w_down, NT).astype(BF16)
        d_hpre = gelu_pull(d_hidden.astype(F32))[0].astype(BF16)
        grad_up = dot(z_mid, d_hpre, TN)
        d_z = (g_out.astype(F32) + dot(d_hpre, w_up, NT)).astype(BF16)
        d_pre = jnp.where(pre_act > 0, d_z, jnp.zeros_like(d_z))
        do_t = dot(w_o, d_z, NT).astype(BF16)
        dx_feat, grad_up, grad_down, grad_self, grad_msg, grad_o, grad_q, grad_kv = backward(counts, q_t, do_t, mixed_t, lse, kv_all, kv_all_t, hidden_in, x_feat, agg_msg, d_z, d_pre, adjacency_t, halo_got.reshape(1, halo_rows), w_msg, w_self, w_q.T, w_kv, grad_up, grad_down)
        grad_k, grad_v = grad_kv[:, :head_dim], grad_kv[:, head_dim:]
        return (y_out, dx_feat, grad_msg, grad_self, grad_q, grad_k, grad_v, grad_o, grad_up, grad_down)

    return jax.shard_map(device_step, mesh=mesh, in_specs=(row_spec, flat_spec, halo_spec, row_spec, row_spec, row_spec, flat_spec, row_spec, row_spec) + (P(),) * 8, out_specs=(row_spec, row_spec) + (grad_spec,) * 8, check_vma=False)
```

```python
import functools
import math

import jax
import jax.numpy as jnp
from jax import lax
from jax.experimental import pallas as pl
from jax.experimental.pallas import tpu as pltpu
from jax.sharding import PartitionSpec as P

NEG_FILL = -1e30
LOG2E = math.log2(math.e)
TAIL = 32
F32 = jnp.float32
BF16 = jnp.bfloat16
NN = (((1,), (0,)), ((), ()))
NT = (((1,), (1,)), ((), ()))
TN = (((0,), (0,)), ((), ()))
TT = (((0,), (1,)), ((), ()))


def dot(a, b, dims=NN):
    return lax.dot_general(a, b, dims, preferred_element_type=F32)


def remote(src, dst, send, recv, peer):
    return pltpu.make_async_remote_copy(src_ref=src, dst_ref=dst, send_sem=send, recv_sem=recv, device_id={'nodes': peer}, device_id_type=pl.DeviceIdType.MESH)


def neighbours():
    me = lax.axis_index('nodes')
    chip, side = me // 2, lax.rem(me, 2)
    return me, chip, side, chip * 2 + 1 - side, (1 - chip) * 2 + side, (1 - chip) * 2 + 1 - side


def meet(peers):
    barrier = pltpu.get_barrier_semaphore()
    for peer in peers:
        pl.semaphore_signal(barrier, inc=1, device_id={'nodes': peer}, device_id_type=pl.DeviceIdType.MESH)
    pl.semaphore_wait(barrier, len(peers))


CHUNKS, EDGE_STEP, POS_PIECES, KV_PIECES = 4, 512, 4, 2


def front_kernel(meta_ref, x_ref, pos_ref, src_ref, dst_ref, on_ref, w_qt_ref, w_kv_ref, w_msg_ref, w_self_ref, q_ref, kv_ref, kvt_ref, hid_ref, agg_ref, pre_ref, adj_ref, slot_ref, count_ref, meta_all, pos_all, pos_acc, counts_acc, edge_acc, halo_out, halo_in, kv_all, meta_send, meta_recv, pos_send, pos_recv, halo_send, halo_recv, kv_send, kv_recv):
    rows_dev, width = x_ref.shape
    table_rows = adj_ref.shape[0]
    half = rows_dev // 2
    nodes = meta_all.shape[0]
    halo_pair = halo_in.shape[1]
    me, chip, side, mate, cross, other = neighbours()
    peers = (mate, cross, other)
    meet(peers)

    meta_copies = [remote(meta_ref, meta_all.at[me], meta_send.at[i], meta_recv.at[me], peer) for i, peer in enumerate(peers)]
    for copy in meta_copies:
        copy.start()
    piece = rows_dev // POS_PIECES

    def pos_rows(index):
        return pl.ds(index * piece, piece)

    pos_to_cross = [remote(pos_ref.at[pos_rows(k), :], pos_all.at[me, pos_rows(k), :], pos_send.at[0, k], pos_recv.at[0, k], cross) for k in range(POS_PIECES)]
    pos_to_mate = [remote(pos_ref.at[pos_rows(k), :], pos_all.at[me, pos_rows(k), :], pos_send.at[1, k], pos_recv.at[1, k], mate) for k in range(POS_PIECES)]
    pos_relay = [remote(pos_all.at[cross, pos_rows(k), :], pos_all.at[cross, pos_rows(k), :], pos_send.at[2, k], pos_recv.at[2, k], mate) for k in range(POS_PIECES)]
    for copy in pos_to_cross + pos_to_mate:
        copy.start()
    meta_all[me] = meta_ref[...]

    def relay_pos(k):
        pos_to_cross[k].wait_recv()
        pos_relay[k].start()

    def place_pos(owner, source, first):
        perm = meta_all[owner, 0:1, :] - me * rows_dev
        size = 256

        def body(index, carry):
            rows = pl.ds(pl.multiple_of(index * size, size), size)
            hot = jnp.where(index * size + lax.broadcasted_iota(jnp.int32, (size, rows_dev), 0) == perm, 1.0, 0.0).astype(BF16)
            part = dot(hot, source[...])
            pos_acc[rows, :] = part if first else pos_acc[rows, :] + part
            return carry

        lax.fori_loop(0, rows_dev // size, body, 0)

    edges = src_ref.shape[1]
    steps = edges // (CHUNKS * EDGE_STEP)
    assert CHUNKS * EDGE_STEP * steps == edges and EDGE_STEP * steps < 4096

    def edge_block(index):
        cols = pl.ds(pl.multiple_of(index * EDGE_STEP, EDGE_STEP), EDGE_STEP)
        src, dst, on = src_ref[:, cols], dst_ref[:, cols], on_ref[:, cols]
        upper = dst >= half
        place = jnp.where(upper, dst - half, dst)
        weight = jnp.where(on > 0, jnp.where(upper, 4096.0, 1.0), 0.0)
        src_hot = jnp.where(lax.broadcasted_iota(jnp.int32, (table_rows, EDGE_STEP), 0) == src, 1.0, 0.0).astype(BF16)
        dst_hot = jnp.where(lax.broadcasted_iota(jnp.int32, (half, EDGE_STEP), 0) == place, weight, 0.0).astype(BF16)
        return dot(src_hot, dst_hot, NT)

    def count_chunk(chunk):
        edge_acc[...] = jnp.zeros_like(edge_acc)

        def body(step, carry):
            edge_acc[...] += edge_block(chunk * steps + step)
            return carry

        lax.fori_loop(0, steps, body, 0)
        total = edge_acc[...]
        high = jnp.floor(total * (1.0 / 4096.0))
        low = total - high * 4096.0
        if chunk == 0:
            counts_acc[:, :half] = low
            counts_acc[:, half:] = high
        elif chunk < CHUNKS - 1:
            counts_acc[:, :half] += low
            counts_acc[:, half:] += high
        else:
            adj_ref[:, :half] = (counts_acc[:, :half] + low).astype(BF16)
            adj_ref[:, half:] = (counts_acc[:, half:] + high).astype(BF16)

    def halo_copy(peer, owner):
        return remote(halo_out.at[peer], halo_in.at[owner], halo_send.at[peer], halo_recv.at[owner], peer)

    count_chunk(0)
    for peer in peers:
        remote(meta_ref, meta_all.at[peer], meta_send.at[0], meta_recv.at[peer], peer).wait_recv()
    tables = meta_all[0, :, 0:nodes * halo_pair]
    for node in range(1, nodes):
        tables = jnp.maximum(tables, meta_all[node, :, 0:nodes * halo_pair])
    tables = jnp.where(lax.broadcasted_iota(jnp.int32, tables.shape, 0) == 2 + me, tables, -1)
    slots = jnp.max(tables.astype(F32), axis=0, keepdims=True).astype(jnp.int32)
    slot_ref[...] = slots
    slot_hot = jnp.where(lax.broadcasted_iota(jnp.int32, (rows_dev, nodes * halo_pair), 0) == slots, 1.0, 0.0).astype(BF16)
    halo_out[...] = dot(slot_hot, x_ref[...], TN).astype(BF16).reshape(halo_out.shape)
    relay_pos(0)
    place_pos(me, pos_ref, True)
    for peer in peers:
        halo_copy(peer, me).start()
    halo_in[me] = halo_out[me]
    for node in range(nodes):
        held = jnp.sum(meta_all[node, 1:2, :].astype(F32), axis=1, keepdims=True).astype(jnp.int32)
        count_ref[node:node + 1, :] = jnp.broadcast_to(held, (1, count_ref.shape[1]))
    count_chunk(1)
    relay_pos(1)
    for copy in pos_to_mate:
        copy.wait_recv()
    place_pos(mate, pos_all.at[mate], False)
    count_chunk(2)
    relay_pos(2)
    count_chunk(3)
    relay_pos(3)
    place_pos(cross, pos_all.at[cross], False)
    for copy in pos_relay:
        copy.wait_recv()
    place_pos(other, pos_all.at[other], False)

    hidden = (x_ref[...].astype(F32) + pos_acc[...]).astype(BF16)
    hid_ref[...] = hidden
    kv_all[me] = dot(hidden, w_kv_ref[...]).astype(BF16)
    q_ref[...] = dot(w_qt_ref[...], hid_ref[...], NT).astype(BF16)
    kv_piece = rows_dev // KV_PIECES

    def kv_copy(owner, k, kind, peer):
        rows = pl.ds(k * kv_piece, kv_piece)
        return remote(kv_all.at[owner, rows, :], kv_all.at[owner, rows, :], kv_send.at[kind, k], kv_recv.at[kind, k], peer)

    kv_to_cross = [kv_copy(me, k, 0, cross) for k in range(KV_PIECES)]
    kv_to_mate = [kv_copy(me, k, 1, mate) for k in range(KV_PIECES)]
    kv_relay = [kv_copy(cross, k, 2, mate) for k in range(KV_PIECES)]
    for copy in kv_to_cross + kv_to_mate:
        copy.start()
    size = 2 * w_qt_ref.shape[0] // 8
    eye = jnp.where(lax.broadcasted_iota(jnp.int32, (size, size), 0) == lax.broadcasted_iota(jnp.int32, (size, size), 1), 1.0, 0.0).astype(BF16)

    def keep_kv(owner):
        rows = pl.ds(pl.multiple_of(owner * rows_dev, rows_dev), rows_dev)
        kv_ref[rows, :] = kv_all[owner]
        kvt_ref[:, rows] = dot(eye, kv_all[owner], NT).astype(BF16)

    for peer in peers:
        halo_copy(me, peer).wait_recv()
    agg = dot(adj_ref[:rows_dev, :], x_ref[...], TN) + dot(adj_ref[rows_dev:, :], halo_in[...].reshape(nodes * halo_pair, width), TN)
    agg_ref[...] = agg.astype(BF16)
    keep_kv(me)
    kv_to_cross[0].wait_recv()
    kv_relay[0].start()
    pre_ref[...] = dot(agg_ref[...], w_msg_ref[...]) + dot(x_ref[...], w_self_ref[...])
    for k in range(1, KV_PIECES):
        kv_to_cross[k].wait_recv()
        kv_relay[k].start()
    for copy in kv_to_mate:
        copy.wait_recv()
    keep_kv(mate)
    keep_kv(cross)
    for copy in kv_relay:
        copy.wait_recv()
    keep_kv(other)
    for copy in meta_copies + pos_to_cross + pos_to_mate + pos_relay + [halo_copy(peer, me) for peer in peers] + kv_to_cross + kv_to_mate + kv_relay:
        copy.wait_send()


def front(meta, x_feat, pos_enc, edge_src, edge_dst, edge_mask, w_q_t, w_kv, w_msg, w_self, nodes, halo_pair):
    rows, width = x_feat.shape
    pair = w_kv.shape[1]
    keys = nodes * rows
    table_rows = rows + nodes * halo_pair
    vmem = pl.BlockSpec(memory_space=pltpu.VMEM)
    dma = pltpu.SemaphoreType.DMA
    out = [((width, rows), BF16), ((keys, pair), BF16), ((pair, keys), BF16), ((rows, width), BF16), ((rows, width), BF16), ((rows, width), F32), ((table_rows, rows), BF16), ((1, nodes * halo_pair), jnp.int32), ((nodes, 512), jnp.int32)]
    return pl.pallas_call(
        front_kernel,
        out_shape=[jax.ShapeDtypeStruct(shape, dtype) for shape, dtype in out],
        in_specs=[vmem] * 10,
        out_specs=[vmem] * len(out),
        scratch_shapes=[
            pltpu.VMEM((nodes,) + meta.shape, jnp.int32),
            pltpu.VMEM((nodes, rows, width), BF16),
            pltpu.VMEM((rows, width), F32),
            pltpu.VMEM((table_rows, rows), F32),
            pltpu.VMEM((table_rows, rows // 2), F32),
            pltpu.VMEM((nodes, halo_pair, width), BF16),
            pltpu.VMEM((nodes, halo_pair, width), BF16),
            pltpu.VMEM((nodes, rows, pair), BF16),
            dma((3,)), dma((nodes,)), dma((3, POS_PIECES)), dma((3, POS_PIECES)), dma((nodes,)), dma((nodes,)), dma((3, KV_PIECES)), dma((3, KV_PIECES)),
        ],
        compiler_params=pltpu.CompilerParams(vmem_limit_bytes=52 << 20, collective_id=2, has_side_effects=True),
        cost_estimate=pl.CostEstimate(flops=24 << 30, bytes_accessed=20 << 20, transcendentals=0),
        name='front',
    )(meta, x_feat, pos_enc, edge_src, edge_dst, edge_mask, w_q_t, w_kv, w_msg, w_self)


def mask_tail(scores, chunk, key_chunk, part_rows, count_ref):
    start = chunk * key_chunk
    part = start // part_rows
    first = start - part * part_rows + key_chunk - TAIL
    row_ix = first + lax.broadcasted_iota(jnp.int32, (TAIL, scores.shape[1]), 0)
    tail = jnp.where(row_ix < count_ref[pl.ds(part, 1), :scores.shape[1]], scores[key_chunk - TAIL:, :], NEG_FILL)
    return jnp.concatenate([scores[:key_chunk - TAIL, :], tail], axis=0)


def attention_fwd_kernel(head_dim, q_block, key_chunk, part_rows, count_ref, q_ref, kv_ref, kvt_ref, out_ref, lse_ref, w_q, s_buf, stat):
    heads = q_ref.shape[0] // head_dim
    blocks = q_ref.shape[1] // q_block
    units = heads * blocks
    keys = kv_ref.shape[0]
    chunks = keys // key_chunk
    factor = head_dim ** -0.5 * LOG2E
    groups = key_chunk // 8

    def load_weights(unit):
        head, block = unit // blocks, lax.rem(unit, blocks)
        w_q[:head_dim, :] = q_ref[pl.ds(pl.multiple_of(head * head_dim, head_dim), head_dim), pl.ds(pl.multiple_of(block * q_block, q_block), q_block)]

    def score_stage(slot, chunk, run_max):
        rows = pl.ds(pl.multiple_of(chunk * key_chunk, key_chunk), key_chunk)
        scores = mask_tail(dot(kv_ref[rows, :], w_q[...]), chunk, key_chunk, part_rows, count_ref)
        s_buf[slot, rows, :] = scores
        return jnp.maximum(run_max, jnp.max(scores.reshape(groups, 8, q_block), axis=0))

    w_q[head_dim:, :] = jnp.zeros((w_q.shape[0] - head_dim, q_block), BF16)
    floor = jnp.full((8, q_block), -jnp.inf, F32)
    load_weights(0)
    stat[...] = lax.fori_loop(0, chunks, lambda chunk, run_max: score_stage(0, chunk, run_max), floor)

    def unit_body(unit, carry):
        slot = lax.rem(unit, 2)
        load_weights(jnp.minimum(unit + 1, units - 1))
        top = jnp.max(stat[...], axis=0, keepdims=True) * factor

        def chunk_body(chunk, state):
            run_max, run_sum, weighted = state
            cols = pl.ds(pl.multiple_of(chunk * key_chunk, key_chunk), key_chunk)
            prob = jnp.exp2(s_buf[slot, cols, :] * factor - top)
            run_sum = run_sum + jnp.sum(prob.reshape(groups, 8, q_block), axis=0)
            weighted = weighted + dot(kvt_ref[head_dim:2 * head_dim, cols], prob.astype(BF16))
            return score_stage(1 - slot, chunk, run_max), run_sum, weighted

        run_max, run_sum, weighted = lax.fori_loop(0, chunks, chunk_body, (floor, jnp.zeros((8, q_block), F32), jnp.zeros((head_dim, q_block), F32)))
        stat[...] = run_max
        total = jnp.sum(run_sum, axis=0, keepdims=True)
        head, block = unit // blocks, lax.rem(unit, blocks)
        cols = pl.ds(pl.multiple_of(block * q_block, q_block), q_block)
        out_ref[pl.ds(pl.multiple_of(head * head_dim, head_dim), head_dim), cols] = (weighted / total).astype(BF16)
        lse_ref[pl.ds(head, 1), cols] = top + jnp.log2(total)
        return carry

    lax.fori_loop(0, units, unit_body, 0)


def attention_forward(counts, q_t, kv, kv_t, head_dim, part_rows):
    width, rows = q_t.shape
    keys = kv.shape[0]
    heads = width // head_dim
    q_block, key_chunk = 256, 1024
    vmem = pl.BlockSpec(memory_space=pltpu.VMEM)
    return pl.pallas_call(
        functools.partial(attention_fwd_kernel, head_dim, q_block, key_chunk, part_rows),
        out_shape=[jax.ShapeDtypeStruct((width, rows), BF16), jax.ShapeDtypeStruct((heads, rows), F32)],
        in_specs=[vmem] * 4,
        out_specs=[vmem, vmem],
        scratch_shapes=[pltpu.VMEM((2 * head_dim, q_block), BF16), pltpu.VMEM((2, keys, q_block), F32), pltpu.VMEM((8, q_block), F32)],
        compiler_params=pltpu.CompilerParams(vmem_limit_bytes=48 << 20),
        cost_estimate=pl.CostEstimate(flops=4 * heads * rows * keys * head_dim, bytes_accessed=4 << 20, transcendentals=heads * rows * keys),
        name='attention_fwd',
    )(counts, q_t, kv, kv_t)


FINAL_STEPS, FINAL_LAG = 14, 2
FIRST_PIECES, HOLD_PIECES, HOLD_STEP = 2, 7, 68


def backward_kernel(head_dim, q_block, key_chunk, part_rows, pieces, count_ref, q_ref, do_ref, o_ref, lse_ref, kv_ref, kvt_ref, hid_ref, x_ref, agg_ref, dz_ref, dpre_ref, adj_ref, slot_ref, w_msg_ref, w_self_ref, w_qt_ref, w_kv_ref, up_ref, down_ref, *rest):
    arrays = len(pieces)
    dx_ref, rest = rest[0], rest[1:]
    sum_refs, rest = rest[:arrays], rest[arrays:]
    kv_sum_ref, rest = rest[0], rest[1:]
    w_q, w_do, lse_buf, delta_buf, p_buf, ds_buf, dq_acc, dq_all, dkv_acc, dkv_in, dkv_sum, local, own, from_mate, from_cross, kv_local, kv_own, kv_in, halo_out, halo_in, dx_acc, own_sem, send_sem, recv_sem, dkv_send, dkv_recv, kv_sem, kv_send, kv_recv, halo_send, halo_recv = rest
    heads = q_ref.shape[0] // head_dim
    blocks = q_ref.shape[1] // q_block
    units = heads * blocks
    chunks = kv_ref.shape[0] // key_chunk
    steps = units * chunks
    per_group = steps // 4
    halves = part_rows // key_chunk
    scale = head_dim ** -0.5
    factor = scale * LOG2E
    total = own.shape[0]
    first_small = total - 4
    half_rows, width = own.shape[1:]

    me, chip, side, mate, cross, other = neighbours()

    spots = [(array, j) for array in range(arrays) for j in range(pieces[array])]

    def block(refs, spot, half):
        array, j = spot
        ref = refs[array]
        if ref.shape[1] > width:
            return ref.at[pl.ds(half * half_rows, half_rows), pl.ds(j * width, width)]
        return ref.at[pl.ds((half * pieces[array] + j) * half_rows, half_rows), :]

    def source(index, half):
        if index < first_small:
            return block((up_ref, down_ref), spots[index], half)
        return local.at[index - first_small, pl.ds(half * half_rows, half_rows), :]

    def to_peer(src, dst, kind, index, peer):
        return remote(src, dst, send_sem.at[kind, index], recv_sem.at[kind, index], peer)

    def mate_copy(index):
        return to_peer(source(index, 1 - side), from_mate.at[index], 0, index, mate)

    def own_copy(index):
        return pltpu.make_async_copy(source(index, side), own.at[index], own_sem.at[0, index])

    def cross_copy(index):
        return to_peer(own.at[index], from_cross.at[index], 1, index, cross)

    def back_copy(index, half):
        return to_peer(from_mate.at[index], block(sum_refs, spots[index], half), 2, index, mate)

    def keep_copy(index):
        return pltpu.make_async_copy(from_mate.at[index], block(sum_refs, spots[index], side), own_sem.at[1, index])

    def chip_sum(index):
        to_peer(own.at[index], from_mate.at[index], 0, index, mate).wait_recv()
        pltpu.make_async_copy(own.at[index], own.at[index], own_sem.at[0, index]).wait()
        own[index] = own[index] + from_mate[index]

    def group_sum(index):
        cross_copy(index).wait_recv()
        from_mate[index] = own[index] + from_cross[index]

    def start_out(index):
        keep_copy(index).start()
        back_copy(index, side).start()

    dkv_copies = [remote(src, dkv_in.at[i], dkv_send.at[i], dkv_recv.at[i], peer) for i, (src, peer) in enumerate(((dkv_acc.at[0], mate), (dkv_sum, cross), (dkv_acc.at[2], mate)))]

    def kv_rows(half):
        return pl.ds(half * half_rows, half_rows)

    kv_to_mate = remote(kv_local.at[kv_rows(1 - side), :], kv_in.at[0], kv_send.at[0], kv_recv.at[0], mate)
    kv_to_cross = remote(kv_own.at[0], kv_in.at[1], kv_send.at[1], kv_recv.at[1], cross)
    kv_keep = pltpu.make_async_copy(kv_own.at[1], kv_sum_ref.at[kv_rows(side), :], kv_sem)

    def kv_back(half):
        return remote(kv_own.at[1], kv_sum_ref.at[kv_rows(half), :], kv_send.at[2], kv_recv.at[2], mate)

    halo_pair = halo_out.shape[1]

    def halo_copy(peer, owner):
        return remote(halo_out.at[peer], halo_in.at[owner], halo_send.at[peer], halo_recv.at[owner], peer)

    meet((mate, cross, other))
    for index in range(first_small):
        mate_copy(index).start()
        own_copy(index).start()

    def unit_spots(unit):
        head, place = unit // blocks, lax.rem(unit, blocks)
        return head, pl.ds(pl.multiple_of(head * head_dim, head_dim), head_dim), pl.ds(pl.multiple_of(place * q_block, q_block), q_block)

    def prepare(unit, carry):
        head, rows, cols = unit_spots(unit)
        delta_buf[unit] = jnp.sum(do_ref[rows, cols].astype(F32) * o_ref[rows, cols].astype(F32), axis=0, keepdims=True)
        lse_buf[unit] = lse_ref[pl.ds(head, 1), cols]
        dq_acc[unit] = jnp.zeros((head_dim, q_block), F32)
        return carry

    lax.fori_loop(0, units, prepare, 0)
    for index in range(FIRST_PIECES):
        chip_sum(index)
    for slot in range(2):
        w_q[slot, head_dim:, :] = jnp.zeros((head_dim, q_block), BF16)
        w_do[slot, :head_dim, :] = jnp.zeros((head_dim, q_block), BF16)
    dkv_acc[...] = jnp.zeros_like(dkv_acc)
    for index in range(FIRST_PIECES):
        cross_copy(index).start()

    d_agg = dot(dpre_ref[...], w_msg_ref[...], NT).astype(BF16)
    halo_out[...] = dot(adj_ref[part_rows:, :], d_agg).astype(BF16).reshape(halo_out.shape)
    dx_acc[...] = 2.0 * dz_ref[...].astype(F32) + dot(dpre_ref[...], w_self_ref[...], NT)
    dx_acc[...] += dot(adj_ref[:part_rows, :], d_agg)
    for peer in (mate, cross, other):
        halo_copy(peer, me).start()
    halo_in[me] = halo_out[me]
    local[0] = dot(x_ref[...], dpre_ref[...], TN)
    local[1] = dot(agg_ref[...], dpre_ref[...], TN)
    local[2] = dot(o_ref[...], dz_ref[...])

    def place_of(step):
        group = step // per_group
        chunk = step // units
        owner = lax.rem(chip + 1 - group // 2, 2) * 2 + lax.rem(side + 1 - lax.rem(group, 2), 2)
        offset = lax.rem(chunk, halves) * key_chunk
        rows = pl.ds(pl.multiple_of(owner * part_rows + offset, key_chunk), key_chunk)
        return group, owner, offset, rows, lax.rem(step, units), lax.rem(step, 2)

    def first_stage(step):
        group, owner, offset, rows, unit, slot = place_of(step)
        head, unit_rows, cols = unit_spots(unit)
        w_q[slot, :head_dim, :] = q_ref[unit_rows, cols]
        w_do[slot, head_dim:, :] = do_ref[unit_rows, cols]
        kv = kv_ref[rows, :]
        scores = dot(kv, w_q[slot])
        row_ix = offset + key_chunk - TAIL + lax.broadcasted_iota(jnp.int32, (TAIL, q_block), 0)
        tail = jnp.where(row_ix < count_ref[pl.ds(owner, 1), :q_block], scores[key_chunk - TAIL:, :], NEG_FILL)
        scores = jnp.concatenate([scores[:key_chunk - TAIL, :], tail], axis=0)
        prob = jnp.exp2(scores * factor - lse_buf[unit])
        p_buf[slot] = prob.astype(BF16)
        ds_buf[slot] = (prob * (dot(kv, w_do[slot]) - delta_buf[unit])).astype(BF16)

    def second_stage(step):
        group, owner, offset, rows, unit, slot = place_of(step)
        d_scores = ds_buf[slot]
        spot = pl.ds(pl.multiple_of(offset, key_chunk), key_chunk)
        dkv_acc[group, spot, :] += dot(d_scores, w_q[slot], NT) + dot(p_buf[slot], w_do[slot], NT)
        dq_acc[unit] += dot(kvt_ref[:head_dim, rows], d_scores)

    def exchange(step):
        early = jnp.where(step < 4 * (HOLD_PIECES - FIRST_PIECES), 1, 0)
        late = jnp.where(jnp.logical_and(step >= HOLD_STEP, step < HOLD_STEP + 4 * (first_small + 3 - HOLD_PIECES)), 1, 0)
        turn = step // 4 + FIRST_PIECES - late * (HOLD_STEP // 4 + FIRST_PIECES - HOLD_PIECES)
        phase = lax.rem(step, 4)

        @pl.when(jnp.logical_and(early + late == 1, phase == 1))
        def sum_chip():
            chip_sum(turn)

        @pl.when(jnp.logical_and(early + late == 1, phase == 2))
        def send_cross():
            cross_copy(turn).start()

        lap, beat = step // FINAL_STEPS - FINAL_LAG, lax.rem(step, FINAL_STEPS)

        @pl.when(jnp.logical_and(lap >= 0, beat == 0))
        def sum_group():
            group_sum(lap)

        @pl.when(jnp.logical_and(lap >= 0, beat == 1))
        def send_back():
            for k in range(done):
                @pl.when(lap == k)
                def start_piece(k=k):
                    start_out(k)

        @pl.when(step == 3)
        def small_pieces():
            for index in range(first_small, total - 1):
                mate_copy(index).start()
                own_copy(index).start()

        @pl.when(step == per_group + 1)
        def first_group():
            dkv_copies[0].start()

        @pl.when(step == 2 * per_group + 1)
        def second_group():
            dkv_copies[0].wait_recv()
            dkv_sum[...] = dkv_acc[1] + dkv_in[0]

        @pl.when(step == 2 * per_group + 2)
        def send_second():
            dkv_copies[1].start()

        @pl.when(step == 3 * per_group + 1)
        def third_group():
            dkv_copies[2].start()

    done = (steps - 1) // FINAL_STEPS - FINAL_LAG + 1
    assert (steps - 1) % FINAL_STEPS >= 1 and 0 < done <= first_small and HOLD_STEP > 2 * per_group + 2 and HOLD_STEP % 4 == 0

    first_stage(0)

    def body(step, carry):
        exchange(step)
        second_stage(step - 1)
        first_stage(step)
        return carry

    lax.fori_loop(1, steps, body, 0)
    second_stage(steps - 1)

    def gather_dq(unit, carry):
        head, rows, cols = unit_spots(unit)
        dq_all[rows, cols] = (dq_acc[unit] * scale).astype(BF16)
        return carry

    lax.fori_loop(0, units, gather_dq, 0)
    last = total - 1
    local[3] = dot(dq_all[...], hid_ref[...]).T
    dkv_copies[2].wait_recv()
    dkv_copies[1].wait_recv()
    dkv = dkv_acc[3] + dkv_in[2] + dkv_in[1]
    lane = lax.broadcasted_iota(jnp.int32, dkv.shape, 1)
    dkv = jnp.where(lane < head_dim, dkv * scale, dkv).astype(BF16)
    mate_copy(last).start()
    own_copy(last).start()
    kv_local[...] = dot(hid_ref[...], dkv, TN)
    dx_acc[...] += dot(dkv, w_kv_ref[...], NT)
    kv_to_mate.start()
    chip_sum(last)
    kv_to_mate.wait_recv()
    kv_own[0] = kv_local[kv_rows(side), :] + kv_in[0]
    for peer in (mate, cross, other):
        halo_copy(me, peer).wait_recv()
    slot_hot = jnp.where(lax.broadcasted_iota(jnp.int32, (part_rows, 4 * halo_pair), 0) == slot_ref[...], 1.0, 0.0).astype(BF16)
    dx_acc[...] += dot(slot_hot, halo_in[...].reshape(4 * halo_pair, width))
    cross_copy(last).start()
    kv_to_cross.start()
    dx_ref[...] = (dx_acc[...] + dot(dq_all[...], w_qt_ref[...], TN)).astype(BF16)
    for index in range(done, total):
        group_sum(index)
        if index > done:
            start_out(index - 1)
    kv_to_cross.wait_recv()
    kv_own[1] = kv_own[0] + kv_in[1]
    start_out(last)
    kv_keep.start()
    kv_back(side).start()
    for copy in dkv_copies + [kv_to_mate, kv_to_cross, kv_back(side)] + [halo_copy(peer, me) for peer in (mate, cross, other)]:
        copy.wait_send()
    kv_keep.wait()
    kv_back(1 - side).wait_recv()
    for index in range(total):
        mate_copy(index).wait_send()
        cross_copy(index).wait_send()
        keep_copy(index).wait()
        back_copy(index, side).wait_send()
        back_copy(index, 1 - side).wait_recv()


def backward(counts, q_t, do_t, o_t, lse, kv, kv_t, hidden_in, x_feat, agg_msg, d_z, d_pre, adjacency_t, halo_got, w_msg, w_self, w_q_t, w_kv, grad_up, grad_down):
    width, rows = q_t.shape
    keys = kv.shape[0]
    head_dim = kv.shape[1] // 2
    heads = width // head_dim
    nodes = keys // rows
    q_block, key_chunk = 512, 512
    units = heads * rows // q_block
    piece_rows = width // 2
    shapes = [grad_up.shape, grad_down.shape] + [(width, width)] * 4
    pieces = [r * c // (2 * piece_rows * width) for r, c in shapes]
    total = sum(pieces)
    halo_pair = halo_got.shape[1] // nodes
    vmem = pl.BlockSpec(memory_space=pltpu.VMEM)
    anywhere = pl.BlockSpec(memory_space=pl.ANY)
    dma = pltpu.SemaphoreType.DMA
    return pl.pallas_call(
        functools.partial(backward_kernel, head_dim, q_block, key_chunk, rows, pieces),
        out_shape=[jax.ShapeDtypeStruct((rows, width), BF16)] + [jax.ShapeDtypeStruct(shape, F32) for shape in shapes] + [jax.ShapeDtypeStruct((width, 2 * head_dim), F32)],
        in_specs=[vmem] * 18 + [anywhere] * 2,
        out_specs=[vmem] + [anywhere] * 7,
        scratch_shapes=[
            pltpu.VMEM((2, 2 * head_dim, q_block), BF16),
            pltpu.VMEM((2, 2 * head_dim, q_block), BF16),
            pltpu.VMEM((units, 1, q_block), F32),
            pltpu.VMEM((units, 1, q_block), F32),
            pltpu.VMEM((2, key_chunk, q_block), BF16),
            pltpu.VMEM((2, key_chunk, q_block), BF16),
            pltpu.VMEM((units, head_dim, q_block), F32),
            pltpu.VMEM((width, rows), BF16),
            pltpu.VMEM((4, rows, 2 * head_dim), F32),
            pltpu.VMEM((3, rows, 2 * head_dim), F32),
            pltpu.VMEM((rows, 2 * head_dim), F32),
            pltpu.VMEM((4, width, width), F32),
            pltpu.VMEM((total, piece_rows, width), F32),
            pltpu.VMEM((total, piece_rows, width), F32),
            pltpu.VMEM((total, piece_rows, width), F32),
            pltpu.VMEM((width, 2 * head_dim), F32),
            pltpu.VMEM((2, piece_rows, 2 * head_dim), F32),
            pltpu.VMEM((2, piece_rows, 2 * head_dim), F32),
            pltpu.VMEM((nodes, halo_pair, width), BF16),
            pltpu.VMEM((nodes, halo_pair, width), BF16),
            pltpu.VMEM((rows, width), F32),
            dma((2, total)), dma((3, total)), dma((3, total)), dma((3,)), dma((3,)), dma, dma((3,)), dma((3,)), dma((nodes,)), dma((nodes,)),
        ],
        compiler_params=pltpu.CompilerParams(vmem_limit_bytes=62 << 20, collective_id=1, has_side_effects=True),
        cost_estimate=pl.CostEstimate(flops=10 * heads * rows * keys * head_dim, bytes_accessed=40 << 20, transcendentals=heads * rows * keys),
        name='backward',
    )(counts, q_t, do_t, o_t, lse, kv, kv_t, hidden_in, x_feat, agg_msg, d_z, d_pre, adjacency_t, halo_got, w_msg, w_self, w_q_t, w_kv, grad_up, grad_down)


def solution(mesh):
    nodes = mesh.shape['nodes']
    row_spec = P(('graphs', 'nodes'), None)
    flat_spec = P(('graphs', 'nodes'))
    halo_spec = P(('graphs', 'nodes'), None, None)
    grad_spec = P('graphs', None)

    def device_step(x_feat, valid, halo_slot, edge_src, edge_dst, edge_mask, bal_perm, pos_enc, y_cot, w_msg, w_self, w_q, w_k, w_v, w_o, w_up, w_down):
        rows_dev, width = x_feat.shape
        head_dim = w_k.shape[1]
        me = lax.axis_index('nodes')
        halo_pair = halo_slot.shape[2]

        lane_owner = jnp.arange(rows_dev)[None, :] // halo_pair
        wanted = jnp.where(lane_owner == me, jnp.tile(halo_slot.reshape(nodes, halo_pair), (1, rows_dev // halo_pair)), -1)
        meta = jnp.concatenate([bal_perm[None, :], valid[None, :], wanted, jnp.zeros((6 - nodes, rows_dev), jnp.int32)], axis=0)
        w_kv = jnp.concatenate([w_k, w_v], axis=1)
        w_q_t = w_q.T
        q_t, kv_all, kv_all_t, hidden_in, agg_msg, pre_act, adjacency_t, slots, counts = front(meta, x_feat, pos_enc, edge_src, edge_dst, edge_mask, w_q_t, w_kv, w_msg, w_self, nodes, halo_pair)
        mixed_t, lse = attention_forward(counts, q_t, kv_all, kv_all_t, head_dim, rows_dev)
        u_part = dot(mixed_t, w_o, TN).astype(BF16).astype(F32)
        x_wide = x_feat.astype(F32)
        z_mid = (x_wide + jax.nn.relu(pre_act) + x_wide + u_part).astype(BF16)
        h_pre = dot(z_mid, w_up)
        hidden, gelu_pull = jax.vjp(jax.nn.gelu, h_pre)
        hidden = hidden.astype(BF16)
        keep_row = valid[:, None] > 0
        y_out = jnp.where(keep_row, z_mid.astype(F32) + dot(hidden, w_down), 0.0).astype(BF16)

        g_out = jnp.where(keep_row, y_cot, jnp.zeros_like(y_cot))
        grad_down = dot(hidden, g_out, TN)
        d_hidden = dot(g_out, w_down, NT).astype(BF16)
        d_hpre = gelu_pull(d_hidden.astype(F32))[0].astype(BF16)
        grad_up = dot(z_mid, d_hpre, TN)
        d_z = (g_out.astype(F32) + dot(d_hpre, w_up, NT)).astype(BF16)
        d_pre = jnp.where(pre_act > 0, d_z, jnp.zeros_like(d_z))
        do_t = dot(w_o, d_z, NT).astype(BF16)
        dx_feat, grad_up, grad_down, grad_self, grad_msg, grad_o, grad_q, grad_kv = backward(counts, q_t, do_t, mixed_t, lse, kv_all, kv_all_t, hidden_in, x_feat, agg_msg, d_z, d_pre, adjacency_t, slots, w_msg, w_self, w_q_t, w_kv, grad_up, grad_down)
        grad_k, grad_v = grad_kv[:, :head_dim], grad_kv[:, head_dim:]
        return (y_out, dx_feat, grad_msg, grad_self, grad_q, grad_k, grad_v, grad_o, grad_up, grad_down)

    return jax.shard_map(device_step, mesh=mesh, in_specs=(row_spec, flat_spec, halo_spec, row_spec, row_spec, row_spec, flat_spec, row_spec, row_spec) + (P(),) * 8, out_specs=(row_spec, row_spec) + (grad_spec,) * 8, check_vma=False)
```

```python
import functools
import math

import jax
import jax.numpy as jnp
from jax import lax
from jax.experimental import pallas as pl
from jax.experimental.pallas import tpu as pltpu
from jax.sharding import PartitionSpec as P

NEG_FILL = -1e30
LOG2E = math.log2(math.e)
TAIL = 32
F32 = jnp.float32
BF16 = jnp.bfloat16
NN = (((1,), (0,)), ((), ()))
NT = (((1,), (1,)), ((), ()))
TN = (((0,), (0,)), ((), ()))
TT = (((0,), (1,)), ((), ()))


def dot(a, b, dims=NN):
    return lax.dot_general(a, b, dims, preferred_element_type=F32)


def remote(src, dst, send, recv, peer):
    return pltpu.make_async_remote_copy(src_ref=src, dst_ref=dst, send_sem=send, recv_sem=recv, device_id={'nodes': peer}, device_id_type=pl.DeviceIdType.MESH)


def neighbours():
    me = lax.axis_index('nodes')
    chip, side = me // 2, lax.rem(me, 2)
    return me, chip, side, chip * 2 + 1 - side, (1 - chip) * 2 + side, (1 - chip) * 2 + 1 - side


def meet(peers):
    barrier = pltpu.get_barrier_semaphore()
    for peer in peers:
        pl.semaphore_signal(barrier, inc=1, device_id={'nodes': peer}, device_id_type=pl.DeviceIdType.MESH)
    pl.semaphore_wait(barrier, len(peers))


CHUNKS, EDGE_STEP, POS_PIECES, KV_PIECES = 4, 512, 4, 2


def front_kernel(meta_ref, x_ref, pos_ref, src_ref, dst_ref, on_ref, w_qt_ref, w_kt_ref, w_vt_ref, w_msg_ref, w_self_ref, q_ref, kv_ref, kvt_ref, hid_ref, agg_ref, pre_ref, adj_ref, slot_ref, count_ref, meta_all, pos_all, pos_acc, counts_acc, edge_acc, halo_out, halo_in, kv_all, meta_send, meta_recv, pos_send, pos_recv, halo_send, halo_recv, kv_send, kv_recv):
    rows_dev, width = x_ref.shape
    table_rows = adj_ref.shape[0]
    half = rows_dev // 2
    nodes = meta_all.shape[0]
    halo_pair = halo_in.shape[1]
    me, chip, side, mate, cross, other = neighbours()
    peers = (mate, cross, other)
    meet(peers)

    meta_copies = [remote(meta_ref, meta_all.at[me], meta_send.at[i], meta_recv.at[me], peer) for i, peer in enumerate(peers)]
    for copy in meta_copies:
        copy.start()
    piece = rows_dev // POS_PIECES

    def pos_rows(index):
        return pl.ds(index * piece, piece)

    pos_to_cross = [remote(pos_ref.at[pos_rows(k), :], pos_all.at[me, pos_rows(k), :], pos_send.at[0, k], pos_recv.at[0, k], cross) for k in range(POS_PIECES)]
    pos_to_mate = [remote(pos_ref.at[pos_rows(k), :], pos_all.at[me, pos_rows(k), :], pos_send.at[1, k], pos_recv.at[1, k], mate) for k in range(POS_PIECES)]
    pos_relay = [remote(pos_all.at[cross, pos_rows(k), :], pos_all.at[cross, pos_rows(k), :], pos_send.at[2, k], pos_recv.at[2, k], mate) for k in range(POS_PIECES)]
    for copy in pos_to_cross + pos_to_mate:
        copy.start()
    meta_all[me] = meta_ref[...]

    def relay_pos(k):
        pos_to_cross[k].wait_recv()
        pos_relay[k].start()

    def place_pos(owner, source, first):
        perm = meta_all[owner, 0:1, :] - me * rows_dev
        size = 256

        def body(index, carry):
            rows = pl.ds(pl.multiple_of(index * size, size), size)
            hot = jnp.where(index * size + lax.broadcasted_iota(jnp.int32, (size, rows_dev), 0) == perm, 1.0, 0.0).astype(BF16)
            part = dot(hot, source[...])
            pos_acc[rows, :] = part if first else pos_acc[rows, :] + part
            return carry

        lax.fori_loop(0, rows_dev // size, body, 0)

    edges = src_ref.shape[1]
    steps = edges // (CHUNKS * EDGE_STEP)
    assert CHUNKS * EDGE_STEP * steps == edges and EDGE_STEP * steps < 4096

    def edge_block(index):
        cols = pl.ds(pl.multiple_of(index * EDGE_STEP, EDGE_STEP), EDGE_STEP)
        src, dst, on = src_ref[:, cols], dst_ref[:, cols], on_ref[:, cols]
        upper = dst >= half
        place = jnp.where(upper, dst - half, dst)
        weight = jnp.where(on > 0, jnp.where(upper, 4096.0, 1.0), 0.0)
        src_hot = jnp.where(lax.broadcasted_iota(jnp.int32, (table_rows, EDGE_STEP), 0) == src, 1.0, 0.0).astype(BF16)
        dst_hot = jnp.where(lax.broadcasted_iota(jnp.int32, (half, EDGE_STEP), 0) == place, weight, 0.0).astype(BF16)
        return dot(src_hot, dst_hot, NT)

    def count_chunk(chunk):
        edge_acc[...] = jnp.zeros_like(edge_acc)

        def body(step, carry):
            edge_acc[...] += edge_block(chunk * steps + step)
            return carry

        lax.fori_loop(0, steps, body, 0)
        total = edge_acc[...]
        high = jnp.floor(total * (1.0 / 4096.0))
        low = total - high * 4096.0
        if chunk == 0:
            counts_acc[:, :half] = low
            counts_acc[:, half:] = high
        elif chunk < CHUNKS - 1:
            counts_acc[:, :half] += low
            counts_acc[:, half:] += high
        else:
            adj_ref[:, :half] = (counts_acc[:, :half] + low).astype(BF16)
            adj_ref[:, half:] = (counts_acc[:, half:] + high).astype(BF16)

    def halo_copy(peer, owner):
        return remote(halo_out.at[peer], halo_in.at[owner], halo_send.at[peer], halo_recv.at[owner], peer)

    count_chunk(0)
    for peer in peers:
        remote(meta_ref, meta_all.at[peer], meta_send.at[0], meta_recv.at[peer], peer).wait_recv()
    tables = meta_all[0, :, 0:nodes * halo_pair]
    for node in range(1, nodes):
        tables = jnp.maximum(tables, meta_all[node, :, 0:nodes * halo_pair])
    tables = jnp.where(lax.broadcasted_iota(jnp.int32, tables.shape, 0) == 2 + me, tables, -1)
    slots = jnp.max(tables.astype(F32), axis=0, keepdims=True).astype(jnp.int32)
    slot_ref[...] = slots
    slot_hot = jnp.where(lax.broadcasted_iota(jnp.int32, (rows_dev, nodes * halo_pair), 0) == slots, 1.0, 0.0).astype(BF16)
    halo_out[...] = dot(slot_hot, x_ref[...], TN).astype(BF16).reshape(halo_out.shape)
    relay_pos(0)
    place_pos(me, pos_ref, True)
    for peer in peers:
        halo_copy(peer, me).start()
    halo_in[me] = halo_out[me]
    for node in range(nodes):
        held = jnp.sum(meta_all[node, 1:2, :].astype(F32), axis=1, keepdims=True).astype(jnp.int32)
        count_ref[node:node + 1, :] = jnp.broadcast_to(held, (1, count_ref.shape[1]))
    count_chunk(1)
    relay_pos(1)
    for copy in pos_to_mate:
        copy.wait_recv()
    place_pos(mate, pos_all.at[mate], False)
    count_chunk(2)
    relay_pos(2)
    count_chunk(3)
    relay_pos(3)
    place_pos(cross, pos_all.at[cross], False)
    for copy in pos_relay:
        copy.wait_recv()
    place_pos(other, pos_all.at[other], False)

    hid_ref[...] = (x_ref[...].astype(F32) + pos_acc[...]).astype(BF16)
    kv_all[me] = dot(hid_ref[...], jnp.concatenate([w_kt_ref[...], w_vt_ref[...]], axis=0), NT).astype(BF16)
    q_ref[...] = dot(w_qt_ref[...], hid_ref[...], NT).astype(BF16)
    kv_piece = rows_dev // KV_PIECES

    def kv_copy(owner, k, kind, peer):
        rows = pl.ds(k * kv_piece, kv_piece)
        return remote(kv_all.at[owner, rows, :], kv_all.at[owner, rows, :], kv_send.at[kind, k], kv_recv.at[kind, k], peer)

    kv_to_cross = [kv_copy(me, k, 0, cross) for k in range(KV_PIECES)]
    kv_to_mate = [kv_copy(me, k, 1, mate) for k in range(KV_PIECES)]
    kv_relay = [kv_copy(cross, k, 2, mate) for k in range(KV_PIECES)]
    for copy in kv_to_cross + kv_to_mate:
        copy.start()
    size = kv_all.shape[2]
    eye = jnp.where(lax.broadcasted_iota(jnp.int32, (size, size), 0) == lax.broadcasted_iota(jnp.int32, (size, size), 1), 1.0, 0.0).astype(BF16)

    def keep_kv(owner):
        rows = pl.ds(pl.multiple_of(owner * rows_dev, rows_dev), rows_dev)
        kv_ref[rows, :] = kv_all[owner]
        kvt_ref[:, rows] = dot(eye, kv_all[owner], NT).astype(BF16)

    for peer in peers:
        halo_copy(me, peer).wait_recv()
    agg = dot(adj_ref[:rows_dev, :], x_ref[...], TN) + dot(adj_ref[rows_dev:, :], halo_in[...].reshape(nodes * halo_pair, width), TN)
    agg_ref[...] = agg.astype(BF16)
    keep_kv(me)
    kv_to_cross[0].wait_recv()
    kv_relay[0].start()
    pre_ref[...] = dot(agg_ref[...], w_msg_ref[...]) + dot(x_ref[...], w_self_ref[...])
    for k in range(1, KV_PIECES):
        kv_to_cross[k].wait_recv()
        kv_relay[k].start()
    for copy in kv_to_mate:
        copy.wait_recv()
    keep_kv(mate)
    keep_kv(cross)
    for copy in kv_relay:
        copy.wait_recv()
    keep_kv(other)
    for copy in meta_copies + pos_to_cross + pos_to_mate + pos_relay + [halo_copy(peer, me) for peer in peers] + kv_to_cross + kv_to_mate + kv_relay:
        copy.wait_send()


def front(meta, x_feat, pos_enc, edge_src, edge_dst, edge_mask, w_q_t, w_k_t, w_v_t, w_msg, w_self, nodes, halo_pair):
    rows, width = x_feat.shape
    pair = 2 * w_k_t.shape[0]
    keys = nodes * rows
    table_rows = rows + nodes * halo_pair
    vmem = pl.BlockSpec(memory_space=pltpu.VMEM)
    dma = pltpu.SemaphoreType.DMA
    out = [((width, rows), BF16), ((keys, pair), BF16), ((pair, keys), BF16), ((rows, width), BF16), ((rows, width), BF16), ((rows, width), F32), ((table_rows, rows), BF16), ((1, nodes * halo_pair), jnp.int32), ((nodes, 512), jnp.int32)]
    return pl.pallas_call(
        front_kernel,
        out_shape=[jax.ShapeDtypeStruct(shape, dtype) for shape, dtype in out],
        in_specs=[vmem] * 11,
        out_specs=[vmem] * len(out),
        scratch_shapes=[
            pltpu.VMEM((nodes,) + meta.shape, jnp.int32),
            pltpu.VMEM((nodes, rows, width), BF16),
            pltpu.VMEM((rows, width), F32),
            pltpu.VMEM((table_rows, rows), F32),
            pltpu.VMEM((table_rows, rows // 2), F32),
            pltpu.VMEM((nodes, halo_pair, width), BF16),
            pltpu.VMEM((nodes, halo_pair, width), BF16),
            pltpu.VMEM((nodes, rows, pair), BF16),
            dma((3,)), dma((nodes,)), dma((3, POS_PIECES)), dma((3, POS_PIECES)), dma((nodes,)), dma((nodes,)), dma((3, KV_PIECES)), dma((3, KV_PIECES)),
        ],
        compiler_params=pltpu.CompilerParams(vmem_limit_bytes=52 << 20, collective_id=2, has_side_effects=True),
        cost_estimate=pl.CostEstimate(flops=24 << 30, bytes_accessed=20 << 20, transcendentals=0),
        name='front',
    )(meta, x_feat, pos_enc, edge_src, edge_dst, edge_mask, w_q_t, w_k_t, w_v_t, w_msg, w_self)


def mask_tail(scores, chunk, key_chunk, part_rows, count_ref):
    start = chunk * key_chunk
    part = start // part_rows
    first = start - part * part_rows + key_chunk - TAIL
    row_ix = first + lax.broadcasted_iota(jnp.int32, (TAIL, scores.shape[1]), 0)
    tail = jnp.where(row_ix < count_ref[pl.ds(part, 1), :scores.shape[1]], scores[key_chunk - TAIL:, :], NEG_FILL)
    return jnp.concatenate([scores[:key_chunk - TAIL, :], tail], axis=0)


def attention_fwd_kernel(head_dim, q_block, key_chunk, part_rows, count_ref, q_ref, kv_ref, kvt_ref, out_ref, lse_ref, w_q, s_buf, stat):
    heads = q_ref.shape[0] // head_dim
    blocks = q_ref.shape[1] // q_block
    units = heads * blocks
    keys = kv_ref.shape[0]
    chunks = keys // key_chunk
    factor = head_dim ** -0.5 * LOG2E
    groups = key_chunk // 8

    def load_weights(unit):
        head, block = unit // blocks, lax.rem(unit, blocks)
        w_q[:head_dim, :] = q_ref[pl.ds(pl.multiple_of(head * head_dim, head_dim), head_dim), pl.ds(pl.multiple_of(block * q_block, q_block), q_block)]

    def score_stage(slot, chunk, run_max):
        rows = pl.ds(pl.multiple_of(chunk * key_chunk, key_chunk), key_chunk)
        scores = mask_tail(dot(kv_ref[rows, :], w_q[...]), chunk, key_chunk, part_rows, count_ref)
        s_buf[slot, rows, :] = scores
        return jnp.maximum(run_max, jnp.max(scores.reshape(groups, 8, q_block), axis=0))

    w_q[head_dim:, :] = jnp.zeros((w_q.shape[0] - head_dim, q_block), BF16)
    floor = jnp.full((8, q_block), -jnp.inf, F32)
    load_weights(0)
    stat[...] = lax.fori_loop(0, chunks, lambda chunk, run_max: score_stage(0, chunk, run_max), floor)

    def unit_body(unit, carry):
        slot = lax.rem(unit, 2)
        load_weights(jnp.minimum(unit + 1, units - 1))
        top = jnp.max(stat[...], axis=0, keepdims=True) * factor

        def chunk_body(chunk, state):
            run_max, run_sum, weighted = state
            cols = pl.ds(pl.multiple_of(chunk * key_chunk, key_chunk), key_chunk)
            prob = jnp.exp2(s_buf[slot, cols, :] * factor - top)
            run_sum = run_sum + jnp.sum(prob.reshape(groups, 8, q_block), axis=0)
            weighted = weighted + dot(kvt_ref[head_dim:2 * head_dim, cols], prob.astype(BF16))
            return score_stage(1 - slot, chunk, run_max), run_sum, weighted

        run_max, run_sum, weighted = lax.fori_loop(0, chunks, chunk_body, (floor, jnp.zeros((8, q_block), F32), jnp.zeros((head_dim, q_block), F32)))
        stat[...] = run_max
        total = jnp.sum(run_sum, axis=0, keepdims=True)
        head, block = unit // blocks, lax.rem(unit, blocks)
        cols = pl.ds(pl.multiple_of(block * q_block, q_block), q_block)
        out_ref[pl.ds(pl.multiple_of(head * head_dim, head_dim), head_dim), cols] = (weighted / total).astype(BF16)
        lse_ref[pl.ds(head, 1), cols] = top + jnp.log2(total)
        return carry

    lax.fori_loop(0, units, unit_body, 0)


def attention_forward(counts, q_t, kv, kv_t, head_dim, part_rows):
    width, rows = q_t.shape
    keys = kv.shape[0]
    heads = width // head_dim
    q_block, key_chunk = 256, 1024
    vmem = pl.BlockSpec(memory_space=pltpu.VMEM)
    return pl.pallas_call(
        functools.partial(attention_fwd_kernel, head_dim, q_block, key_chunk, part_rows),
        out_shape=[jax.ShapeDtypeStruct((width, rows), BF16), jax.ShapeDtypeStruct((heads, rows), F32)],
        in_specs=[vmem] * 4,
        out_specs=[vmem, vmem],
        scratch_shapes=[pltpu.VMEM((2 * head_dim, q_block), BF16), pltpu.VMEM((2, keys, q_block), F32), pltpu.VMEM((8, q_block), F32)],
        compiler_params=pltpu.CompilerParams(vmem_limit_bytes=48 << 20),
        cost_estimate=pl.CostEstimate(flops=4 * heads * rows * keys * head_dim, bytes_accessed=4 << 20, transcendentals=heads * rows * keys),
        name='attention_fwd',
    )(counts, q_t, kv, kv_t)


FINAL_STEPS, FINAL_LAG = 14, 1
HOLD_STEP = 68
ROW_BLOCK = 256
GELU_A, GELU_B = math.sqrt(2.0 / math.pi), 0.044715


def backward_kernel(head_dim, q_block, key_chunk, part_rows, count_ref, q_ref, o_ref, lse_ref, kv_ref, kvt_ref, hid_ref, x_ref, agg_ref, adj_ref, slot_ref, w_msg_ref, w_self_ref, w_qt_ref, w_kt_ref, w_vt_ref, w_o_ref, pre_hbm, cot_hbm, up_hbm, down_hbm, *rest):
    y_ref, dx_ref, rest = rest[0], rest[1], rest[2:]
    sum_refs, kv_sum_ref, rest = rest[:6], rest[6], rest[7:]
    do_buf, dz_buf, dpre_buf, dx_acc, dkv_in, dkv_sum, local, from_mate, from_cross, kv_local, kv_own, kv_in, halo_out, halo_in, load_sem, keep_sem, send_sem, recv_sem, dkv_send, dkv_recv, kv_sem, kv_send, kv_recv, halo_send, halo_recv = rest
    heads = q_ref.shape[0] // head_dim
    blocks = q_ref.shape[1] // q_block
    units = heads * blocks
    chunks = kv_ref.shape[0] // key_chunk
    steps = units * chunks
    per_group = steps // 4
    halves = part_rows // key_chunk
    scale = head_dim ** -0.5
    factor = scale * LOG2E
    total, width = local.shape[0], local.shape[1]
    half_rows = width // 2
    ffn_chunks = up_hbm.shape[1] // width
    first_small = 2 * ffn_chunks
    me, chip, side, mate, cross, other = neighbours()

    def block(index, half):
        if index >= first_small:
            return sum_refs[2 + index - first_small].at[pl.ds(half * half_rows, half_rows), :]
        chunk = index // 2
        if index % 2 == 0:
            return sum_refs[1].at[pl.ds(chunk * width + half * half_rows, half_rows), :]
        return sum_refs[0].at[pl.ds(half * half_rows, half_rows), pl.ds(chunk * width, width)]

    def part(index, half):
        return local.at[index, pl.ds(half * half_rows, half_rows), :]

    def to_peer(src, dst, kind, index, peer):
        return remote(src, dst, send_sem.at[kind, index], recv_sem.at[kind, index], peer)

    def mate_copy(index):
        return to_peer(part(index, 1 - side), from_mate.at[index], 0, index, mate)

    def cross_copy(index):
        return to_peer(part(index, side), from_cross.at[index], 1, index, cross)

    def back_copy(index, half):
        return to_peer(from_mate.at[index], block(index, half), 2, index, mate)

    def keep_copy(index):
        return pltpu.make_async_copy(from_mate.at[index], block(index, side), keep_sem.at[index])

    my_half = pl.ds(pl.multiple_of(side * half_rows, half_rows), half_rows)

    def chip_sum(index):
        mate_copy(index).wait_recv()
        local[index, my_half, :] = local[index, my_half, :] + from_mate[index]

    def group_sum(index):
        cross_copy(index).wait_recv()
        from_mate[index] = local[index, my_half, :] + from_cross[index]

    def start_out(index):
        keep_copy(index).start()
        back_copy(index, side).start()

    kv_half = kv_local.shape[0] // 2

    def kv_rows(half):
        return pl.ds(half * kv_half, kv_half)

    kv_to_mate = remote(kv_local.at[kv_rows(1 - side), :], kv_in.at[0], kv_send.at[0], kv_recv.at[0], mate)
    kv_to_cross = remote(kv_own.at[0], kv_in.at[1], kv_send.at[1], kv_recv.at[1], cross)
    kv_keep = pltpu.make_async_copy(kv_own.at[1], kv_sum_ref.at[kv_rows(side), :], kv_sem)

    def kv_back(half):
        return remote(kv_own.at[1], kv_sum_ref.at[kv_rows(half), :], kv_send.at[2], kv_recv.at[2], mate)

    halo_pair = halo_out.shape[1]

    def halo_copy(peer, owner):
        return remote(halo_out.at[peer], halo_in.at[owner], halo_send.at[peer], halo_recv.at[owner], peer)

    def ffn_phase(w_up, w_down, g_buf, z_buf, y_acc, act, d_act):
        loads = [pltpu.make_async_copy(src, dst, load_sem.at[i]) for i, (src, dst) in enumerate(((pre_hbm, dx_acc), (cot_hbm, g_buf), (up_hbm, w_up), (down_hbm, w_down)))]
        for copy in loads:
            copy.start()
        meet((mate, cross, other))
        y_acc[...] = dot(o_ref[...], w_o_ref[...], TN)
        loads[0].wait()
        pre = dx_acc[...]
        x_wide = x_ref[...].astype(F32)
        z_mid = (x_wide + jnp.maximum(pre, 0.0) + x_wide + y_acc[...].astype(BF16).astype(F32)).astype(BF16)
        dpre_buf[...] = jnp.where(pre > 0, 1.0, 0.0).astype(BF16)
        z_buf[...] = z_mid
        loads[1].wait()
        keep = lax.broadcasted_iota(jnp.int32, (part_rows, width), 0) < count_ref[pl.ds(me, 1), :width]
        g_wide = jnp.where(keep, g_buf[...].astype(F32), 0.0)
        g_buf[...] = g_wide.astype(BF16)
        dx_acc[...] = g_wide
        y_acc[...] = z_mid.astype(F32)
        loads[2].wait()
        loads[3].wait()

        def ffn_chunk(chunk, carry):
            cols = pl.ds(pl.multiple_of(chunk * width, width), width)

            def row_block(index, inner):
                rows = pl.ds(pl.multiple_of(index * ROW_BLOCK, ROW_BLOCK), ROW_BLOCK)
                h_pre = dot(z_buf[rows, :], w_up[:, cols])
                square = h_pre * h_pre
                bend = jnp.tanh(h_pre * (GELU_A + GELU_A * GELU_B * square))
                gate = 0.5 + 0.5 * bend
                act[rows, :] = (h_pre * gate).astype(BF16)
                slope = gate + (0.5 * h_pre) * (1.0 - bend * bend) * (GELU_A + 3.0 * GELU_A * GELU_B * square)
                d_hidden = dot(g_buf[rows, :], w_down[cols, :], NT).astype(BF16)
                d_act[rows, :] = (d_hidden.astype(F32) * slope).astype(BF16)
                y_acc[rows, :] += dot(act[rows, :], w_down[cols, :])
                dx_acc[rows, :] += dot(d_act[rows, :], w_up[:, cols], NT)
                return inner

            lax.fori_loop(0, part_rows // ROW_BLOCK, row_block, 0)
            local[2 * chunk] = dot(act[...], g_buf[...], TN)

            @pl.when(chunk > 0)
            def sum_previous():
                chip_sum(2 * chunk - 1)

            local[2 * chunk + 1] = dot(z_buf[...], d_act[...], TN)
            mate_copy(2 * chunk).start()

            @pl.when(chunk > 0)
            def send_previous():
                cross_copy(2 * chunk - 1).start()

            chip_sum(2 * chunk)
            mate_copy(2 * chunk + 1).start()
            cross_copy(2 * chunk).start()
            return carry

        lax.fori_loop(0, ffn_chunks, ffn_chunk, 0)
        y_ref[...] = jnp.where(keep, y_acc[...], 0.0).astype(BF16)

    pl.run_scoped(ffn_phase, pltpu.VMEM(up_hbm.shape, BF16), pltpu.VMEM(down_hbm.shape, BF16), pltpu.VMEM(x_ref.shape, BF16), pltpu.VMEM(x_ref.shape, BF16), pltpu.VMEM(x_ref.shape, F32), pltpu.VMEM(x_ref.shape, BF16), pltpu.VMEM(x_ref.shape, BF16))
    d_z = dx_acc[...].astype(BF16)
    dz_buf[...] = d_z
    dpre_buf[...] = jnp.where(dpre_buf[...] > 0, d_z, jnp.zeros_like(d_z))
    chip_sum(first_small - 1)
    do_buf[...] = dot(w_o_ref[...], dz_buf[...], NT).astype(BF16)
    cross_copy(first_small - 1).start()

    d_agg = dot(dpre_buf[...], w_msg_ref[...], NT).astype(BF16)
    halo_out[...] = dot(adj_ref[part_rows:, :], d_agg).astype(BF16).reshape(halo_out.shape)
    dx_acc[...] = 2.0 * dz_buf[...].astype(F32) + dot(dpre_buf[...], w_self_ref[...], NT)
    dx_acc[...] += dot(adj_ref[:part_rows, :], d_agg)
    for peer in (mate, cross, other):
        halo_copy(peer, me).start()
    halo_in[me] = halo_out[me]
    local[first_small] = dot(x_ref[...], dpre_buf[...], TN)
    local[first_small + 1] = dot(agg_ref[...], dpre_buf[...], TN)
    local[first_small + 2] = dot(o_ref[...], dz_buf[...])

    def attention_phase(w_q, w_do, lse_buf, delta_buf, p_buf, ds_buf, dq_acc, dq_all, dkv_acc):
        dkv_copies = [remote(src, dkv_in.at[i], dkv_send.at[i], dkv_recv.at[i], peer) for i, (src, peer) in enumerate(((dkv_acc.at[0], mate), (dkv_sum, cross), (dkv_acc.at[2], mate)))]

        def unit_spots(unit):
            head, place = unit // blocks, lax.rem(unit, blocks)
            return head, pl.ds(pl.multiple_of(head * head_dim, head_dim), head_dim), pl.ds(pl.multiple_of(place * q_block, q_block), q_block)

        def prepare(unit, carry):
            head, rows, cols = unit_spots(unit)
            delta_buf[unit] = jnp.sum(do_buf[rows, cols].astype(F32) * o_ref[rows, cols].astype(F32), axis=0, keepdims=True)
            lse_buf[unit] = lse_ref[pl.ds(head, 1), cols]
            dq_acc[unit] = jnp.zeros((head_dim, q_block), F32)
            return carry

        lax.fori_loop(0, units, prepare, 0)
        for slot in range(2):
            w_q[slot, head_dim:, :] = jnp.zeros((head_dim, q_block), BF16)
            w_do[slot, :head_dim, :] = jnp.zeros((head_dim, q_block), BF16)
        dkv_acc[...] = jnp.zeros_like(dkv_acc)

        def place_of(step):
            group = step // per_group
            chunk = step // units
            owner = lax.rem(chip + 1 - group // 2, 2) * 2 + lax.rem(side + 1 - lax.rem(group, 2), 2)
            offset = lax.rem(chunk, halves) * key_chunk
            rows = pl.ds(pl.multiple_of(owner * part_rows + offset, key_chunk), key_chunk)
            return group, owner, offset, rows, lax.rem(step, units), lax.rem(step, 2)

        def first_stage(step):
            group, owner, offset, rows, unit, slot = place_of(step)
            head, unit_rows, cols = unit_spots(unit)
            w_q[slot, :head_dim, :] = q_ref[unit_rows, cols]
            w_do[slot, head_dim:, :] = do_buf[unit_rows, cols]
            kv = kv_ref[rows, :]
            scores = dot(kv, w_q[slot])
            row_ix = offset + key_chunk - TAIL + lax.broadcasted_iota(jnp.int32, (TAIL, q_block), 0)
            tail = jnp.where(row_ix < count_ref[pl.ds(owner, 1), :q_block], scores[key_chunk - TAIL:, :], NEG_FILL)
            scores = jnp.concatenate([scores[:key_chunk - TAIL, :], tail], axis=0)
            prob = jnp.exp2(scores * factor - lse_buf[unit])
            p_buf[slot] = prob.astype(BF16)
            ds_buf[slot] = (prob * (dot(kv, w_do[slot]) - delta_buf[unit])).astype(BF16)

        def second_stage(step):
            group, owner, offset, rows, unit, slot = place_of(step)
            d_scores = ds_buf[slot]
            spot = pl.ds(pl.multiple_of(offset, key_chunk), key_chunk)
            dkv_acc[group, spot, :] += dot(d_scores, w_q[slot], NT) + dot(p_buf[slot], w_do[slot], NT)
            dq_acc[unit] += dot(kvt_ref[:head_dim, rows], d_scores)

        def exchange(step):
            held = jnp.logical_and(step >= HOLD_STEP, step < HOLD_STEP + 12)
            turn = (step - HOLD_STEP) // 4 + first_small
            phase = lax.rem(step, 4)

            @pl.when(jnp.logical_and(held, phase == 1))
            def sum_chip():
                chip_sum(turn)

            @pl.when(jnp.logical_and(held, phase == 2))
            def send_cross():
                cross_copy(turn).start()

            lap, beat = step // FINAL_STEPS - FINAL_LAG, lax.rem(step, FINAL_STEPS)

            @pl.when(jnp.logical_and(lap >= 0, beat == 0))
            def sum_group():
                group_sum(lap)

            @pl.when(jnp.logical_and(lap >= 0, beat == 1))
            def send_back():
                for k in range(done):
                    @pl.when(lap == k)
                    def start_piece(k=k):
                        start_out(k)

            @pl.when(step == 3)
            def small_pieces():
                for index in range(first_small, total - 1):
                    mate_copy(index).start()

            @pl.when(step == per_group + 1)
            def first_group():
                dkv_copies[0].start()

            @pl.when(step == 2 * per_group + 1)
            def second_group():
                dkv_copies[0].wait_recv()
                dkv_sum[...] = dkv_acc[1] + dkv_in[0]

            @pl.when(step == 2 * per_group + 2)
            def send_second():
                dkv_copies[1].start()

            @pl.when(step == 3 * per_group + 1)
            def third_group():
                dkv_copies[2].start()

        done = (steps - 1) // FINAL_STEPS - FINAL_LAG + 1
        assert (steps - 1) % FINAL_STEPS >= 1 and 0 < done < total - 2 and HOLD_STEP > 2 * per_group + 2 and HOLD_STEP % 4 == 0

        first_stage(0)

        def body(step, carry):
            exchange(step)
            second_stage(step - 1)
            first_stage(step)
            return carry

        lax.fori_loop(1, steps, body, 0)
        second_stage(steps - 1)

        def gather_dq(unit, carry):
            head, rows, cols = unit_spots(unit)
            dq_all[rows, cols] = (dq_acc[unit] * scale).astype(BF16)
            return carry

        lax.fori_loop(0, units, gather_dq, 0)
        last = total - 1
        local[last] = dot(dq_all[...], hid_ref[...]).T
        dkv_copies[2].wait_recv()
        dkv_copies[1].wait_recv()
        dkv = dkv_acc[3] + dkv_in[2] + dkv_in[1]
        lane = lax.broadcasted_iota(jnp.int32, dkv.shape, 1)
        dkv = jnp.where(lane < head_dim, dkv * scale, dkv).astype(BF16)
        mate_copy(last).start()
        kv_local[...] = dot(dkv, hid_ref[...], TN)
        dx_acc[...] += dot(dkv, jnp.concatenate([w_kt_ref[...], w_vt_ref[...]], axis=0))
        kv_to_mate.start()
        chip_sum(last)
        kv_to_mate.wait_recv()
        kv_own[0] = kv_local[pl.ds(pl.multiple_of(side * kv_half, kv_half), kv_half), :] + kv_in[0]
        for peer in (mate, cross, other):
            halo_copy(me, peer).wait_recv()
        slot_hot = jnp.where(lax.broadcasted_iota(jnp.int32, (part_rows, 4 * halo_pair), 0) == slot_ref[...], 1.0, 0.0).astype(BF16)
        dx_acc[...] += dot(slot_hot, halo_in[...].reshape(4 * halo_pair, width))
        cross_copy(last).start()
        kv_to_cross.start()
        dx_ref[...] = (dx_acc[...] + dot(dq_all[...], w_qt_ref[...], TN)).astype(BF16)
        for index in range(done, total):
            group_sum(index)
            if index > done:
                start_out(index - 1)
        kv_to_cross.wait_recv()
        kv_own[1] = kv_own[0] + kv_in[1]
        start_out(last)
        kv_keep.start()
        kv_back(side).start()
        for copy in dkv_copies:
            copy.wait_send()

    pl.run_scoped(
        attention_phase,
        pltpu.VMEM((2, 2 * head_dim, q_block), BF16),
        pltpu.VMEM((2, 2 * head_dim, q_block), BF16),
        pltpu.VMEM((units, 1, q_block), F32),
        pltpu.VMEM((units, 1, q_block), F32),
        pltpu.VMEM((2, key_chunk, q_block), BF16),
        pltpu.VMEM((2, key_chunk, q_block), BF16),
        pltpu.VMEM((units, head_dim, q_block), F32),
        pltpu.VMEM((width, part_rows), BF16),
        pltpu.VMEM((4, part_rows, 2 * head_dim), F32),
    )
    for copy in [kv_to_mate, kv_to_cross, kv_back(side)] + [halo_copy(peer, me) for peer in (mate, cross, other)]:
        copy.wait_send()
    kv_keep.wait()
    kv_back(1 - side).wait_recv()
    for index in range(total):
        mate_copy(index).wait_send()
        cross_copy(index).wait_send()
        keep_copy(index).wait()
        back_copy(index, side).wait_send()
        back_copy(index, 1 - side).wait_recv()


def backward(counts, q_t, o_t, lse, kv, kv_t, hidden_in, x_feat, agg_msg, adjacency_t, slots, w_msg, w_self, w_q_t, w_k_t, w_v_t, w_o, pre_act, y_cot, w_up, w_down):
    width, rows = q_t.shape
    keys = kv.shape[0]
    head_dim = kv.shape[1] // 2
    heads = width // head_dim
    nodes = keys // rows
    q_block, key_chunk = 512, 512
    half = width // 2
    shapes = [w_up.shape, w_down.shape] + [(width, width)] * 4
    total = sum(r * c // (width * width) for r, c in shapes)
    halo_pair = slots.shape[1] // nodes
    vmem = pl.BlockSpec(memory_space=pltpu.VMEM)
    anywhere = pl.BlockSpec(memory_space=pl.ANY)
    dma = pltpu.SemaphoreType.DMA
    return pl.pallas_call(
        functools.partial(backward_kernel, head_dim, q_block, key_chunk, rows),
        out_shape=[jax.ShapeDtypeStruct((rows, width), BF16)] * 2 + [jax.ShapeDtypeStruct(shape, F32) for shape in shapes] + [jax.ShapeDtypeStruct((2 * head_dim, width), F32)],
        in_specs=[vmem] * 17 + [anywhere] * 4,
        out_specs=[vmem] * 2 + [anywhere] * 7,
        scratch_shapes=[
            pltpu.VMEM((width, rows), BF16),
            pltpu.VMEM((rows, width), BF16),
            pltpu.VMEM((rows, width), BF16),
            pltpu.VMEM((rows, width), F32),
            pltpu.VMEM((3, rows, 2 * head_dim), F32),
            pltpu.VMEM((rows, 2 * head_dim), F32),
            pltpu.VMEM((total, width, width), F32),
            pltpu.VMEM((total, half, width), F32),
            pltpu.VMEM((total, half, width), F32),
            pltpu.VMEM((2 * head_dim, width), F32),
            pltpu.VMEM((2, head_dim, width), F32),
            pltpu.VMEM((2, head_dim, width), F32),
            pltpu.VMEM((nodes, halo_pair, width), BF16),
            pltpu.VMEM((nodes, halo_pair, width), BF16),
            dma((4,)), dma((total,)), dma((3, total)), dma((3, total)), dma((3,)), dma((3,)), dma, dma((3,)), dma((3,)), dma((nodes,)), dma((nodes,)),
        ],
        compiler_params=pltpu.CompilerParams(vmem_limit_bytes=67043328, collective_id=1, has_side_effects=True),
        cost_estimate=pl.CostEstimate(flops=10 * heads * rows * keys * head_dim, bytes_accessed=40 << 20, transcendentals=heads * rows * keys),
        name='backward',
    )(counts, q_t, o_t, lse, kv, kv_t, hidden_in, x_feat, agg_msg, adjacency_t, slots, w_msg, w_self, w_q_t, w_k_t, w_v_t, w_o, pre_act, y_cot, w_up, w_down)


def solution(mesh):
    nodes = mesh.shape['nodes']
    row_spec = P(('graphs', 'nodes'), None)
    flat_spec = P(('graphs', 'nodes'))
    halo_spec = P(('graphs', 'nodes'), None, None)
    grad_spec = P('graphs', None)

    def device_step(x_feat, valid, halo_slot, edge_src, edge_dst, edge_mask, bal_perm, pos_enc, y_cot, w_msg, w_self, w_q, w_k, w_v, w_o, w_up, w_down):
        rows_dev, width = x_feat.shape
        head_dim = w_k.shape[1]
        me = lax.axis_index('nodes')
        halo_pair = halo_slot.shape[2]

        lane_owner = jnp.arange(rows_dev)[None, :] // halo_pair
        wanted = jnp.where(lane_owner == me, jnp.tile(halo_slot.reshape(nodes, halo_pair), (1, rows_dev // halo_pair)), -1)
        meta = jnp.concatenate([bal_perm[None, :], valid[None, :], wanted, jnp.zeros((6 - nodes, rows_dev), jnp.int32)], axis=0)
        w_q_t, w_k_t, w_v_t = w_q.T, w_k.T, w_v.T
        q_t, kv_all, kv_all_t, hidden_in, agg_msg, pre_act, adjacency_t, slots, counts = front(meta, x_feat, pos_enc, edge_src, edge_dst, edge_mask, w_q_t, w_k_t, w_v_t, w_msg, w_self, nodes, halo_pair)
        mixed_t, lse = attention_forward(counts, q_t, kv_all, kv_all_t, head_dim, rows_dev)
        y_out, dx_feat, grad_up, grad_down, grad_self, grad_msg, grad_o, grad_q, grad_kv = backward(counts, q_t, mixed_t, lse, kv_all, kv_all_t, hidden_in, x_feat, agg_msg, adjacency_t, slots, w_msg, w_self, w_q_t, w_k_t, w_v_t, w_o, pre_act, y_cot, w_up, w_down)
        grad_k, grad_v = grad_kv[:head_dim].T, grad_kv[head_dim:].T
        return (y_out, dx_feat, grad_msg, grad_self, grad_q, grad_k, grad_v, grad_o, grad_up, grad_down)

    return jax.shard_map(device_step, mesh=mesh, in_specs=(row_spec, flat_spec, halo_spec, row_spec, row_spec, row_spec, flat_spec, row_spec, row_spec) + (P(),) * 8, out_specs=(row_spec, row_spec) + (grad_spec,) * 8, check_vma=False)
```

```python
import functools
import math

import jax
import jax.numpy as jnp
from jax import lax
from jax.experimental import pallas as pl
from jax.experimental.pallas import tpu as pltpu
from jax.sharding import PartitionSpec as P

NEG_FILL = -1e30
LOG2E = math.log2(math.e)
TAIL = 32
F32 = jnp.float32
BF16 = jnp.bfloat16
NN = (((1,), (0,)), ((), ()))
NT = (((1,), (1,)), ((), ()))
TN = (((0,), (0,)), ((), ()))
TT = (((0,), (1,)), ((), ()))


def dot(a, b, dims=NN):
    return lax.dot_general(a, b, dims, preferred_element_type=F32)


def remote(src, dst, send, recv, peer):
    return pltpu.make_async_remote_copy(src_ref=src, dst_ref=dst, send_sem=send, recv_sem=recv, device_id={'nodes': peer}, device_id_type=pl.DeviceIdType.MESH)


def neighbours():
    me = lax.axis_index('nodes')
    chip, side = me // 2, lax.rem(me, 2)
    return me, chip, side, chip * 2 + 1 - side, (1 - chip) * 2 + side, (1 - chip) * 2 + 1 - side


def meet(peers):
    barrier = pltpu.get_barrier_semaphore()
    for peer in peers:
        pl.semaphore_signal(barrier, inc=1, device_id={'nodes': peer}, device_id_type=pl.DeviceIdType.MESH)
    pl.semaphore_wait(barrier, len(peers))


CHUNKS, EDGE_STEP, POS_PIECES, KV_PIECES = 4, 512, 4, 2


def front_kernel(head_dim, perm_ref, valid_ref, halo_ref, x_hbm, pos_hbm, src_hbm, dst_hbm, on_hbm, w_q_hbm, w_kt_hbm, w_vt_hbm, w_msg_hbm, w_self_hbm, *rest):
    (out_ref, lse_ref, slot_ref, count_ref), rest = rest[:4], rest[4:]
    saved, rest = rest[:7], rest[7:]
    kept, rest = rest[:7], rest[7:]
    q_ref, kv_ref, kvt_ref, hid_ref, agg_ref, pre_ref, adj_ref = kept
    loaded, rest = rest[:10], rest[10:]
    x_ref, pos_ref, src_ref, dst_ref, on_ref, w_q_ref, w_kt_ref, w_vt_ref, w_msg_ref, w_self_ref = loaded
    w_unit, s_even, s_odd, stat, meta_ref, meta_all, pos_all, pos_acc, counts_acc, edge_acc, halo_out, halo_in, kv_all, load_sem, save_sem, meta_send, meta_recv, pos_send, pos_recv, halo_send, halo_recv, kv_send, kv_recv = rest
    rows_dev, width = x_ref.shape
    table_rows = adj_ref.shape[0]
    half = rows_dev // 2
    nodes = meta_all.shape[0]
    halo_pair = halo_in.shape[1]
    me, chip, side, mate, cross, other = neighbours()
    peers = (mate, cross, other)
    loads = [pltpu.make_async_copy(src, dst, load_sem.at[i]) for i, (src, dst) in enumerate(zip((x_hbm, pos_hbm, src_hbm, dst_hbm, on_hbm, w_q_hbm, w_kt_hbm, w_vt_hbm, w_msg_hbm, w_self_hbm), loaded))]
    saves = [pltpu.make_async_copy(src, dst, save_sem.at[i]) for i, (src, dst) in enumerate(zip(kept, saved))]
    for copy in loads:
        copy.start()
    meta_ref[...] = jnp.zeros_like(meta_ref)
    meta_ref[0:1, :] = perm_ref[...]
    meta_ref[1:2, :] = valid_ref[...]
    lanes = nodes * halo_pair
    mine = lax.broadcasted_iota(jnp.int32, (nodes, lanes), 1) // halo_pair == me
    meta_ref[2:2 + nodes, 0:lanes] = jnp.where(mine, jnp.concatenate([halo_ref[...]] * nodes, axis=1), -1)
    meet(peers)

    meta_copies = [remote(meta_ref, meta_all.at[me], meta_send.at[i], meta_recv.at[me], peer) for i, peer in enumerate(peers)]
    piece = rows_dev // POS_PIECES

    def pos_rows(index):
        return pl.ds(index * piece, piece)

    pos_to_cross = [remote(pos_ref.at[pos_rows(k), :], pos_all.at[me, pos_rows(k), :], pos_send.at[0, k], pos_recv.at[0, k], cross) for k in range(POS_PIECES)]
    pos_to_mate = [remote(pos_ref.at[pos_rows(k), :], pos_all.at[me, pos_rows(k), :], pos_send.at[1, k], pos_recv.at[1, k], mate) for k in range(POS_PIECES)]
    pos_relay = [remote(pos_all.at[cross, pos_rows(k), :], pos_all.at[cross, pos_rows(k), :], pos_send.at[2, k], pos_recv.at[2, k], mate) for k in range(POS_PIECES)]
    for copy in meta_copies:
        copy.start()
    loads[1].wait()
    for copy in pos_to_cross + pos_to_mate:
        copy.start()
    meta_all[me] = meta_ref[...]
    for copy in loads[:1] + loads[2:]:
        copy.wait()

    def relay_pos(k):
        pos_to_cross[k].wait_recv()
        pos_relay[k].start()

    def place_pos(owner, source, first):
        perm = meta_all[owner, 0:1, :] - me * rows_dev
        size = 256

        def body(index, carry):
            rows = pl.ds(pl.multiple_of(index * size, size), size)
            hot = jnp.where(index * size + lax.broadcasted_iota(jnp.int32, (size, rows_dev), 0) == perm, 1.0, 0.0).astype(BF16)
            part = dot(hot, source[...])
            pos_acc[rows, :] = part if first else pos_acc[rows, :] + part
            return carry

        lax.fori_loop(0, rows_dev // size, body, 0)

    edges = src_ref.shape[1]
    steps = edges // (CHUNKS * EDGE_STEP)
    assert CHUNKS * EDGE_STEP * steps == edges and EDGE_STEP * steps < 4096

    def edge_block(index):
        cols = pl.ds(pl.multiple_of(index * EDGE_STEP, EDGE_STEP), EDGE_STEP)
        src, dst, on = src_ref[:, cols], dst_ref[:, cols], on_ref[:, cols]
        upper = dst >= half
        place = jnp.where(upper, dst - half, dst)
        weight = jnp.where(on > 0, jnp.where(upper, 4096.0, 1.0), 0.0)
        src_hot = jnp.where(lax.broadcasted_iota(jnp.int32, (table_rows, EDGE_STEP), 0) == src, 1.0, 0.0).astype(BF16)
        dst_hot = jnp.where(lax.broadcasted_iota(jnp.int32, (half, EDGE_STEP), 0) == place, weight, 0.0).astype(BF16)
        return dot(src_hot, dst_hot, NT)

    def count_chunk(chunk):
        edge_acc[...] = jnp.zeros_like(edge_acc)

        def body(step, carry):
            edge_acc[...] += edge_block(chunk * steps + step)
            return carry

        lax.fori_loop(0, steps, body, 0)
        total = edge_acc[...]
        high = jnp.floor(total * (1.0 / 4096.0))
        low = total - high * 4096.0
        if chunk == 0:
            counts_acc[:, :half] = low
            counts_acc[:, half:] = high
        elif chunk < CHUNKS - 1:
            counts_acc[:, :half] += low
            counts_acc[:, half:] += high
        else:
            adj_ref[:, :half] = (counts_acc[:, :half] + low).astype(BF16)
            adj_ref[:, half:] = (counts_acc[:, half:] + high).astype(BF16)

    def halo_copy(peer, owner):
        return remote(halo_out.at[peer], halo_in.at[owner], halo_send.at[peer], halo_recv.at[owner], peer)

    count_chunk(0)
    for peer in peers:
        remote(meta_ref, meta_all.at[peer], meta_send.at[0], meta_recv.at[peer], peer).wait_recv()
    tables = meta_all[0, :, 0:nodes * halo_pair]
    for node in range(1, nodes):
        tables = jnp.maximum(tables, meta_all[node, :, 0:nodes * halo_pair])
    tables = jnp.where(lax.broadcasted_iota(jnp.int32, tables.shape, 0) == 2 + me, tables, -1)
    slots = jnp.max(tables.astype(F32), axis=0, keepdims=True).astype(jnp.int32)
    slot_ref[...] = slots
    slot_hot = jnp.where(lax.broadcasted_iota(jnp.int32, (rows_dev, nodes * halo_pair), 0) == slots, 1.0, 0.0).astype(BF16)
    halo_out[...] = dot(slot_hot, x_ref[...], TN).astype(BF16).reshape(halo_out.shape)
    relay_pos(0)
    place_pos(me, pos_ref, True)
    for peer in peers:
        halo_copy(peer, me).start()
    halo_in[me] = halo_out[me]
    for node in range(nodes):
        held = jnp.sum(meta_all[node, 1:2, :].astype(F32), axis=1, keepdims=True).astype(jnp.int32)
        count_ref[node:node + 1, :] = jnp.broadcast_to(held, (1, count_ref.shape[1]))
    count_chunk(1)
    relay_pos(1)
    for copy in pos_to_mate:
        copy.wait_recv()
    place_pos(mate, pos_all.at[mate], False)
    count_chunk(2)
    relay_pos(2)
    count_chunk(3)
    relay_pos(3)
    place_pos(cross, pos_all.at[cross], False)
    for copy in pos_relay:
        copy.wait_recv()
    place_pos(other, pos_all.at[other], False)

    hid_ref[...] = (x_ref[...].astype(F32) + pos_acc[...]).astype(BF16)
    kv_all[me] = dot(hid_ref[...], jnp.concatenate([w_kt_ref[...], w_vt_ref[...]], axis=0), NT).astype(BF16)
    q_ref[...] = dot(w_q_ref[...].T, hid_ref[...], NT).astype(BF16)
    kv_piece = rows_dev // KV_PIECES

    def kv_copy(owner, k, kind, peer):
        rows = pl.ds(k * kv_piece, kv_piece)
        return remote(kv_all.at[owner, rows, :], kv_all.at[owner, rows, :], kv_send.at[kind, k], kv_recv.at[kind, k], peer)

    kv_to_cross = [kv_copy(me, k, 0, cross) for k in range(KV_PIECES)]
    kv_to_mate = [kv_copy(me, k, 1, mate) for k in range(KV_PIECES)]
    kv_relay = [kv_copy(cross, k, 2, mate) for k in range(KV_PIECES)]
    for copy in kv_to_cross + kv_to_mate:
        copy.start()
    size = kv_all.shape[2]
    eye = jnp.where(lax.broadcasted_iota(jnp.int32, (size, size), 0) == lax.broadcasted_iota(jnp.int32, (size, size), 1), 1.0, 0.0).astype(BF16)

    def keep_kv(owner):
        rows = pl.ds(pl.multiple_of(owner * rows_dev, rows_dev), rows_dev)
        kv_ref[rows, :] = kv_all[owner]
        kvt_ref[:, rows] = dot(eye, kv_all[owner], NT).astype(BF16)

    for peer in peers:
        halo_copy(me, peer).wait_recv()
    agg = dot(adj_ref[:rows_dev, :], x_ref[...], TN) + dot(adj_ref[rows_dev:, :], halo_in[...].reshape(nodes * halo_pair, width), TN)
    agg_ref[...] = agg.astype(BF16)
    keep_kv(me)
    kv_to_cross[0].wait_recv()
    kv_relay[0].start()
    pre_ref[...] = dot(agg_ref[...], w_msg_ref[...]) + dot(x_ref[...], w_self_ref[...])
    for k in range(1, KV_PIECES):
        kv_to_cross[k].wait_recv()
        kv_relay[k].start()
    for copy in kv_to_mate:
        copy.wait_recv()
    keep_kv(mate)
    keep_kv(cross)
    for copy in kv_relay:
        copy.wait_recv()
    keep_kv(other)
    for copy in saves:
        copy.start()
    attention_forward(head_dim, rows_dev, count_ref, q_ref, kv_ref, kvt_ref, out_ref, lse_ref, w_unit, s_even, s_odd, stat)
    for copy in saves:
        copy.wait()
    for copy in meta_copies + pos_to_cross + pos_to_mate + pos_relay + [halo_copy(peer, me) for peer in peers] + kv_to_cross + kv_to_mate + kv_relay:
        copy.wait_send()


def front(perm, valid, halo_slot, x_feat, pos_enc, edge_src, edge_dst, edge_mask, w_q, w_k_t, w_v_t, w_msg, w_self):
    rows, width = x_feat.shape
    nodes, halo_pair = halo_slot.shape
    head_dim = w_k_t.shape[0]
    pair = 2 * head_dim
    heads = width // head_dim
    keys = nodes * rows
    table_rows = rows + nodes * halo_pair
    vmem = pl.BlockSpec(memory_space=pltpu.VMEM)
    anywhere = pl.BlockSpec(memory_space=pl.ANY)
    dma = pltpu.SemaphoreType.DMA
    small = [((width, rows), BF16), ((heads, rows), F32), ((1, nodes * halo_pair), jnp.int32), ((nodes, 512), jnp.int32)]
    saved = [((width, rows), BF16), ((keys, pair), BF16), ((pair, keys), BF16), ((rows, width), BF16), ((rows, width), BF16), ((rows, width), F32), ((table_rows, rows), BF16)]
    inputs = (x_feat, pos_enc, edge_src, edge_dst, edge_mask, w_q, w_k_t, w_v_t, w_msg, w_self)
    return pl.pallas_call(
        functools.partial(front_kernel, head_dim),
        out_shape=[jax.ShapeDtypeStruct(shape, dtype) for shape, dtype in small + saved],
        in_specs=[vmem] * 3 + [anywhere] * len(inputs),
        out_specs=[vmem] * len(small) + [anywhere] * len(saved),
        scratch_shapes=[pltpu.VMEM(shape, dtype) for shape, dtype in saved] + [pltpu.VMEM(a.shape, a.dtype) for a in inputs] + [
            pltpu.VMEM((pair, Q_BLOCK), BF16),
            pltpu.VMEM((keys, Q_BLOCK), F32),
            pltpu.VMEM((keys, Q_BLOCK), F32),
            pltpu.VMEM((8, Q_BLOCK), F32),
            pltpu.VMEM((8, rows), jnp.int32),
            pltpu.VMEM((nodes, 8, rows), jnp.int32),
            pltpu.VMEM((nodes, rows, width), BF16),
            pltpu.VMEM((rows, width), F32),
            pltpu.VMEM((table_rows, rows), F32),
            pltpu.VMEM((table_rows, rows // 2), F32),
            pltpu.VMEM((nodes, halo_pair, width), BF16),
            pltpu.VMEM((nodes, halo_pair, width), BF16),
            pltpu.VMEM((nodes, rows, pair), BF16),
            dma((len(inputs),)), dma((len(saved),)), dma((3,)), dma((nodes,)), dma((3, POS_PIECES)), dma((3, POS_PIECES)), dma((nodes,)), dma((nodes,)), dma((3, KV_PIECES)), dma((3, KV_PIECES)),
        ],
        compiler_params=pltpu.CompilerParams(vmem_limit_bytes=60 << 20, collective_id=2, has_side_effects=True),
        cost_estimate=pl.CostEstimate(flops=24 << 30, bytes_accessed=20 << 20, transcendentals=heads * rows * keys),
        name='front',
    )(perm, valid, halo_slot, *inputs)


def mask_tail(scores, chunk, key_chunk, part_rows, count_ref):
    start = chunk * key_chunk
    part = start // part_rows
    first = start - part * part_rows + key_chunk - TAIL
    row_ix = first + lax.broadcasted_iota(jnp.int32, (TAIL, scores.shape[1]), 0)
    tail = jnp.where(row_ix < count_ref[pl.ds(part, 1), :scores.shape[1]], scores[key_chunk - TAIL:, :], NEG_FILL)
    return jnp.concatenate([scores[:key_chunk - TAIL, :], tail], axis=0)


Q_BLOCK, KEY_CHUNK = 256, 1024


def attention_forward(head_dim, part_rows, count_ref, q_ref, kv_ref, kvt_ref, out_ref, lse_ref, w_q, s_even, s_odd, stat):
    heads = q_ref.shape[0] // head_dim
    blocks = q_ref.shape[1] // Q_BLOCK
    units = heads * blocks
    chunks = kv_ref.shape[0] // KEY_CHUNK
    factor = head_dim ** -0.5 * LOG2E
    groups = KEY_CHUNK // 8

    def load_weights(unit):
        head, block = unit // blocks, lax.rem(unit, blocks)
        w_q[:head_dim, :] = q_ref[pl.ds(pl.multiple_of(head * head_dim, head_dim), head_dim), pl.ds(pl.multiple_of(block * Q_BLOCK, Q_BLOCK), Q_BLOCK)]

    def score_stage(buffer, chunk, run_max):
        rows = pl.ds(pl.multiple_of(chunk * KEY_CHUNK, KEY_CHUNK), KEY_CHUNK)
        scores = mask_tail(dot(kv_ref[rows, :], w_q[...]), chunk, KEY_CHUNK, part_rows, count_ref)
        buffer[rows, :] = scores
        return jnp.maximum(run_max, jnp.max(scores.reshape(groups, 8, Q_BLOCK), axis=0))

    w_q[head_dim:, :] = jnp.zeros((w_q.shape[0] - head_dim, Q_BLOCK), BF16)
    floor = jnp.full((8, Q_BLOCK), -jnp.inf, F32)
    load_weights(0)
    stat[...] = lax.fori_loop(0, chunks, lambda chunk, run_max: score_stage(s_even, chunk, run_max), floor)

    def one_unit(unit, held, free):
        load_weights(jnp.minimum(unit + 1, units - 1))
        top = jnp.max(stat[...], axis=0, keepdims=True) * factor

        def chunk_body(chunk, state):
            run_max, run_sum, weighted = state
            cols = pl.ds(pl.multiple_of(chunk * KEY_CHUNK, KEY_CHUNK), KEY_CHUNK)
            run_max = score_stage(free, chunk, run_max)
            prob = jnp.exp2(held[cols, :] * factor - top)
            run_sum = run_sum + jnp.sum(prob.reshape(groups, 8, Q_BLOCK), axis=0)
            weighted = weighted + dot(kvt_ref[head_dim:2 * head_dim, cols], prob.astype(BF16))
            return run_max, run_sum, weighted

        run_max, run_sum, weighted = lax.fori_loop(0, chunks, chunk_body, (floor, jnp.zeros((8, Q_BLOCK), F32), jnp.zeros((head_dim, Q_BLOCK), F32)))
        stat[...] = run_max
        total = jnp.sum(run_sum, axis=0, keepdims=True)
        head, block = unit // blocks, lax.rem(unit, blocks)
        cols = pl.ds(pl.multiple_of(block * Q_BLOCK, Q_BLOCK), Q_BLOCK)
        out_ref[pl.ds(pl.multiple_of(head * head_dim, head_dim), head_dim), cols] = (weighted / total).astype(BF16)
        lse_ref[pl.ds(head, 1), cols] = top + jnp.log2(total)

    def unit_pair(pair, carry):
        one_unit(2 * pair, s_even, s_odd)
        one_unit(2 * pair + 1, s_odd, s_even)
        return carry

    lax.fori_loop(0, units // 2, unit_pair, 0)


FINAL_STEPS, FINAL_LAG = 14, 1
HOLD_STEP = 68
ROW_BLOCK = 256
GELU_A, GELU_B = math.sqrt(2.0 / math.pi), 0.044715


def backward_kernel(head_dim, q_block, key_chunk, part_rows, count_ref, o_ref, lse_ref, slot_ref, x_ref, w_o_ref, pre_hbm, cot_hbm, up_hbm, down_hbm, *rest):
    later, rest = rest[:10], rest[10:]
    y_ref, dx_ref, rest = rest[0], rest[1], rest[2:]
    sum_refs, kv_sum_ref, rest = rest[:6], rest[6], rest[7:]
    held, rest = rest[:10], rest[10:]
    q_ref, kv_ref, kvt_ref, hid_ref, agg_ref, adj_ref, w_msg_ref, w_self_ref, w_q_ref, w_kvt_ref = held
    do_buf, dz_buf, dpre_buf, dx_acc, dkv_in, dkv_sum, local, from_mate, from_cross, kv_local, kv_own, kv_in, halo_out, halo_in, load_sem, held_sem, keep_sem, send_sem, recv_sem, dkv_send, dkv_recv, kv_sem, kv_send, kv_recv, halo_send, halo_recv = rest
    heads = q_ref.shape[0] // head_dim
    blocks = q_ref.shape[1] // q_block
    units = heads * blocks
    chunks = kv_ref.shape[0] // key_chunk
    steps = units * chunks
    per_group = steps // 4
    halves = part_rows // key_chunk
    scale = head_dim ** -0.5
    factor = scale * LOG2E
    total, width = local.shape[0], local.shape[1]
    half_rows = width // 2
    ffn_chunks = up_hbm.shape[1] // width
    first_small = 2 * ffn_chunks
    me, chip, side, mate, cross, other = neighbours()

    def block(index, half):
        if index >= first_small:
            return sum_refs[2 + index - first_small].at[pl.ds(half * half_rows, half_rows), :]
        chunk = index // 2
        if index % 2 == 0:
            return sum_refs[1].at[pl.ds(chunk * width + half * half_rows, half_rows), :]
        return sum_refs[0].at[pl.ds(half * half_rows, half_rows), pl.ds(chunk * width, width)]

    def part(index, half):
        return local.at[index, pl.ds(half * half_rows, half_rows), :]

    def to_peer(src, dst, kind, index, peer):
        return remote(src, dst, send_sem.at[kind, index], recv_sem.at[kind, index], peer)

    def mate_copy(index):
        return to_peer(part(index, 1 - side), from_mate.at[index], 0, index, mate)

    def cross_copy(index):
        return to_peer(part(index, side), from_cross.at[index], 1, index, cross)

    def back_copy(index, half):
        return to_peer(from_mate.at[index], block(index, half), 2, index, mate)

    def keep_copy(index):
        return pltpu.make_async_copy(from_mate.at[index], block(index, side), keep_sem.at[index])

    my_half = pl.ds(pl.multiple_of(side * half_rows, half_rows), half_rows)

    def chip_sum(index):
        mate_copy(index).wait_recv()
        local[index, my_half, :] = local[index, my_half, :] + from_mate[index]

    def group_sum(index):
        cross_copy(index).wait_recv()
        from_mate[index] = local[index, my_half, :] + from_cross[index]

    def start_out(index):
        keep_copy(index).start()
        back_copy(index, side).start()

    kv_half = kv_local.shape[0] // 2

    def kv_rows(half):
        return pl.ds(half * kv_half, kv_half)

    kv_to_mate = remote(kv_local.at[kv_rows(1 - side), :], kv_in.at[0], kv_send.at[0], kv_recv.at[0], mate)
    kv_to_cross = remote(kv_own.at[0], kv_in.at[1], kv_send.at[1], kv_recv.at[1], cross)
    kv_keep = pltpu.make_async_copy(kv_own.at[1], kv_sum_ref.at[kv_rows(side), :], kv_sem)

    def kv_back(half):
        return remote(kv_own.at[1], kv_sum_ref.at[kv_rows(half), :], kv_send.at[2], kv_recv.at[2], mate)

    halo_pair = halo_out.shape[1]

    def halo_copy(peer, owner):
        return remote(halo_out.at[peer], halo_in.at[owner], halo_send.at[peer], halo_recv.at[owner], peer)

    held_loads = [pltpu.make_async_copy(src, dst, held_sem.at[i]) for i, (src, dst) in enumerate(zip(later, held))]

    def ffn_phase(w_up, w_down, g_buf, z_buf, y_acc, act, d_act):
        loads = [pltpu.make_async_copy(src, dst, load_sem.at[i]) for i, (src, dst) in enumerate(((pre_hbm, dx_acc), (cot_hbm, g_buf), (up_hbm, w_up), (down_hbm, w_down)))]
        for copy in loads + held_loads:
            copy.start()
        meet((mate, cross, other))
        y_acc[...] = dot(o_ref[...], w_o_ref[...], TN)
        loads[0].wait()
        pre = dx_acc[...]
        x_wide = x_ref[...].astype(F32)
        z_mid = (x_wide + jnp.maximum(pre, 0.0) + x_wide + y_acc[...].astype(BF16).astype(F32)).astype(BF16)
        dpre_buf[...] = jnp.where(pre > 0, 1.0, 0.0).astype(BF16)
        z_buf[...] = z_mid
        loads[1].wait()
        keep = lax.broadcasted_iota(jnp.int32, (part_rows, width), 0) < count_ref[pl.ds(me, 1), :width]
        g_wide = jnp.where(keep, g_buf[...].astype(F32), 0.0)
        g_buf[...] = g_wide.astype(BF16)
        dx_acc[...] = g_wide
        y_acc[...] = z_mid.astype(F32)
        loads[2].wait()
        loads[3].wait()

        def ffn_chunk(chunk, carry):
            cols = pl.ds(pl.multiple_of(chunk * width, width), width)

            def row_block(index, inner):
                rows = pl.ds(pl.multiple_of(index * ROW_BLOCK, ROW_BLOCK), ROW_BLOCK)
                h_pre = dot(z_buf[rows, :], w_up[:, cols])
                square = h_pre * h_pre
                bend = jnp.tanh(h_pre * (GELU_A + GELU_A * GELU_B * square))
                gate = 0.5 + 0.5 * bend
                act[rows, :] = (h_pre * gate).astype(BF16)
                slope = gate + (0.5 * h_pre) * (1.0 - bend * bend) * (GELU_A + 3.0 * GELU_A * GELU_B * square)
                d_hidden = dot(g_buf[rows, :], w_down[cols, :], NT).astype(BF16)
                d_act[rows, :] = (d_hidden.astype(F32) * slope).astype(BF16)
                y_acc[rows, :] += dot(act[rows, :], w_down[cols, :])
                dx_acc[rows, :] += dot(d_act[rows, :], w_up[:, cols], NT)
                return inner

            lax.fori_loop(0, part_rows // ROW_BLOCK, row_block, 0)
            local[2 * chunk] = dot(act[...], g_buf[...], TN)

            @pl.when(chunk > 0)
            def sum_previous():
                chip_sum(2 * chunk - 1)

            local[2 * chunk + 1] = dot(z_buf[...], d_act[...], TN)
            mate_copy(2 * chunk).start()

            @pl.when(chunk > 0)
            def send_previous():
                cross_copy(2 * chunk - 1).start()

            chip_sum(2 * chunk)
            mate_copy(2 * chunk + 1).start()
            cross_copy(2 * chunk).start()
            return carry

        lax.fori_loop(0, ffn_chunks, ffn_chunk, 0)
        y_ref[...] = jnp.where(keep, y_acc[...], 0.0).astype(BF16)

    pl.run_scoped(ffn_phase, pltpu.VMEM(up_hbm.shape, BF16), pltpu.VMEM(down_hbm.shape, BF16), pltpu.VMEM(x_ref.shape, BF16), pltpu.VMEM(x_ref.shape, BF16), pltpu.VMEM(x_ref.shape, F32), pltpu.VMEM(x_ref.shape, BF16), pltpu.VMEM(x_ref.shape, BF16))
    for copy in held_loads:
        copy.wait()
    d_z = dx_acc[...].astype(BF16)
    dz_buf[...] = d_z
    dpre_buf[...] = jnp.where(dpre_buf[...] > 0, d_z, jnp.zeros_like(d_z))
    chip_sum(first_small - 1)
    do_buf[...] = dot(w_o_ref[...], dz_buf[...], NT).astype(BF16)
    cross_copy(first_small - 1).start()

    d_agg = dot(dpre_buf[...], w_msg_ref[...], NT).astype(BF16)
    halo_out[...] = dot(adj_ref[part_rows:, :], d_agg).astype(BF16).reshape(halo_out.shape)
    dx_acc[...] = 2.0 * dz_buf[...].astype(F32) + dot(dpre_buf[...], w_self_ref[...], NT)
    dx_acc[...] += dot(adj_ref[:part_rows, :], d_agg)
    for peer in (mate, cross, other):
        halo_copy(peer, me).start()
    halo_in[me] = halo_out[me]
    local[first_small] = dot(x_ref[...], dpre_buf[...], TN)
    local[first_small + 1] = dot(agg_ref[...], dpre_buf[...], TN)
    local[first_small + 2] = dot(o_ref[...], dz_buf[...])

    def attention_phase(w_q, w_do, lse_buf, delta_buf, p_buf, ds_buf, dq_acc, dq_all, dkv_acc):
        dkv_copies = [remote(src, dkv_in.at[i], dkv_send.at[i], dkv_recv.at[i], peer) for i, (src, peer) in enumerate(((dkv_acc.at[0], mate), (dkv_sum, cross), (dkv_acc.at[2], mate)))]

        def unit_spots(unit):
            head, place = unit // blocks, lax.rem(unit, blocks)
            return head, pl.ds(pl.multiple_of(head * head_dim, head_dim), head_dim), pl.ds(pl.multiple_of(place * q_block, q_block), q_block)

        def prepare(unit, carry):
            head, rows, cols = unit_spots(unit)
            delta_buf[unit] = jnp.sum(do_buf[rows, cols].astype(F32) * o_ref[rows, cols].astype(F32), axis=0, keepdims=True)
            lse_buf[unit] = lse_ref[pl.ds(head, 1), cols]
            dq_acc[unit] = jnp.zeros((head_dim, q_block), F32)
            return carry

        lax.fori_loop(0, units, prepare, 0)
        for slot in range(2):
            w_q[slot, head_dim:, :] = jnp.zeros((head_dim, q_block), BF16)
            w_do[slot, :head_dim, :] = jnp.zeros((head_dim, q_block), BF16)
        dkv_acc[...] = jnp.zeros_like(dkv_acc)

        def place_of(step):
            group = step // per_group
            chunk = step // units
            owner = lax.rem(chip + 1 - group // 2, 2) * 2 + lax.rem(side + 1 - lax.rem(group, 2), 2)
            offset = lax.rem(chunk, halves) * key_chunk
            rows = pl.ds(pl.multiple_of(owner * part_rows + offset, key_chunk), key_chunk)
            return group, owner, offset, rows, lax.rem(step, units), lax.rem(step, 2)

        def first_stage(step):
            group, owner, offset, rows, unit, slot = place_of(step)
            head, unit_rows, cols = unit_spots(unit)
            w_q[slot, :head_dim, :] = q_ref[unit_rows, cols]
            w_do[slot, head_dim:, :] = do_buf[unit_rows, cols]
            kv = kv_ref[rows, :]
            scores = dot(kv, w_q[slot])
            row_ix = offset + key_chunk - TAIL + lax.broadcasted_iota(jnp.int32, (TAIL, q_block), 0)
            tail = jnp.where(row_ix < count_ref[pl.ds(owner, 1), :q_block], scores[key_chunk - TAIL:, :], NEG_FILL)
            scores = jnp.concatenate([scores[:key_chunk - TAIL, :], tail], axis=0)
            prob = jnp.exp2(scores * factor - lse_buf[unit])
            p_buf[slot] = prob.astype(BF16)
            ds_buf[slot] = (prob * (dot(kv, w_do[slot]) - delta_buf[unit])).astype(BF16)

        def second_stage(step):
            group, owner, offset, rows, unit, slot = place_of(step)
            d_scores = ds_buf[slot]
            spot = pl.ds(pl.multiple_of(offset, key_chunk), key_chunk)
            dkv_acc[group, spot, :] += dot(d_scores, w_q[slot], NT) + dot(p_buf[slot], w_do[slot], NT)
            dq_acc[unit] += dot(kvt_ref[:head_dim, rows], d_scores)

        def exchange(step):
            held = jnp.logical_and(step >= HOLD_STEP, step < HOLD_STEP + 12)
            turn = (step - HOLD_STEP) // 4 + first_small
            phase = lax.rem(step, 4)

            @pl.when(jnp.logical_and(held, phase == 1))
            def sum_chip():
                chip_sum(turn)

            @pl.when(jnp.logical_and(held, phase == 2))
            def send_cross():
                cross_copy(turn).start()

            lap, beat = step // FINAL_STEPS - FINAL_LAG, lax.rem(step, FINAL_STEPS)

            @pl.when(jnp.logical_and(lap >= 0, beat == 0))
            def sum_group():
                group_sum(lap)

            @pl.when(jnp.logical_and(lap >= 0, beat == 1))
            def send_back():
                for k in range(done):
                    @pl.when(lap == k)
                    def start_piece(k=k):
                        start_out(k)

            @pl.when(step == 3)
            def small_pieces():
                for index in range(first_small, total - 1):
                    mate_copy(index).start()

            @pl.when(step == per_group + 1)
            def first_group():
                dkv_copies[0].start()

            @pl.when(step == 2 * per_group + 1)
            def second_group():
                dkv_copies[0].wait_recv()
                dkv_sum[...] = dkv_acc[1] + dkv_in[0]

            @pl.when(step == 2 * per_group + 2)
            def send_second():
                dkv_copies[1].start()

            @pl.when(step == 3 * per_group + 1)
            def third_group():
                dkv_copies[2].start()

        done = (steps - 1) // FINAL_STEPS - FINAL_LAG + 1
        assert (steps - 1) % FINAL_STEPS >= 1 and 0 < done < total - 2 and HOLD_STEP > 2 * per_group + 2 and HOLD_STEP % 4 == 0

        first_stage(0)

        def body(step, carry):
            exchange(step)
            second_stage(step - 1)
            first_stage(step)
            return carry

        lax.fori_loop(1, steps, body, 0)
        second_stage(steps - 1)

        def gather_dq(unit, carry):
            head, rows, cols = unit_spots(unit)
            dq_all[rows, cols] = (dq_acc[unit] * scale).astype(BF16)
            return carry

        lax.fori_loop(0, units, gather_dq, 0)
        last = total - 1
        local[last] = dot(dq_all[...], hid_ref[...]).T
        dkv_copies[2].wait_recv()
        dkv_copies[1].wait_recv()
        dkv = dkv_acc[3] + dkv_in[2] + dkv_in[1]
        lane = lax.broadcasted_iota(jnp.int32, dkv.shape, 1)
        dkv = jnp.where(lane < head_dim, dkv * scale, dkv).astype(BF16)
        mate_copy(last).start()
        kv_local[...] = dot(dkv, hid_ref[...], TN)
        dx_acc[...] += dot(dkv, w_kvt_ref[...])
        kv_to_mate.start()
        chip_sum(last)
        kv_to_mate.wait_recv()
        kv_own[0] = kv_local[pl.ds(pl.multiple_of(side * kv_half, kv_half), kv_half), :] + kv_in[0]
        for peer in (mate, cross, other):
            halo_copy(me, peer).wait_recv()
        slot_hot = jnp.where(lax.broadcasted_iota(jnp.int32, (part_rows, 4 * halo_pair), 0) == slot_ref[...], 1.0, 0.0).astype(BF16)
        dx_acc[...] += dot(slot_hot, halo_in[...].reshape(4 * halo_pair, width))
        cross_copy(last).start()
        kv_to_cross.start()
        dx_ref[...] = (dx_acc[...] + dot(dq_all[...], w_q_ref[...].T, TN)).astype(BF16)
        for index in range(done, total):
            group_sum(index)
            if index > done:
                start_out(index - 1)
        kv_to_cross.wait_recv()
        kv_own[1] = kv_own[0] + kv_in[1]
        start_out(last)
        kv_keep.start()
        kv_back(side).start()
        for copy in dkv_copies:
            copy.wait_send()

    pl.run_scoped(
        attention_phase,
        pltpu.VMEM((2, 2 * head_dim, q_block), BF16),
        pltpu.VMEM((2, 2 * head_dim, q_block), BF16),
        pltpu.VMEM((units, 1, q_block), F32),
        pltpu.VMEM((units, 1, q_block), F32),
        pltpu.VMEM((2, key_chunk, q_block), BF16),
        pltpu.VMEM((2, key_chunk, q_block), BF16),
        pltpu.VMEM((units, head_dim, q_block), F32),
        pltpu.VMEM((width, part_rows), BF16),
        pltpu.VMEM((4, part_rows, 2 * head_dim), F32),
    )
    for copy in [kv_to_mate, kv_to_cross, kv_back(side)] + [halo_copy(peer, me) for peer in (mate, cross, other)]:
        copy.wait_send()
    kv_keep.wait()
    kv_back(1 - side).wait_recv()
    for index in range(total):
        mate_copy(index).wait_send()
        cross_copy(index).wait_send()
        keep_copy(index).wait()
        back_copy(index, side).wait_send()
        back_copy(index, 1 - side).wait_recv()


def backward(counts, o_t, lse, slots, x_feat, w_o, pre_act, y_cot, w_up, w_down, q_t, kv, kv_t, hidden_in, agg_msg, adjacency_t, w_msg, w_self, w_q, w_kv_t):
    width, rows = q_t.shape
    keys = kv.shape[0]
    head_dim = kv.shape[1] // 2
    heads = width // head_dim
    nodes = keys // rows
    q_block, key_chunk = 512, 512
    half = width // 2
    shapes = [w_up.shape, w_down.shape] + [(width, width)] * 4
    total = sum(r * c // (width * width) for r, c in shapes)
    halo_pair = slots.shape[1] // nodes
    later = (q_t, kv, kv_t, hidden_in, agg_msg, adjacency_t, w_msg, w_self, w_q, w_kv_t)
    vmem = pl.BlockSpec(memory_space=pltpu.VMEM)
    anywhere = pl.BlockSpec(memory_space=pl.ANY)
    dma = pltpu.SemaphoreType.DMA
    return pl.pallas_call(
        functools.partial(backward_kernel, head_dim, q_block, key_chunk, rows),
        out_shape=[jax.ShapeDtypeStruct((rows, width), BF16)] * 2 + [jax.ShapeDtypeStruct(shape, F32) for shape in shapes] + [jax.ShapeDtypeStruct((2 * head_dim, width), F32)],
        in_specs=[vmem] * 6 + [anywhere] * 14,
        out_specs=[vmem] * 2 + [anywhere] * 7,
        scratch_shapes=[pltpu.VMEM(a.shape, a.dtype) for a in later] + [
            pltpu.VMEM((width, rows), BF16),
            pltpu.VMEM((rows, width), BF16),
            pltpu.VMEM((rows, width), BF16),
            pltpu.VMEM((rows, width), F32),
            pltpu.VMEM((3, rows, 2 * head_dim), F32),
            pltpu.VMEM((rows, 2 * head_dim), F32),
            pltpu.VMEM((total, width, width), F32),
            pltpu.VMEM((total, half, width), F32),
            pltpu.VMEM((total, half, width), F32),
            pltpu.VMEM((2 * head_dim, width), F32),
            pltpu.VMEM((2, head_dim, width), F32),
            pltpu.VMEM((2, head_dim, width), F32),
            pltpu.VMEM((nodes, halo_pair, width), BF16),
            pltpu.VMEM((nodes, halo_pair, width), BF16),
            dma((4,)), dma((len(later),)), dma((total,)), dma((3, total)), dma((3, total)), dma((3,)), dma((3,)), dma, dma((3,)), dma((3,)), dma((nodes,)), dma((nodes,)),
        ],
        compiler_params=pltpu.CompilerParams(vmem_limit_bytes=67043328, collective_id=1, has_side_effects=True),
        cost_estimate=pl.CostEstimate(flops=10 * heads * rows * keys * head_dim, bytes_accessed=40 << 20, transcendentals=heads * rows * keys),
        name='backward',
    )(counts, o_t, lse, slots, x_feat, w_o, pre_act, y_cot, w_up, w_down, *later)


def solution(mesh):
    nodes = mesh.shape['nodes']
    row_spec = P(('graphs', 'nodes'), None)
    flat_spec = P(('graphs', 'nodes'))
    halo_spec = P(('graphs', 'nodes'), None, None)
    grad_spec = P('graphs', None)

    def device_step(x_feat, valid, halo_slot, edge_src, edge_dst, edge_mask, bal_perm, pos_enc, y_cot, w_msg, w_self, w_q, w_k, w_v, w_o, w_up, w_down):
        head_dim = w_k.shape[1]
        mixed_t, lse, slots, counts, q_t, kv, kv_t, hidden_in, agg_msg, pre_act, adjacency_t = front(bal_perm[None, :], valid[None, :], halo_slot.reshape(nodes, -1), x_feat, pos_enc, edge_src, edge_dst, edge_mask, w_q, w_k.T, w_v.T, w_msg, w_self)
        w_kv_t = jnp.concatenate([w_k.T, w_v.T], axis=0)
        y_out, dx_feat, grad_up, grad_down, grad_self, grad_msg, grad_o, grad_q, grad_kv = backward(counts, mixed_t, lse, slots, x_feat, w_o, pre_act, y_cot, w_up, w_down, q_t, kv, kv_t, hidden_in, agg_msg, adjacency_t, w_msg, w_self, w_q, w_kv_t)
        grad_k, grad_v = grad_kv[:head_dim].T, grad_kv[head_dim:].T
        return (y_out, dx_feat, grad_msg, grad_self, grad_q, grad_k, grad_v, grad_o, grad_up, grad_down)

    return jax.shard_map(device_step, mesh=mesh, in_specs=(row_spec, flat_spec, halo_spec, row_spec, row_spec, row_spec, flat_spec, row_spec, row_spec) + (P(),) * 8, out_specs=(row_spec, row_spec) + (grad_spec,) * 8, check_vma=False)
```

```python
import functools
import math

import jax
import jax.numpy as jnp
from jax import lax
from jax.experimental import pallas as pl
from jax.experimental.pallas import tpu as pltpu
from jax.sharding import PartitionSpec as P

NEG_FILL = -1e30
LOG2E = math.log2(math.e)
TAIL = 32
F32 = jnp.float32
BF16 = jnp.bfloat16
NN = (((1,), (0,)), ((), ()))
NT = (((1,), (1,)), ((), ()))
TN = (((0,), (0,)), ((), ()))
TT = (((0,), (1,)), ((), ()))


def dot(a, b, dims=NN):
    return lax.dot_general(a, b, dims, preferred_element_type=F32)


def remote(src, dst, send, recv, peer):
    return pltpu.make_async_remote_copy(src_ref=src, dst_ref=dst, send_sem=send, recv_sem=recv, device_id={'nodes': peer}, device_id_type=pl.DeviceIdType.MESH)


def neighbours():
    me = lax.axis_index('nodes')
    chip, side = me // 2, lax.rem(me, 2)
    return me, chip, side, chip * 2 + 1 - side, (1 - chip) * 2 + side, (1 - chip) * 2 + 1 - side


def meet(peers):
    barrier = pltpu.get_barrier_semaphore()
    for peer in peers:
        pl.semaphore_signal(barrier, inc=1, device_id={'nodes': peer}, device_id_type=pl.DeviceIdType.MESH)
    pl.semaphore_wait(barrier, len(peers))


CHUNKS, EDGE_STEP, POS_PIECES, KV_PIECES = 4, 512, 4, 2


def front_kernel(head_dim, perm_ref, valid_ref, halo_ref, x_hbm, pos_hbm, src_hbm, dst_hbm, on_hbm, w_q_hbm, w_kt_hbm, w_vt_hbm, w_msg_hbm, w_self_hbm, *rest):
    (out_ref, lse_ref, slot_ref, count_ref), rest = rest[:4], rest[4:]
    saved, rest = rest[:7], rest[7:]
    kept, rest = rest[:7], rest[7:]
    q_ref, kv_ref, kvt_ref, hid_ref, agg_ref, pre_ref, adj_ref = kept
    loaded, rest = rest[:10], rest[10:]
    x_ref, pos_ref, src_ref, dst_ref, on_ref, w_q_ref, w_kt_ref, w_vt_ref, w_msg_ref, w_self_ref = loaded
    w_unit, s_even, s_odd, stat, meta_ref, meta_all, pos_all, pos_acc, counts_acc, edge_acc, halo_out, halo_in, kv_all, load_sem, save_sem, meta_send, meta_recv, pos_send, pos_recv, halo_send, halo_recv, kv_send, kv_recv = rest
    rows_dev, width = x_ref.shape
    table_rows = adj_ref.shape[0]
    half = rows_dev // 2
    nodes = meta_all.shape[0]
    halo_pair = halo_in.shape[1]
    me, chip, side, mate, cross, other = neighbours()
    peers = (mate, cross, other)
    loads = [pltpu.make_async_copy(src, dst, load_sem.at[i]) for i, (src, dst) in enumerate(zip((x_hbm, pos_hbm, src_hbm, dst_hbm, on_hbm, w_q_hbm, w_kt_hbm, w_vt_hbm, w_msg_hbm, w_self_hbm), loaded))]
    saves = [pltpu.make_async_copy(src, dst, save_sem.at[i]) for i, (src, dst) in enumerate(zip(kept, saved))]
    for copy in loads:
        copy.start()
    lanes = nodes * halo_pair
    assert (nodes + 1) * lanes <= rows_dev
    meta_ref[0:1, :] = perm_ref[...]
    mine = lax.broadcasted_iota(jnp.int32, (1, lanes), 1) // halo_pair == me
    for owner in range(nodes):
        meta_ref[1:2, owner * lanes:(owner + 1) * lanes] = jnp.where(mine, jnp.concatenate([halo_ref[owner:owner + 1, :]] * nodes, axis=1), -1)
    held = jnp.sum(valid_ref[...].astype(F32), axis=1, keepdims=True).astype(jnp.int32)
    meta_ref[1:2, nodes * lanes:] = jnp.broadcast_to(held, (1, rows_dev - nodes * lanes))
    meet(peers)

    meta_copies = [remote(meta_ref, meta_all.at[me], meta_send.at[i], meta_recv.at[me], peer) for i, peer in enumerate(peers)]
    piece = rows_dev // POS_PIECES

    def pos_rows(index):
        return pl.ds(index * piece, piece)

    pos_to_cross = [remote(pos_ref.at[pos_rows(k), :], pos_all.at[me, pos_rows(k), :], pos_send.at[0, k], pos_recv.at[0, k], cross) for k in range(POS_PIECES)]
    pos_to_mate = [remote(pos_ref.at[pos_rows(k), :], pos_all.at[me, pos_rows(k), :], pos_send.at[1, k], pos_recv.at[1, k], mate) for k in range(POS_PIECES)]
    pos_relay = [remote(pos_all.at[cross, pos_rows(k), :], pos_all.at[cross, pos_rows(k), :], pos_send.at[2, k], pos_recv.at[2, k], mate) for k in range(POS_PIECES)]
    for copy in meta_copies:
        copy.start()
    loads[1].wait()
    for copy in pos_to_cross + pos_to_mate:
        copy.start()
    meta_all[me] = meta_ref[...]
    for copy in loads[:1] + loads[2:]:
        copy.wait()

    def relay_pos(k):
        pos_to_cross[k].wait_recv()
        pos_relay[k].start()

    def place_pos(owner, source, first):
        perm = meta_all[owner, 0:1, :] - me * rows_dev
        size = 256

        def body(index, carry):
            rows = pl.ds(pl.multiple_of(index * size, size), size)
            hot = jnp.where(index * size + lax.broadcasted_iota(jnp.int32, (size, rows_dev), 0) == perm, 1.0, 0.0).astype(BF16)
            part = dot(hot, source[...])
            pos_acc[rows, :] = part if first else pos_acc[rows, :] + part
            return carry

        lax.fori_loop(0, rows_dev // size, body, 0)

    edges = src_ref.shape[1]
    steps = edges // (CHUNKS * EDGE_STEP)
    assert CHUNKS * EDGE_STEP * steps == edges and EDGE_STEP * steps < 4096

    def edge_block(index):
        cols = pl.ds(pl.multiple_of(index * EDGE_STEP, EDGE_STEP), EDGE_STEP)
        src, dst, on = src_ref[:, cols], dst_ref[:, cols], on_ref[:, cols]
        upper = dst >= half
        place = jnp.where(upper, dst - half, dst)
        weight = jnp.where(on > 0, jnp.where(upper, 4096.0, 1.0), 0.0)
        src_hot = jnp.where(lax.broadcasted_iota(jnp.int32, (table_rows, EDGE_STEP), 0) == src, 1.0, 0.0).astype(BF16)
        dst_hot = jnp.where(lax.broadcasted_iota(jnp.int32, (half, EDGE_STEP), 0) == place, weight, 0.0).astype(BF16)
        return dot(src_hot, dst_hot, NT)

    def count_chunk(chunk):
        edge_acc[...] = jnp.zeros_like(edge_acc)

        def body(step, carry):
            edge_acc[...] += edge_block(chunk * steps + step)
            return carry

        lax.fori_loop(0, steps, body, 0)
        total = edge_acc[...]
        high = jnp.floor(total * (1.0 / 4096.0))
        low = total - high * 4096.0
        if chunk == 0:
            counts_acc[:, :half] = low
            counts_acc[:, half:] = high
        elif chunk < CHUNKS - 1:
            counts_acc[:, :half] += low
            counts_acc[:, half:] += high
        else:
            adj_ref[:, :half] = (counts_acc[:, :half] + low).astype(BF16)
            adj_ref[:, half:] = (counts_acc[:, half:] + high).astype(BF16)

    def halo_copy(peer, owner):
        return remote(halo_out.at[peer], halo_in.at[owner], halo_send.at[peer], halo_recv.at[owner], peer)

    count_chunk(0)
    for peer in peers:
        remote(meta_ref, meta_all.at[peer], meta_send.at[0], meta_recv.at[peer], peer).wait_recv()
    slots = jnp.full((1, lanes), -1, jnp.int32)
    for node in range(nodes):
        for owner in range(nodes):
            slots = jnp.maximum(slots, jnp.where(me == owner, meta_all[node, 1:2, owner * lanes:(owner + 1) * lanes], -1))
    slot_ref[...] = slots
    slot_hot = jnp.where(lax.broadcasted_iota(jnp.int32, (rows_dev, nodes * halo_pair), 0) == slots, 1.0, 0.0).astype(BF16)
    halo_out[...] = dot(slot_hot, x_ref[...], TN).astype(BF16).reshape(halo_out.shape)
    relay_pos(0)
    place_pos(me, pos_ref, True)
    for peer in peers:
        halo_copy(peer, me).start()
    halo_in[me] = halo_out[me]
    for node in range(nodes):
        count_ref[node:node + 1, :] = meta_all[node, 1:2, nodes * lanes:]
    count_chunk(1)
    relay_pos(1)
    for copy in pos_to_mate:
        copy.wait_recv()
    place_pos(mate, pos_all.at[mate], False)
    count_chunk(2)
    relay_pos(2)
    count_chunk(3)
    relay_pos(3)
    place_pos(cross, pos_all.at[cross], False)
    for copy in pos_relay:
        copy.wait_recv()
    place_pos(other, pos_all.at[other], False)

    hid_ref[...] = (x_ref[...].astype(F32) + pos_acc[...]).astype(BF16)
    kv_all[me] = dot(hid_ref[...], jnp.concatenate([w_kt_ref[...], w_vt_ref[...]], axis=0), NT).astype(BF16)
    q_ref[...] = dot(w_q_ref[...].T, hid_ref[...], NT).astype(BF16)
    kv_piece = rows_dev // KV_PIECES

    def kv_copy(owner, k, kind, peer):
        rows = pl.ds(k * kv_piece, kv_piece)
        return remote(kv_all.at[owner, rows, :], kv_all.at[owner, rows, :], kv_send.at[kind, k], kv_recv.at[kind, k], peer)

    kv_to_cross = [kv_copy(me, k, 0, cross) for k in range(KV_PIECES)]
    kv_to_mate = [kv_copy(me, k, 1, mate) for k in range(KV_PIECES)]
    kv_relay = [kv_copy(cross, k, 2, mate) for k in range(KV_PIECES)]
    for copy in kv_to_cross + kv_to_mate:
        copy.start()
    size = kv_all.shape[2]
    eye = jnp.where(lax.broadcasted_iota(jnp.int32, (size, size), 0) == lax.broadcasted_iota(jnp.int32, (size, size), 1), 1.0, 0.0).astype(BF16)

    def keep_kv(owner):
        rows = pl.ds(pl.multiple_of(owner * rows_dev, rows_dev), rows_dev)
        kv_ref[rows, :] = kv_all[owner]
        kvt_ref[:, rows] = dot(eye, kv_all[owner], NT).astype(BF16)

    for peer in peers:
        halo_copy(me, peer).wait_recv()
    agg = dot(adj_ref[:rows_dev, :], x_ref[...], TN) + dot(adj_ref[rows_dev:, :], halo_in[...].reshape(nodes * halo_pair, width), TN)
    agg_ref[...] = agg.astype(BF16)
    keep_kv(me)
    kv_to_cross[0].wait_recv()
    kv_relay[0].start()
    pre_ref[...] = dot(agg_ref[...], w_msg_ref[...]) + dot(x_ref[...], w_self_ref[...])
    for k in range(1, KV_PIECES):
        kv_to_cross[k].wait_recv()
        kv_relay[k].start()
    for copy in kv_to_mate:
        copy.wait_recv()
    keep_kv(mate)
    keep_kv(cross)
    for copy in kv_relay:
        copy.wait_recv()
    keep_kv(other)
    for copy in saves:
        copy.start()
    attention_forward(head_dim, rows_dev, count_ref, q_ref, kv_ref, kvt_ref, out_ref, lse_ref, w_unit, s_even, s_odd, stat)
    for copy in saves:
        copy.wait()
    for copy in meta_copies + pos_to_cross + pos_to_mate + pos_relay + [halo_copy(peer, me) for peer in peers] + kv_to_cross + kv_to_mate + kv_relay:
        copy.wait_send()


def front(perm, valid, halo_slot, x_feat, pos_enc, edge_src, edge_dst, edge_mask, w_q, w_k_t, w_v_t, w_msg, w_self):
    rows, width = x_feat.shape
    nodes, halo_pair = halo_slot.shape
    head_dim = w_k_t.shape[0]
    pair = 2 * head_dim
    heads = width // head_dim
    keys = nodes * rows
    table_rows = rows + nodes * halo_pair
    vmem = pl.BlockSpec(memory_space=pltpu.VMEM)
    anywhere = pl.BlockSpec(memory_space=pl.ANY)
    dma = pltpu.SemaphoreType.DMA
    small = [((width, rows), BF16), ((heads, rows), F32), ((1, nodes * halo_pair), jnp.int32), ((nodes, rows - nodes * nodes * halo_pair), jnp.int32)]
    saved = [((width, rows), BF16), ((keys, pair), BF16), ((pair, keys), BF16), ((rows, width), BF16), ((rows, width), BF16), ((rows, width), F32), ((table_rows, rows), BF16)]
    inputs = (x_feat, pos_enc, edge_src, edge_dst, edge_mask, w_q, w_k_t, w_v_t, w_msg, w_self)
    return pl.pallas_call(
        functools.partial(front_kernel, head_dim),
        out_shape=[jax.ShapeDtypeStruct(shape, dtype) for shape, dtype in small + saved],
        in_specs=[vmem] * 3 + [anywhere] * len(inputs),
        out_specs=[vmem] * len(small) + [anywhere] * len(saved),
        scratch_shapes=[pltpu.VMEM(shape, dtype) for shape, dtype in saved] + [pltpu.VMEM(a.shape, a.dtype) for a in inputs] + [
            pltpu.VMEM((pair, Q_BLOCK), BF16),
            pltpu.VMEM((keys, Q_BLOCK), F32),
            pltpu.VMEM((keys, Q_BLOCK), F32),
            pltpu.VMEM((8, Q_BLOCK), F32),
            pltpu.VMEM((2, rows), jnp.int32),
            pltpu.VMEM((nodes, 2, rows), jnp.int32),
            pltpu.VMEM((nodes, rows, width), BF16),
            pltpu.VMEM((rows, width), F32),
            pltpu.VMEM((table_rows, rows), F32),
            pltpu.VMEM((table_rows, rows // 2), F32),
            pltpu.VMEM((nodes, halo_pair, width), BF16),
            pltpu.VMEM((nodes, halo_pair, width), BF16),
            pltpu.VMEM((nodes, rows, pair), BF16),
            dma((len(inputs),)), dma((len(saved),)), dma((3,)), dma((nodes,)), dma((3, POS_PIECES)), dma((3, POS_PIECES)), dma((nodes,)), dma((nodes,)), dma((3, KV_PIECES)), dma((3, KV_PIECES)),
        ],
        compiler_params=pltpu.CompilerParams(vmem_limit_bytes=60 << 20, collective_id=2, has_side_effects=True),
        cost_estimate=pl.CostEstimate(flops=24 << 30, bytes_accessed=20 << 20, transcendentals=heads * rows * keys),
        name='front',
    )(perm, valid, halo_slot, *inputs)


def mask_tail(scores, chunk, key_chunk, part_rows, count_ref):
    start = chunk * key_chunk
    part = start // part_rows
    first = start - part * part_rows + key_chunk - TAIL
    row_ix = first + lax.broadcasted_iota(jnp.int32, (TAIL, scores.shape[1]), 0)
    tail = jnp.where(row_ix < count_ref[pl.ds(part, 1), :scores.shape[1]], scores[key_chunk - TAIL:, :], NEG_FILL)
    return jnp.concatenate([scores[:key_chunk - TAIL, :], tail], axis=0)


Q_BLOCK, KEY_CHUNK = 256, 1024


def attention_forward(head_dim, part_rows, count_ref, q_ref, kv_ref, kvt_ref, out_ref, lse_ref, w_q, s_even, s_odd, stat):
    heads = q_ref.shape[0] // head_dim
    blocks = q_ref.shape[1] // Q_BLOCK
    units = heads * blocks
    chunks = kv_ref.shape[0] // KEY_CHUNK
    factor = head_dim ** -0.5 * LOG2E
    groups = KEY_CHUNK // 8

    def load_weights(unit):
        head, block = unit // blocks, lax.rem(unit, blocks)
        w_q[:head_dim, :] = q_ref[pl.ds(pl.multiple_of(head * head_dim, head_dim), head_dim), pl.ds(pl.multiple_of(block * Q_BLOCK, Q_BLOCK), Q_BLOCK)]

    def score_stage(buffer, chunk, run_max):
        rows = pl.ds(pl.multiple_of(chunk * KEY_CHUNK, KEY_CHUNK), KEY_CHUNK)
        scores = mask_tail(dot(kv_ref[rows, :], w_q[...]), chunk, KEY_CHUNK, part_rows, count_ref)
        buffer[rows, :] = scores
        return jnp.maximum(run_max, jnp.max(scores.reshape(groups, 8, Q_BLOCK), axis=0))

    w_q[head_dim:, :] = jnp.zeros((w_q.shape[0] - head_dim, Q_BLOCK), BF16)
    floor = jnp.full((8, Q_BLOCK), -jnp.inf, F32)
    load_weights(0)
    stat[...] = lax.fori_loop(0, chunks, lambda chunk, run_max: score_stage(s_even, chunk, run_max), floor)

    def one_unit(unit, held, free):
        load_weights(jnp.minimum(unit + 1, units - 1))
        top = jnp.max(stat[...], axis=0, keepdims=True) * factor

        def chunk_body(chunk, state):
            run_max, run_sum, weighted = state
            cols = pl.ds(pl.multiple_of(chunk * KEY_CHUNK, KEY_CHUNK), KEY_CHUNK)
            run_max = score_stage(free, chunk, run_max)
            prob = jnp.exp2(held[cols, :] * factor - top)
            run_sum = run_sum + jnp.sum(prob.reshape(groups, 8, Q_BLOCK), axis=0)
            weighted = weighted + dot(kvt_ref[head_dim:2 * head_dim, cols], prob.astype(BF16))
            return run_max, run_sum, weighted

        run_max, run_sum, weighted = lax.fori_loop(0, chunks, chunk_body, (floor, jnp.zeros((8, Q_BLOCK), F32), jnp.zeros((head_dim, Q_BLOCK), F32)))
        stat[...] = run_max
        total = jnp.sum(run_sum, axis=0, keepdims=True)
        head, block = unit // blocks, lax.rem(unit, blocks)
        cols = pl.ds(pl.multiple_of(block * Q_BLOCK, Q_BLOCK), Q_BLOCK)
        out_ref[pl.ds(pl.multiple_of(head * head_dim, head_dim), head_dim), cols] = (weighted / total).astype(BF16)
        lse_ref[pl.ds(head, 1), cols] = top + jnp.log2(total)

    def unit_pair(pair, carry):
        one_unit(2 * pair, s_even, s_odd)
        one_unit(2 * pair + 1, s_odd, s_even)
        return carry

    lax.fori_loop(0, units // 2, unit_pair, 0)


FINAL_STEPS, FINAL_LAG = 14, 1
HOLD_STEP = 68
ROW_BLOCK = 256
GELU_A, GELU_B = math.sqrt(2.0 / math.pi), 0.044715


def backward_kernel(head_dim, q_block, key_chunk, part_rows, count_ref, o_ref, lse_ref, slot_ref, x_ref, w_o_ref, pre_hbm, cot_hbm, up_hbm, down_hbm, *rest):
    later, rest = rest[:11], rest[11:]
    row_outs, rest = rest[:2], rest[2:]
    sum_refs, kv_sum_ref, rest = rest[:6], rest[6], rest[7:]
    held, rest = rest[:11], rest[11:]
    (y_ref, dx_ref), rest = rest[:2], rest[2:]
    row_copies = [pltpu.make_async_copy(src, dst, rest[-1].at[i]) for i, (src, dst) in enumerate(zip((y_ref, dx_ref), row_outs))]
    rest = rest[:-1]
    q_ref, kv_ref, kvt_ref, hid_ref, agg_ref, adj_ref, w_msg_ref, w_self_ref, w_q_ref, w_kt_ref, w_vt_ref = held
    do_buf, dz_buf, dpre_buf, dx_acc, dkv_in, dkv_sum, local, from_mate, from_cross, kv_local, kv_own, kv_in, halo_out, halo_in, load_sem, held_sem, keep_sem, send_sem, recv_sem, dkv_send, dkv_recv, kv_sem, kv_send, kv_recv, halo_send, halo_recv = rest
    heads = q_ref.shape[0] // head_dim
    blocks = q_ref.shape[1] // q_block
    units = heads * blocks
    chunks = kv_ref.shape[0] // key_chunk
    steps = units * chunks
    per_group = steps // 4
    halves = part_rows // key_chunk
    scale = head_dim ** -0.5
    factor = scale * LOG2E
    total, width = local.shape[0], local.shape[1]
    half_rows = width // 2
    ffn_chunks = up_hbm.shape[1] // width
    first_small = 2 * ffn_chunks
    me, chip, side, mate, cross, other = neighbours()

    def block(index, half):
        if index >= first_small:
            return sum_refs[2 + index - first_small].at[pl.ds(half * half_rows, half_rows), :]
        chunk = index // 2
        if index % 2 == 0:
            return sum_refs[1].at[pl.ds(chunk * width + half * half_rows, half_rows), :]
        return sum_refs[0].at[pl.ds(half * half_rows, half_rows), pl.ds(chunk * width, width)]

    def part(index, half):
        return local.at[index, pl.ds(half * half_rows, half_rows), :]

    def to_peer(src, dst, kind, index, peer):
        return remote(src, dst, send_sem.at[kind, index], recv_sem.at[kind, index], peer)

    def mate_copy(index):
        return to_peer(part(index, 1 - side), from_mate.at[index], 0, index, mate)

    def cross_copy(index):
        return to_peer(part(index, side), from_cross.at[index], 1, index, cross)

    def back_copy(index, half):
        return to_peer(from_mate.at[index], block(index, half), 2, index, mate)

    def keep_copy(index):
        return pltpu.make_async_copy(from_mate.at[index], block(index, side), keep_sem.at[index])

    my_half = pl.ds(pl.multiple_of(side * half_rows, half_rows), half_rows)

    def chip_sum(index):
        mate_copy(index).wait_recv()
        local[index, my_half, :] = local[index, my_half, :] + from_mate[index]

    def group_sum(index):
        cross_copy(index).wait_recv()
        from_mate[index] = local[index, my_half, :] + from_cross[index]

    def start_out(index):
        keep_copy(index).start()
        back_copy(index, side).start()

    kv_half = kv_local.shape[0] // 2

    def kv_rows(half):
        return pl.ds(half * kv_half, kv_half)

    kv_to_mate = remote(kv_local.at[kv_rows(1 - side), :], kv_in.at[0], kv_send.at[0], kv_recv.at[0], mate)
    kv_to_cross = remote(kv_own.at[0], kv_in.at[1], kv_send.at[1], kv_recv.at[1], cross)
    kv_keep = pltpu.make_async_copy(kv_own.at[1], kv_sum_ref.at[kv_rows(side), :], kv_sem)

    def kv_back(half):
        return remote(kv_own.at[1], kv_sum_ref.at[kv_rows(half), :], kv_send.at[2], kv_recv.at[2], mate)

    halo_pair = halo_out.shape[1]

    def halo_copy(peer, owner):
        return remote(halo_out.at[peer], halo_in.at[owner], halo_send.at[peer], halo_recv.at[owner], peer)

    held_loads = [pltpu.make_async_copy(src, dst, held_sem.at[i]) for i, (src, dst) in enumerate(zip(later, held))]

    def ffn_phase(w_up, w_down, g_buf, z_buf, y_acc, act, d_act):
        loads = [pltpu.make_async_copy(src, dst, load_sem.at[i]) for i, (src, dst) in enumerate(((pre_hbm, dx_acc), (cot_hbm, g_buf), (up_hbm, w_up), (down_hbm, w_down)))]
        for copy in loads:
            copy.start()
        meet((mate, cross, other))
        y_acc[...] = dot(o_ref[...], w_o_ref[...], TN)
        loads[0].wait()
        pre = dx_acc[...]
        x_wide = x_ref[...].astype(F32)
        z_mid = (x_wide + jnp.maximum(pre, 0.0) + x_wide + y_acc[...].astype(BF16).astype(F32)).astype(BF16)
        dpre_buf[...] = jnp.where(pre > 0, 1.0, 0.0).astype(BF16)
        z_buf[...] = z_mid
        loads[1].wait()
        keep = lax.broadcasted_iota(jnp.int32, (part_rows, width), 0) < count_ref[pl.ds(me, 1), :width]
        g_wide = jnp.where(keep, g_buf[...].astype(F32), 0.0)
        g_buf[...] = g_wide.astype(BF16)
        dx_acc[...] = g_wide
        y_acc[...] = z_mid.astype(F32)
        loads[2].wait()
        loads[3].wait()
        for copy in held_loads:
            copy.start()

        def ffn_chunk(chunk, carry):
            cols = pl.ds(pl.multiple_of(chunk * width, width), width)

            def row_block(index, inner):
                rows = pl.ds(pl.multiple_of(index * ROW_BLOCK, ROW_BLOCK), ROW_BLOCK)
                h_pre = dot(z_buf[rows, :], w_up[:, cols])
                square = h_pre * h_pre
                bend = jnp.tanh(h_pre * (GELU_A + GELU_A * GELU_B * square))
                gate = 0.5 + 0.5 * bend
                act[rows, :] = (h_pre * gate).astype(BF16)
                slope = gate + (0.5 * h_pre) * (1.0 - bend * bend) * (GELU_A + 3.0 * GELU_A * GELU_B * square)
                d_hidden = dot(g_buf[rows, :], w_down[cols, :], NT).astype(BF16)
                d_act[rows, :] = (d_hidden.astype(F32) * slope).astype(BF16)
                y_acc[rows, :] += dot(act[rows, :], w_down[cols, :])
                dx_acc[rows, :] += dot(d_act[rows, :], w_up[:, cols], NT)
                return inner

            lax.fori_loop(0, part_rows // ROW_BLOCK, row_block, 0)
            local[2 * chunk] = dot(act[...], g_buf[...], TN)

            @pl.when(chunk > 0)
            def sum_previous():
                chip_sum(2 * chunk - 1)

            local[2 * chunk + 1] = dot(z_buf[...], d_act[...], TN)
            mate_copy(2 * chunk).start()

            @pl.when(chunk > 0)
            def send_previous():
                cross_copy(2 * chunk - 1).start()

            chip_sum(2 * chunk)
            mate_copy(2 * chunk + 1).start()
            cross_copy(2 * chunk).start()
            return carry

        lax.fori_loop(0, ffn_chunks, ffn_chunk, 0)
        y_ref[...] = jnp.where(keep, y_acc[...], 0.0).astype(BF16)

    pl.run_scoped(ffn_phase, pltpu.VMEM(up_hbm.shape, BF16), pltpu.VMEM(down_hbm.shape, BF16), pltpu.VMEM(x_ref.shape, BF16), pltpu.VMEM(x_ref.shape, BF16), pltpu.VMEM(x_ref.shape, F32), pltpu.VMEM(x_ref.shape, BF16), pltpu.VMEM(x_ref.shape, BF16))
    row_copies[0].start()
    for copy in held_loads:
        copy.wait()
    d_z = dx_acc[...].astype(BF16)
    dz_buf[...] = d_z
    dpre_buf[...] = jnp.where(dpre_buf[...] > 0, d_z, jnp.zeros_like(d_z))
    chip_sum(first_small - 1)
    do_buf[...] = dot(w_o_ref[...], dz_buf[...], NT).astype(BF16)
    cross_copy(first_small - 1).start()

    d_agg = dot(dpre_buf[...], w_msg_ref[...], NT).astype(BF16)
    halo_out[...] = dot(adj_ref[part_rows:, :], d_agg).astype(BF16).reshape(halo_out.shape)
    dx_acc[...] = 2.0 * dz_buf[...].astype(F32) + dot(dpre_buf[...], w_self_ref[...], NT)
    dx_acc[...] += dot(adj_ref[:part_rows, :], d_agg)
    for peer in (mate, cross, other):
        halo_copy(peer, me).start()
    halo_in[me] = halo_out[me]
    local[first_small] = dot(x_ref[...], dpre_buf[...], TN)
    local[first_small + 1] = dot(agg_ref[...], dpre_buf[...], TN)
    local[first_small + 2] = dot(o_ref[...], dz_buf[...])

    def attention_phase(w_q, w_do, lse_buf, delta_buf, p_buf, ds_buf, dq_acc, dq_all, dkv_acc):
        dkv_copies = [remote(src, dkv_in.at[i], dkv_send.at[i], dkv_recv.at[i], peer) for i, (src, peer) in enumerate(((dkv_acc.at[0], mate), (dkv_sum, cross), (dkv_acc.at[2], mate)))]

        def unit_spots(unit):
            head, place = unit // blocks, lax.rem(unit, blocks)
            return head, pl.ds(pl.multiple_of(head * head_dim, head_dim), head_dim), pl.ds(pl.multiple_of(place * q_block, q_block), q_block)

        def prepare(unit, carry):
            head, rows, cols = unit_spots(unit)
            delta_buf[unit] = jnp.sum(do_buf[rows, cols].astype(F32) * o_ref[rows, cols].astype(F32), axis=0, keepdims=True)
            lse_buf[unit] = lse_ref[pl.ds(head, 1), cols]
            dq_acc[unit] = jnp.zeros((head_dim, q_block), F32)
            return carry

        lax.fori_loop(0, units, prepare, 0)
        for slot in range(2):
            w_q[slot, head_dim:, :] = jnp.zeros((head_dim, q_block), BF16)
            w_do[slot, :head_dim, :] = jnp.zeros((head_dim, q_block), BF16)
        dkv_acc[...] = jnp.zeros_like(dkv_acc)

        def place_of(step):
            group = step // per_group
            chunk = step // units
            owner = lax.rem(chip + 1 - group // 2, 2) * 2 + lax.rem(side + 1 - lax.rem(group, 2), 2)
            offset = lax.rem(chunk, halves) * key_chunk
            rows = pl.ds(pl.multiple_of(owner * part_rows + offset, key_chunk), key_chunk)
            return group, owner, offset, rows, lax.rem(step, units), lax.rem(step, 2)

        def first_stage(step):
            group, owner, offset, rows, unit, slot = place_of(step)
            head, unit_rows, cols = unit_spots(unit)
            w_q[slot, :head_dim, :] = q_ref[unit_rows, cols]
            w_do[slot, head_dim:, :] = do_buf[unit_rows, cols]
            kv = kv_ref[rows, :]
            scores = dot(kv, w_q[slot])
            row_ix = offset + key_chunk - TAIL + lax.broadcasted_iota(jnp.int32, (TAIL, q_block), 0)
            tail = jnp.where(row_ix < count_ref[pl.ds(owner, 1), :q_block], scores[key_chunk - TAIL:, :], NEG_FILL)
            scores = jnp.concatenate([scores[:key_chunk - TAIL, :], tail], axis=0)
            prob = jnp.exp2(scores * factor - lse_buf[unit])
            p_buf[slot] = prob.astype(BF16)
            ds_buf[slot] = (prob * (dot(kv, w_do[slot]) - delta_buf[unit])).astype(BF16)

        def second_stage(step):
            group, owner, offset, rows, unit, slot = place_of(step)
            d_scores = ds_buf[slot]
            spot = pl.ds(pl.multiple_of(offset, key_chunk), key_chunk)
            dkv_acc[group, spot, :] += dot(d_scores, w_q[slot], NT) + dot(p_buf[slot], w_do[slot], NT)
            dq_acc[unit] += dot(kvt_ref[:head_dim, rows], d_scores)

        def exchange(step):
            held = jnp.logical_and(step >= HOLD_STEP, step < HOLD_STEP + 12)
            turn = (step - HOLD_STEP) // 4 + first_small
            phase = lax.rem(step, 4)

            @pl.when(jnp.logical_and(held, phase == 1))
            def sum_chip():
                chip_sum(turn)

            @pl.when(jnp.logical_and(held, phase == 2))
            def send_cross():
                cross_copy(turn).start()

            lap, beat = step // FINAL_STEPS - FINAL_LAG, lax.rem(step, FINAL_STEPS)

            @pl.when(jnp.logical_and(lap >= 0, beat == 0))
            def sum_group():
                group_sum(lap)

            @pl.when(jnp.logical_and(lap >= 0, beat == 1))
            def send_back():
                for k in range(done):
                    @pl.when(lap == k)
                    def start_piece(k=k):
                        start_out(k)

            @pl.when(step == 3)
            def small_pieces():
                for index in range(first_small, total - 1):
                    mate_copy(index).start()

            @pl.when(step == per_group + 1)
            def first_group():
                dkv_copies[0].start()

            @pl.when(step == 2 * per_group + 1)
            def second_group():
                dkv_copies[0].wait_recv()
                dkv_sum[...] = dkv_acc[1] + dkv_in[0]

            @pl.when(step == 2 * per_group + 2)
            def send_second():
                dkv_copies[1].start()

            @pl.when(step == 3 * per_group + 1)
            def third_group():
                dkv_copies[2].start()

        done = (steps - 1) // FINAL_STEPS - FINAL_LAG + 1
        assert (steps - 1) % FINAL_STEPS >= 1 and 0 < done < total - 2 and HOLD_STEP > 2 * per_group + 2 and HOLD_STEP % 4 == 0

        first_stage(0)

        def body(step, carry):
            exchange(step)
            second_stage(step - 1)
            first_stage(step)
            return carry

        lax.fori_loop(1, steps, body, 0)
        second_stage(steps - 1)

        def gather_dq(unit, carry):
            head, rows, cols = unit_spots(unit)
            dq_all[rows, cols] = (dq_acc[unit] * scale).astype(BF16)
            return carry

        lax.fori_loop(0, units, gather_dq, 0)
        last = total - 1
        local[last] = dot(dq_all[...], hid_ref[...]).T
        dkv_copies[2].wait_recv()
        dkv_copies[1].wait_recv()
        dkv = dkv_acc[3] + dkv_in[2] + dkv_in[1]
        lane = lax.broadcasted_iota(jnp.int32, dkv.shape, 1)
        dkv = jnp.where(lane < head_dim, dkv * scale, dkv).astype(BF16)
        mate_copy(last).start()
        kv_local[...] = dot(dkv, hid_ref[...], TN)
        dx_acc[...] += dot(dkv, jnp.concatenate([w_kt_ref[...], w_vt_ref[...]], axis=0))
        kv_to_mate.start()
        chip_sum(last)
        kv_to_mate.wait_recv()
        kv_own[0] = kv_local[pl.ds(pl.multiple_of(side * kv_half, kv_half), kv_half), :] + kv_in[0]
        for peer in (mate, cross, other):
            halo_copy(me, peer).wait_recv()
        slot_hot = jnp.where(lax.broadcasted_iota(jnp.int32, (part_rows, 4 * halo_pair), 0) == slot_ref[...], 1.0, 0.0).astype(BF16)
        dx_acc[...] += dot(slot_hot, halo_in[...].reshape(4 * halo_pair, width))
        cross_copy(last).start()
        kv_to_cross.start()
        dx_ref[...] = (dx_acc[...] + dot(dq_all[...], w_q_ref[...].T, TN)).astype(BF16)
        for index in range(done, total):
            group_sum(index)
            if index == done:
                row_copies[1].start()
            else:
                start_out(index - 1)
        kv_to_cross.wait_recv()
        kv_own[1] = kv_own[0] + kv_in[1]
        start_out(last)
        kv_keep.start()
        kv_back(side).start()
        for copy in dkv_copies:
            copy.wait_send()

    pl.run_scoped(
        attention_phase,
        pltpu.VMEM((2, 2 * head_dim, q_block), BF16),
        pltpu.VMEM((2, 2 * head_dim, q_block), BF16),
        pltpu.VMEM((units, 1, q_block), F32),
        pltpu.VMEM((units, 1, q_block), F32),
        pltpu.VMEM((2, key_chunk, q_block), BF16),
        pltpu.VMEM((2, key_chunk, q_block), BF16),
        pltpu.VMEM((units, head_dim, q_block), F32),
        pltpu.VMEM((width, part_rows), BF16),
        pltpu.VMEM((4, part_rows, 2 * head_dim), F32),
    )
    for copy in [kv_to_mate, kv_to_cross, kv_back(side)] + [halo_copy(peer, me) for peer in (mate, cross, other)]:
        copy.wait_send()
    for copy in row_copies:
        copy.wait()
    kv_keep.wait()
    kv_back(1 - side).wait_recv()
    for index in range(total):
        mate_copy(index).wait_send()
        cross_copy(index).wait_send()
        keep_copy(index).wait()
        back_copy(index, side).wait_send()
        back_copy(index, 1 - side).wait_recv()


def backward(counts, o_t, lse, slots, x_feat, w_o, pre_act, y_cot, w_up, w_down, q_t, kv, kv_t, hidden_in, agg_msg, adjacency_t, w_msg, w_self, w_q, w_k_t, w_v_t):
    width, rows = q_t.shape
    keys = kv.shape[0]
    head_dim = kv.shape[1] // 2
    heads = width // head_dim
    nodes = keys // rows
    q_block, key_chunk = 512, 512
    half = width // 2
    shapes = [w_up.shape, w_down.shape] + [(width, width)] * 4
    total = sum(r * c // (width * width) for r, c in shapes)
    halo_pair = slots.shape[1] // nodes
    later = (q_t, kv, kv_t, hidden_in, agg_msg, adjacency_t, w_msg, w_self, w_q, w_k_t, w_v_t)
    vmem = pl.BlockSpec(memory_space=pltpu.VMEM)
    anywhere = pl.BlockSpec(memory_space=pl.ANY)
    dma = pltpu.SemaphoreType.DMA
    return pl.pallas_call(
        functools.partial(backward_kernel, head_dim, q_block, key_chunk, rows),
        out_shape=[jax.ShapeDtypeStruct((rows, width), BF16)] * 2 + [jax.ShapeDtypeStruct(shape, F32) for shape in shapes] + [jax.ShapeDtypeStruct((2 * head_dim, width), F32)],
        in_specs=[vmem] * 6 + [anywhere] * 15,
        out_specs=[anywhere] * 9,
        scratch_shapes=[pltpu.VMEM(a.shape, a.dtype) for a in later] + [
            pltpu.VMEM((rows, width), BF16),
            pltpu.VMEM((rows, width), BF16),
            pltpu.VMEM((width, rows), BF16),
            pltpu.VMEM((rows, width), BF16),
            pltpu.VMEM((rows, width), BF16),
            pltpu.VMEM((rows, width), F32),
            pltpu.VMEM((3, rows, 2 * head_dim), F32),
            pltpu.VMEM((rows, 2 * head_dim), F32),
            pltpu.VMEM((total, width, width), F32),
            pltpu.VMEM((total, half, width), F32),
            pltpu.VMEM((total, half, width), F32),
            pltpu.VMEM((2 * head_dim, width), F32),
            pltpu.VMEM((2, head_dim, width), F32),
            pltpu.VMEM((2, head_dim, width), F32),
            pltpu.VMEM((nodes, halo_pair, width), BF16),
            pltpu.VMEM((nodes, halo_pair, width), BF16),
            dma((4,)), dma((len(later),)), dma((total,)), dma((3, total)), dma((3, total)), dma((3,)), dma((3,)), dma, dma((3,)), dma((3,)), dma((nodes,)), dma((nodes,)), dma((2,)),
        ],
        compiler_params=pltpu.CompilerParams(vmem_limit_bytes=67043328, collective_id=1, has_side_effects=True),
        cost_estimate=pl.CostEstimate(flops=10 * heads * rows * keys * head_dim, bytes_accessed=40 << 20, transcendentals=heads * rows * keys),
        name='backward',
    )(counts, o_t, lse, slots, x_feat, w_o, pre_act, y_cot, w_up, w_down, *later)


def finish_kernel(plan, *refs):
    inputs = plan[-1][0] + 1
    sources, rest = refs[:inputs], refs[inputs:]
    outputs = plan[-1][1] + 1
    targets, rest = rest[:outputs], rest[outputs:]
    buffers, in_sem, out_sem = rest[:-2], rest[-2], rest[-1]
    gets = [pltpu.make_async_copy(sources[i].at[pl.ds(src, n), :], buf, in_sem.at[k]) for k, ((i, j, src, dst, n), buf) in enumerate(zip(plan, buffers))]
    puts = [pltpu.make_async_copy(buf, targets[j].at[pl.ds(dst, n), :], out_sem.at[k]) for k, ((i, j, src, dst, n), buf) in enumerate(zip(plan, buffers))]
    for copy in gets:
        copy.start()
    for get, put in zip(gets, puts):
        get.wait()
        put.start()
    for copy in puts:
        copy.wait()


def finish(*arrays):
    plan, shapes = [], []
    for i, a in enumerate(arrays):
        last = i == len(arrays) - 1
        step = a.shape[0] // 2 if last else min(a.shape[0], (1 << 20) // (a.shape[1] * a.dtype.itemsize))
        for start in range(0, a.shape[0], step):
            j = i + (start // step if last else 0)
            plan.append((i, j, start, 0 if last else start, step))
        shapes += [jax.ShapeDtypeStruct((step, a.shape[1]), a.dtype)] * 2 if last else [jax.ShapeDtypeStruct(a.shape, a.dtype)]
    anywhere = pl.BlockSpec(memory_space=pl.ANY)
    return pl.pallas_call(
        functools.partial(finish_kernel, plan),
        out_shape=shapes,
        in_specs=[anywhere] * len(arrays),
        out_specs=[anywhere] * len(shapes),
        scratch_shapes=[pltpu.VMEM((n, arrays[i].shape[1]), arrays[i].dtype) for i, j, src, dst, n in plan] + [pltpu.SemaphoreType.DMA((len(plan),))] * 2,
        compiler_params=pltpu.CompilerParams(vmem_limit_bytes=67043328),
        cost_estimate=pl.CostEstimate(flops=1 << 20, bytes_accessed=30 << 20, transcendentals=0),
        name='finish',
    )(*arrays)


def solution(mesh):
    nodes = mesh.shape['nodes']
    row_spec = P(('graphs', 'nodes'), None)
    flat_spec = P(('graphs', 'nodes'))
    halo_spec = P(('graphs', 'nodes'), None, None)
    grad_spec = P('graphs', None)

    def device_step(x_feat, valid, halo_slot, edge_src, edge_dst, edge_mask, bal_perm, pos_enc, y_cot, w_msg, w_self, w_q, w_k, w_v, w_o, w_up, w_down):
        head_dim = w_k.shape[1]
        mixed_t, lse, slots, counts, q_t, kv, kv_t, hidden_in, agg_msg, pre_act, adjacency_t = front(bal_perm[None, :], valid[None, :], halo_slot.reshape(nodes, -1), x_feat, pos_enc, edge_src, edge_dst, edge_mask, w_q, w_k.T, w_v.T, w_msg, w_self)
        results = backward(counts, mixed_t, lse, slots, x_feat, w_o, pre_act, y_cot, w_up, w_down, q_t, kv, kv_t, hidden_in, agg_msg, adjacency_t, w_msg, w_self, w_q, w_k.T, w_v.T)
        y_out, dx_feat, grad_up, grad_down, grad_self, grad_msg, grad_o, grad_q, grad_k, grad_v = finish(*results)
        return (y_out, dx_feat, grad_msg, grad_self, grad_q, grad_k.T, grad_v.T, grad_o, grad_up, grad_down)

    return jax.shard_map(device_step, mesh=mesh, in_specs=(row_spec, flat_spec, halo_spec, row_spec, row_spec, row_spec, flat_spec, row_spec, row_spec) + (P(),) * 8, out_specs=(row_spec, row_spec) + (grad_spec,) * 8, check_vma=False)
```

```python
import functools
import math

import jax
import jax.numpy as jnp
from jax import lax
from jax.experimental import pallas as pl
from jax.experimental.pallas import tpu as pltpu
from jax.sharding import PartitionSpec as P

NEG_FILL = -1e30
LOG2E = math.log2(math.e)
TAIL = 32
F32 = jnp.float32
BF16 = jnp.bfloat16
NN = (((1,), (0,)), ((), ()))
NT = (((1,), (1,)), ((), ()))
TN = (((0,), (0,)), ((), ()))
TT = (((0,), (1,)), ((), ()))


def dot(a, b, dims=NN):
    return lax.dot_general(a, b, dims, preferred_element_type=F32)


def remote(src, dst, send, recv, peer):
    return pltpu.make_async_remote_copy(src_ref=src, dst_ref=dst, send_sem=send, recv_sem=recv, device_id={'nodes': peer}, device_id_type=pl.DeviceIdType.MESH)


def neighbours():
    me = lax.axis_index('nodes')
    chip, side = me // 2, lax.rem(me, 2)
    return me, chip, side, chip * 2 + 1 - side, (1 - chip) * 2 + side, (1 - chip) * 2 + 1 - side


def meet(peers):
    barrier = pltpu.get_barrier_semaphore()
    for peer in peers:
        pl.semaphore_signal(barrier, inc=1, device_id={'nodes': peer}, device_id_type=pl.DeviceIdType.MESH)
    pl.semaphore_wait(barrier, len(peers))


CHUNKS, EDGE_STEP, POS_PIECES, KV_PIECES = 4, 512, 4, 2


def front_kernel(head_dim, perm_ref, valid_ref, halo_ref, x_hbm, pos_hbm, src_hbm, dst_hbm, on_hbm, w_q_hbm, w_kt_hbm, w_vt_hbm, w_msg_hbm, w_self_hbm, *rest):
    (out_ref, lse_ref, slot_ref, count_ref), rest = rest[:4], rest[4:]
    saved, rest = rest[:7], rest[7:]
    kept, rest = rest[:7], rest[7:]
    q_ref, kv_ref, kvt_ref, hid_ref, agg_ref, pre_ref, adj_ref = kept
    loaded, rest = rest[:10], rest[10:]
    x_ref, pos_ref, src_ref, dst_ref, on_ref, w_q_ref, w_kt_ref, w_vt_ref, w_msg_ref, w_self_ref = loaded
    w_unit, s_even, s_odd, stat, meta_ref, meta_all, pos_all, pos_acc, counts_acc, edge_acc, halo_out, halo_in, kv_all, load_sem, save_sem, meta_send, meta_recv, pos_send, pos_recv, halo_send, halo_recv, kv_send, kv_recv = rest
    rows_dev, width = x_ref.shape
    table_rows = adj_ref.shape[0]
    half = rows_dev // 2
    nodes = meta_all.shape[0]
    halo_pair = halo_in.shape[1]
    me, chip, side, mate, cross, other = neighbours()
    peers = (mate, cross, other)
    loads = [pltpu.make_async_copy(src, dst, load_sem.at[i]) for i, (src, dst) in enumerate(zip((x_hbm, pos_hbm, src_hbm, dst_hbm, on_hbm, w_q_hbm, w_kt_hbm, w_vt_hbm, w_msg_hbm, w_self_hbm), loaded))]
    saves = [pltpu.make_async_copy(src, dst, save_sem.at[i]) for i, (src, dst) in enumerate(zip(kept, saved))]
    for copy in loads:
        copy.start()
    lanes = nodes * halo_pair
    assert (nodes + 1) * lanes <= rows_dev
    meta_ref[0:1, :] = perm_ref[...]
    mine = lax.broadcasted_iota(jnp.int32, (1, lanes), 1) // halo_pair == me
    for owner in range(nodes):
        meta_ref[1:2, owner * lanes:(owner + 1) * lanes] = jnp.where(mine, jnp.concatenate([halo_ref[owner:owner + 1, :]] * nodes, axis=1), -1)
    held = jnp.sum(valid_ref[...].astype(F32), axis=1, keepdims=True).astype(jnp.int32)
    meta_ref[1:2, nodes * lanes:] = jnp.broadcast_to(held, (1, rows_dev - nodes * lanes))
    meet(peers)

    meta_copies = [remote(meta_ref, meta_all.at[me], meta_send.at[i], meta_recv.at[me], peer) for i, peer in enumerate(peers)]
    piece = rows_dev // POS_PIECES

    def pos_rows(index):
        return pl.ds(index * piece, piece)

    pos_to_cross = [remote(pos_ref.at[pos_rows(k), :], pos_all.at[me, pos_rows(k), :], pos_send.at[0, k], pos_recv.at[0, k], cross) for k in range(POS_PIECES)]
    pos_to_mate = [remote(pos_ref.at[pos_rows(k), :], pos_all.at[me, pos_rows(k), :], pos_send.at[1, k], pos_recv.at[1, k], mate) for k in range(POS_PIECES)]
    pos_relay = [remote(pos_all.at[cross, pos_rows(k), :], pos_all.at[cross, pos_rows(k), :], pos_send.at[2, k], pos_recv.at[2, k], mate) for k in range(POS_PIECES)]
    for copy in meta_copies:
        copy.start()
    loads[1].wait()
    for copy in pos_to_cross + pos_to_mate:
        copy.start()
    meta_all[me] = meta_ref[...]
    for copy in loads[:1] + loads[2:]:
        copy.wait()

    def relay_pos(k):
        pos_to_cross[k].wait_recv()
        pos_relay[k].start()

    def place_pos(owner, source, first):
        perm = meta_all[owner, 0:1, :] - me * rows_dev
        size = 256

        def body(index, carry):
            rows = pl.ds(pl.multiple_of(index * size, size), size)
            hot = jnp.where(index * size + lax.broadcasted_iota(jnp.int32, (size, rows_dev), 0) == perm, 1.0, 0.0).astype(BF16)
            part = dot(hot, source[...])
            pos_acc[rows, :] = part if first else pos_acc[rows, :] + part
            return carry

        lax.fori_loop(0, rows_dev // size, body, 0)

    edges = src_ref.shape[1]
    steps = edges // (CHUNKS * EDGE_STEP)
    assert CHUNKS * EDGE_STEP * steps == edges and EDGE_STEP * steps < 4096

    def edge_block(index):
        cols = pl.ds(pl.multiple_of(index * EDGE_STEP, EDGE_STEP), EDGE_STEP)
        src, dst, on = src_ref[:, cols], dst_ref[:, cols], on_ref[:, cols]
        upper = dst >= half
        place = jnp.where(upper, dst - half, dst)
        weight = jnp.where(on > 0, jnp.where(upper, 4096.0, 1.0), 0.0)
        src_hot = jnp.where(lax.broadcasted_iota(jnp.int32, (table_rows, EDGE_STEP), 0) == src, 1.0, 0.0).astype(BF16)
        dst_hot = jnp.where(lax.broadcasted_iota(jnp.int32, (half, EDGE_STEP), 0) == place, weight, 0.0).astype(BF16)
        return dot(src_hot, dst_hot, NT)

    def count_chunk(chunk):
        edge_acc[...] = jnp.zeros_like(edge_acc)

        def body(step, carry):
            edge_acc[...] += edge_block(chunk * steps + step)
            return carry

        lax.fori_loop(0, steps, body, 0)
        total = edge_acc[...]
        high = jnp.floor(total * (1.0 / 4096.0))
        low = total - high * 4096.0
        if chunk == 0:
            counts_acc[:, :half] = low
            counts_acc[:, half:] = high
        elif chunk < CHUNKS - 1:
            counts_acc[:, :half] += low
            counts_acc[:, half:] += high
        else:
            adj_ref[:, :half] = (counts_acc[:, :half] + low).astype(BF16)
            adj_ref[:, half:] = (counts_acc[:, half:] + high).astype(BF16)

    def halo_copy(peer, owner):
        return remote(halo_out.at[peer], halo_in.at[owner], halo_send.at[peer], halo_recv.at[owner], peer)

    count_chunk(0)
    for peer in peers:
        remote(meta_ref, meta_all.at[peer], meta_send.at[0], meta_recv.at[peer], peer).wait_recv()
    slots = jnp.full((1, lanes), -1, jnp.int32)
    for node in range(nodes):
        for owner in range(nodes):
            slots = jnp.maximum(slots, jnp.where(me == owner, meta_all[node, 1:2, owner * lanes:(owner + 1) * lanes], -1))
    slot_ref[...] = slots
    slot_hot = jnp.where(lax.broadcasted_iota(jnp.int32, (rows_dev, nodes * halo_pair), 0) == slots, 1.0, 0.0).astype(BF16)
    halo_out[...] = dot(slot_hot, x_ref[...], TN).astype(BF16).reshape(halo_out.shape)
    relay_pos(0)
    place_pos(me, pos_ref, True)
    for peer in peers:
        halo_copy(peer, me).start()
    halo_in[me] = halo_out[me]
    for node in range(nodes):
        count_ref[node:node + 1, :] = meta_all[node, 1:2, nodes * lanes:]
    count_chunk(1)
    relay_pos(1)
    for copy in pos_to_mate:
        copy.wait_recv()
    place_pos(mate, pos_all.at[mate], False)
    count_chunk(2)
    relay_pos(2)
    count_chunk(3)
    relay_pos(3)
    place_pos(cross, pos_all.at[cross], False)
    for copy in pos_relay:
        copy.wait_recv()
    place_pos(other, pos_all.at[other], False)

    hid_ref[...] = (x_ref[...].astype(F32) + pos_acc[...]).astype(BF16)
    kv_all[me] = dot(hid_ref[...], jnp.concatenate([w_kt_ref[...], w_vt_ref[...]], axis=0), NT).astype(BF16)
    q_ref[...] = dot(w_q_ref[...].T, hid_ref[...], NT).astype(BF16)
    kv_piece = rows_dev // KV_PIECES

    def kv_copy(owner, k, kind, peer):
        rows = pl.ds(k * kv_piece, kv_piece)
        return remote(kv_all.at[owner, rows, :], kv_all.at[owner, rows, :], kv_send.at[kind, k], kv_recv.at[kind, k], peer)

    kv_to_cross = [kv_copy(me, k, 0, cross) for k in range(KV_PIECES)]
    kv_to_mate = [kv_copy(me, k, 1, mate) for k in range(KV_PIECES)]
    kv_relay = [kv_copy(cross, k, 2, mate) for k in range(KV_PIECES)]
    for copy in kv_to_cross + kv_to_mate:
        copy.start()
    size = kv_all.shape[2]
    eye = jnp.where(lax.broadcasted_iota(jnp.int32, (size, size), 0) == lax.broadcasted_iota(jnp.int32, (size, size), 1), 1.0, 0.0).astype(BF16)

    def keep_kv(owner):
        rows = pl.ds(pl.multiple_of(owner * rows_dev, rows_dev), rows_dev)
        kv_ref[rows, :] = kv_all[owner]
        kvt_ref[:, rows] = dot(eye, kv_all[owner], NT).astype(BF16)

    for peer in peers:
        halo_copy(me, peer).wait_recv()
    agg = dot(adj_ref[:rows_dev, :], x_ref[...], TN) + dot(adj_ref[rows_dev:, :], halo_in[...].reshape(nodes * halo_pair, width), TN)
    agg_ref[...] = agg.astype(BF16)
    keep_kv(me)
    kv_to_cross[0].wait_recv()
    kv_relay[0].start()
    pre_ref[...] = dot(agg_ref[...], w_msg_ref[...]) + dot(x_ref[...], w_self_ref[...])
    for k in range(1, KV_PIECES):
        kv_to_cross[k].wait_recv()
        kv_relay[k].start()
    for copy in kv_to_mate:
        copy.wait_recv()
    keep_kv(mate)
    keep_kv(cross)
    for copy in kv_relay:
        copy.wait_recv()
    keep_kv(other)
    for copy in saves:
        copy.start()
    attention_forward(head_dim, rows_dev, count_ref, q_ref, kv_ref, kvt_ref, out_ref, lse_ref, w_unit, s_even, s_odd, stat)
    for copy in saves:
        copy.wait()
    for copy in meta_copies + pos_to_cross + pos_to_mate + pos_relay + [halo_copy(peer, me) for peer in peers] + kv_to_cross + kv_to_mate + kv_relay:
        copy.wait_send()


def front(perm, valid, halo_slot, x_feat, pos_enc, edge_src, edge_dst, edge_mask, w_q, w_k_t, w_v_t, w_msg, w_self):
    rows, width = x_feat.shape
    nodes, halo_pair = halo_slot.shape
    head_dim = w_k_t.shape[0]
    pair = 2 * head_dim
    heads = width // head_dim
    keys = nodes * rows
    table_rows = rows + nodes * halo_pair
    vmem = pl.BlockSpec(memory_space=pltpu.VMEM)
    anywhere = pl.BlockSpec(memory_space=pl.ANY)
    dma = pltpu.SemaphoreType.DMA
    small = [((width, rows), BF16), ((heads, rows), F32), ((1, nodes * halo_pair), jnp.int32), ((nodes, rows - nodes * nodes * halo_pair), jnp.int32)]
    saved = [((width, rows), BF16), ((keys, pair), BF16), ((pair, keys), BF16), ((rows, width), BF16), ((rows, width), BF16), ((rows, width), F32), ((table_rows, rows), BF16)]
    inputs = (x_feat, pos_enc, edge_src, edge_dst, edge_mask, w_q, w_k_t, w_v_t, w_msg, w_self)
    return pl.pallas_call(
        functools.partial(front_kernel, head_dim),
        out_shape=[jax.ShapeDtypeStruct(shape, dtype) for shape, dtype in small + saved],
        in_specs=[vmem] * 3 + [anywhere] * len(inputs),
        out_specs=[vmem] * len(small) + [anywhere] * len(saved),
        scratch_shapes=[pltpu.VMEM(shape, dtype) for shape, dtype in saved] + [pltpu.VMEM(a.shape, a.dtype) for a in inputs] + [
            pltpu.VMEM((pair, Q_BLOCK), BF16),
            pltpu.VMEM((keys, Q_BLOCK), F32),
            pltpu.VMEM((keys, Q_BLOCK), F32),
            pltpu.VMEM((8, Q_BLOCK), F32),
            pltpu.VMEM((2, rows), jnp.int32),
            pltpu.VMEM((nodes, 2, rows), jnp.int32),
            pltpu.VMEM((nodes, rows, width), BF16),
            pltpu.VMEM((rows, width), F32),
            pltpu.VMEM((table_rows, rows), F32),
            pltpu.VMEM((table_rows, rows // 2), F32),
            pltpu.VMEM((nodes, halo_pair, width), BF16),
            pltpu.VMEM((nodes, halo_pair, width), BF16),
            pltpu.VMEM((nodes, rows, pair), BF16),
            dma((len(inputs),)), dma((len(saved),)), dma((3,)), dma((nodes,)), dma((3, POS_PIECES)), dma((3, POS_PIECES)), dma((nodes,)), dma((nodes,)), dma((3, KV_PIECES)), dma((3, KV_PIECES)),
        ],
        compiler_params=pltpu.CompilerParams(vmem_limit_bytes=60 << 20, collective_id=2, has_side_effects=True),
        cost_estimate=pl.CostEstimate(flops=24 << 30, bytes_accessed=20 << 20, transcendentals=heads * rows * keys),
        name='front',
    )(perm, valid, halo_slot, *inputs)


def mask_tail(scores, chunk, key_chunk, part_rows, count_ref):
    start = chunk * key_chunk
    part = start // part_rows
    first = start - part * part_rows + key_chunk - TAIL
    row_ix = first + lax.broadcasted_iota(jnp.int32, (TAIL, scores.shape[1]), 0)
    tail = jnp.where(row_ix < count_ref[pl.ds(part, 1), :scores.shape[1]], scores[key_chunk - TAIL:, :], NEG_FILL)
    return jnp.concatenate([scores[:key_chunk - TAIL, :], tail], axis=0)


Q_BLOCK, KEY_CHUNK, UNROLL = 256, 1024, 2


def attention_forward(head_dim, part_rows, count_ref, q_ref, kv_ref, kvt_ref, out_ref, lse_ref, w_q, s_even, s_odd, stat):
    heads = q_ref.shape[0] // head_dim
    blocks = q_ref.shape[1] // Q_BLOCK
    units = heads * blocks
    chunks = kv_ref.shape[0] // KEY_CHUNK
    factor = head_dim ** -0.5 * LOG2E
    groups = KEY_CHUNK // 8

    def load_weights(unit):
        head, block = unit // blocks, lax.rem(unit, blocks)
        w_q[:head_dim, :] = q_ref[pl.ds(pl.multiple_of(head * head_dim, head_dim), head_dim), pl.ds(pl.multiple_of(block * Q_BLOCK, Q_BLOCK), Q_BLOCK)]

    def score_stage(buffer, chunk, run_max):
        rows = pl.ds(pl.multiple_of(chunk * KEY_CHUNK, KEY_CHUNK), KEY_CHUNK)
        scores = mask_tail(dot(kv_ref[rows, :], w_q[...]), chunk, KEY_CHUNK, part_rows, count_ref)
        buffer[rows, :] = scores
        return jnp.maximum(run_max, jnp.max(scores.reshape(groups, 8, Q_BLOCK), axis=0))

    w_q[head_dim:, :] = jnp.zeros((w_q.shape[0] - head_dim, Q_BLOCK), BF16)
    floor = jnp.full((8, Q_BLOCK), -jnp.inf, F32)
    load_weights(0)
    stat[...] = lax.fori_loop(0, chunks, lambda chunk, run_max: score_stage(s_even, chunk, run_max), floor)

    def one_unit(unit, held, free):
        load_weights(jnp.minimum(unit + 1, units - 1))
        top = jnp.max(stat[...], axis=0, keepdims=True) * factor

        def chunk_body(index, state):
            run_max, run_sum, weighted = state
            for k in range(UNROLL):
                chunk = index * UNROLL + k
                run_max = score_stage(free, chunk, run_max)
                cols = pl.ds(pl.multiple_of(chunk * KEY_CHUNK, KEY_CHUNK), KEY_CHUNK)
                prob = jnp.exp2(held[cols, :] * factor - top)
                run_sum = run_sum + jnp.sum(prob.reshape(groups, 8, Q_BLOCK), axis=0)
                weighted = weighted + dot(kvt_ref[head_dim:2 * head_dim, cols], prob.astype(BF16))
            return run_max, run_sum, weighted

        run_max, run_sum, weighted = lax.fori_loop(0, chunks // UNROLL, chunk_body, (floor, jnp.zeros((8, Q_BLOCK), F32), jnp.zeros((head_dim, Q_BLOCK), F32)))
        stat[...] = run_max
        total = jnp.sum(run_sum, axis=0, keepdims=True)
        head, block = unit // blocks, lax.rem(unit, blocks)
        cols = pl.ds(pl.multiple_of(block * Q_BLOCK, Q_BLOCK), Q_BLOCK)
        out_ref[pl.ds(pl.multiple_of(head * head_dim, head_dim), head_dim), cols] = (weighted / total).astype(BF16)
        lse_ref[pl.ds(head, 1), cols] = top + jnp.log2(total)

    def unit_pair(pair, carry):
        one_unit(2 * pair, s_even, s_odd)
        one_unit(2 * pair + 1, s_odd, s_even)
        return carry

    lax.fori_loop(0, units // 2, unit_pair, 0)


FINAL_STEPS, FINAL_LAG = 14, 1
HOLD_STEP = 68
ROW_BLOCK = 256
GELU_A, GELU_B = math.sqrt(2.0 / math.pi), 0.044715


def backward_kernel(head_dim, q_block, key_chunk, part_rows, count_ref, lse_ref, slot_ref, o_hbm, x_hbm, w_o_hbm, pre_hbm, cot_hbm, up_hbm, down_hbm, *rest):
    later, rest = rest[:11], rest[11:]
    row_outs, rest = rest[:2], rest[2:]
    sum_refs, kv_sum_ref, rest = rest[:6], rest[6], rest[7:]
    held, rest = rest[:11], rest[11:]
    (y_ref, dx_ref, o_ref, x_ref, w_o_ref), rest = rest[:5], rest[5:]
    row_copies = [pltpu.make_async_copy(src, dst, rest[-1].at[i]) for i, (src, dst) in enumerate(zip((y_ref, dx_ref), row_outs))]
    rest = rest[:-1]
    q_ref, kv_ref, kvt_ref, hid_ref, agg_ref, adj_ref, w_msg_ref, w_self_ref, w_q_ref, w_kt_ref, w_vt_ref = held
    do_buf, dz_buf, dpre_buf, dx_acc, dkv_in, dkv_sum, local, from_mate, from_cross, kv_local, kv_own, kv_in, halo_out, halo_in, load_sem, held_sem, keep_sem, send_sem, recv_sem, dkv_send, dkv_recv, kv_sem, kv_send, kv_recv, halo_send, halo_recv = rest
    heads = q_ref.shape[0] // head_dim
    blocks = q_ref.shape[1] // q_block
    units = heads * blocks
    chunks = kv_ref.shape[0] // key_chunk
    steps = units * chunks
    per_group = steps // 4
    halves = part_rows // key_chunk
    scale = head_dim ** -0.5
    factor = scale * LOG2E
    total, width = local.shape[0], local.shape[1]
    half_rows = width // 2
    ffn_chunks = up_hbm.shape[1] // width
    first_small = 2 * ffn_chunks
    me, chip, side, mate, cross, other = neighbours()

    def block(index, half):
        if index >= first_small:
            return sum_refs[2 + index - first_small].at[pl.ds(half * half_rows, half_rows), :]
        chunk = index // 2
        if index % 2 == 0:
            return sum_refs[1].at[pl.ds(chunk * width + half * half_rows, half_rows), :]
        return sum_refs[0].at[pl.ds(half * half_rows, half_rows), pl.ds(chunk * width, width)]

    def part(index, half):
        return local.at[index, pl.ds(half * half_rows, half_rows), :]

    def to_peer(src, dst, kind, index, peer):
        return remote(src, dst, send_sem.at[kind, index], recv_sem.at[kind, index], peer)

    def mate_copy(index):
        return to_peer(part(index, 1 - side), from_mate.at[index], 0, index, mate)

    def cross_copy(index):
        return to_peer(part(index, side), from_cross.at[index], 1, index, cross)

    def back_copy(index, half):
        return to_peer(from_mate.at[index], block(index, half), 2, index, mate)

    def keep_copy(index):
        return pltpu.make_async_copy(from_mate.at[index], block(index, side), keep_sem.at[index])

    my_half = pl.ds(pl.multiple_of(side * half_rows, half_rows), half_rows)

    def chip_sum(index):
        mate_copy(index).wait_recv()
        local[index, my_half, :] = local[index, my_half, :] + from_mate[index]

    def group_sum(index):
        cross_copy(index).wait_recv()
        from_mate[index] = local[index, my_half, :] + from_cross[index]

    def start_out(index):
        keep_copy(index).start()
        back_copy(index, side).start()

    kv_half = kv_local.shape[0] // 2

    def kv_rows(half):
        return pl.ds(half * kv_half, kv_half)

    kv_to_mate = remote(kv_local.at[kv_rows(1 - side), :], kv_in.at[0], kv_send.at[0], kv_recv.at[0], mate)
    kv_to_cross = remote(kv_own.at[0], kv_in.at[1], kv_send.at[1], kv_recv.at[1], cross)
    kv_keep = pltpu.make_async_copy(kv_own.at[1], kv_sum_ref.at[kv_rows(side), :], kv_sem)

    def kv_back(half):
        return remote(kv_own.at[1], kv_sum_ref.at[kv_rows(half), :], kv_send.at[2], kv_recv.at[2], mate)

    halo_pair = halo_out.shape[1]

    def halo_copy(peer, owner):
        return remote(halo_out.at[peer], halo_in.at[owner], halo_send.at[peer], halo_recv.at[owner], peer)

    held_loads = [pltpu.make_async_copy(src, dst, held_sem.at[i]) for i, (src, dst) in enumerate(zip(later, held))]

    def ffn_phase(w_up, w_down, g_buf, z_buf, y_acc, act, d_act):
        loads = [pltpu.make_async_copy(src, dst, load_sem.at[i]) for i, (src, dst) in enumerate(((o_hbm, o_ref), (w_o_hbm, w_o_ref), (x_hbm, x_ref), (pre_hbm, dx_acc), (cot_hbm, g_buf), (up_hbm, w_up), (down_hbm, w_down)))]
        for copy in loads:
            copy.start()
        meet((mate, cross, other))
        loads[0].wait()
        loads[1].wait()
        y_acc[...] = dot(o_ref[...], w_o_ref[...], TN)
        loads[2].wait()
        loads[3].wait()
        pre = dx_acc[...]
        x_wide = x_ref[...].astype(F32)
        z_mid = (x_wide + jnp.maximum(pre, 0.0) + x_wide + y_acc[...].astype(BF16).astype(F32)).astype(BF16)
        dpre_buf[...] = jnp.where(pre > 0, 1.0, 0.0).astype(BF16)
        z_buf[...] = z_mid
        loads[4].wait()
        keep = lax.broadcasted_iota(jnp.int32, (part_rows, width), 0) < count_ref[pl.ds(me, 1), :width]
        g_wide = jnp.where(keep, g_buf[...].astype(F32), 0.0)
        g_buf[...] = g_wide.astype(BF16)
        dx_acc[...] = g_wide
        y_acc[...] = z_mid.astype(F32)
        loads[5].wait()
        loads[6].wait()

        def ffn_chunk(chunk, carry):
            cols = pl.ds(pl.multiple_of(chunk * width, width), width)

            def act_block(index, inner):
                rows = pl.ds(pl.multiple_of(index * ROW_BLOCK, ROW_BLOCK), ROW_BLOCK)
                h_pre = dot(z_buf[rows, :], w_up[:, cols])
                bend = jnp.tanh(h_pre * (GELU_A + GELU_A * GELU_B * (h_pre * h_pre)))
                act[rows, :] = (h_pre * (0.5 + 0.5 * bend)).astype(BF16)
                return inner

            def row_block(index, inner):
                rows = pl.ds(pl.multiple_of(index * ROW_BLOCK, ROW_BLOCK), ROW_BLOCK)
                h_pre = dot(z_buf[rows, :], w_up[:, cols])
                square = h_pre * h_pre
                bend = jnp.tanh(h_pre * (GELU_A + GELU_A * GELU_B * square))
                slope = 0.5 + 0.5 * bend + (0.5 * h_pre) * (1.0 - bend * bend) * (GELU_A + 3.0 * GELU_A * GELU_B * square)
                d_hidden = dot(g_buf[rows, :], w_down[cols, :], NT).astype(BF16)
                d_act[rows, :] = (d_hidden.astype(F32) * slope).astype(BF16)
                y_acc[rows, :] += dot(act[rows, :], w_down[cols, :])
                dx_acc[rows, :] += dot(d_act[rows, :], w_up[:, cols], NT)
                return inner

            lax.fori_loop(0, part_rows // ROW_BLOCK, act_block, 0)
            local[2 * chunk] = dot(act[...], g_buf[...], TN)

            @pl.when(chunk == 0)
            def load_later():
                for copy in held_loads:
                    copy.start()

            @pl.when(chunk > 0)
            def sum_previous():
                chip_sum(2 * chunk - 1)

            row_block(0, 0)
            mate_copy(2 * chunk).start()

            @pl.when(chunk > 0)
            def send_previous():
                cross_copy(2 * chunk - 1).start()

            row_block(1, 0)
            chip_sum(2 * chunk)
            row_block(2, 0)
            cross_copy(2 * chunk).start()
            lax.fori_loop(3, part_rows // ROW_BLOCK, row_block, 0)
            local[2 * chunk + 1] = dot(z_buf[...], d_act[...], TN)
            mate_copy(2 * chunk + 1).start()
            return carry

        lax.fori_loop(0, ffn_chunks, ffn_chunk, 0)
        y_ref[...] = jnp.where(keep, y_acc[...], 0.0).astype(BF16)

    pl.run_scoped(ffn_phase, pltpu.VMEM(up_hbm.shape, BF16), pltpu.VMEM(down_hbm.shape, BF16), pltpu.VMEM(x_ref.shape, BF16), pltpu.VMEM(x_ref.shape, BF16), pltpu.VMEM(x_ref.shape, F32), pltpu.VMEM(x_ref.shape, BF16), pltpu.VMEM(x_ref.shape, BF16))
    row_copies[0].start()
    for copy in held_loads:
        copy.wait()
    d_z = dx_acc[...].astype(BF16)
    dz_buf[...] = d_z
    dpre_buf[...] = jnp.where(dpre_buf[...] > 0, d_z, jnp.zeros_like(d_z))
    chip_sum(first_small - 1)
    do_buf[...] = dot(w_o_ref[...], dz_buf[...], NT).astype(BF16)
    cross_copy(first_small - 1).start()

    d_agg = dot(dpre_buf[...], w_msg_ref[...], NT).astype(BF16)
    halo_out[...] = dot(adj_ref[part_rows:, :], d_agg).astype(BF16).reshape(halo_out.shape)
    dx_acc[...] = 2.0 * dz_buf[...].astype(F32) + dot(dpre_buf[...], w_self_ref[...], NT)
    dx_acc[...] += dot(adj_ref[:part_rows, :], d_agg)
    for peer in (mate, cross, other):
        halo_copy(peer, me).start()
    halo_in[me] = halo_out[me]
    local[first_small] = dot(x_ref[...], dpre_buf[...], TN)
    local[first_small + 1] = dot(agg_ref[...], dpre_buf[...], TN)
    local[first_small + 2] = dot(o_ref[...], dz_buf[...])

    def attention_phase(w_q, w_do, lse_buf, delta_buf, p_buf, ds_buf, dq_acc, dq_all, dkv_acc):
        dkv_copies = [remote(src, dkv_in.at[i], dkv_send.at[i], dkv_recv.at[i], peer) for i, (src, peer) in enumerate(((dkv_acc.at[0], mate), (dkv_sum, cross), (dkv_acc.at[2], mate)))]

        def unit_spots(unit):
            head, place = unit // blocks, lax.rem(unit, blocks)
            return head, pl.ds(pl.multiple_of(head * head_dim, head_dim), head_dim), pl.ds(pl.multiple_of(place * q_block, q_block), q_block)

        def prepare(unit, carry):
            head, rows, cols = unit_spots(unit)
            delta_buf[unit] = jnp.sum(do_buf[rows, cols].astype(F32) * o_ref[rows, cols].astype(F32), axis=0, keepdims=True)
            lse_buf[unit] = lse_ref[pl.ds(head, 1), cols]
            dq_acc[unit] = jnp.zeros((head_dim, q_block), F32)
            return carry

        lax.fori_loop(0, units, prepare, 0)
        for slot in range(2):
            w_q[slot, head_dim:, :] = jnp.zeros((head_dim, q_block), BF16)
            w_do[slot, :head_dim, :] = jnp.zeros((head_dim, q_block), BF16)
        dkv_acc[...] = jnp.zeros_like(dkv_acc)

        def place_of(step):
            group = step // per_group
            chunk = step // units
            owner = lax.rem(chip + 1 - group // 2, 2) * 2 + lax.rem(side + 1 - lax.rem(group, 2), 2)
            offset = lax.rem(chunk, halves) * key_chunk
            rows = pl.ds(pl.multiple_of(owner * part_rows + offset, key_chunk), key_chunk)
            return group, owner, offset, rows, lax.rem(step, units), lax.rem(step, 2)

        def first_stage(step):
            group, owner, offset, rows, unit, slot = place_of(step)
            head, unit_rows, cols = unit_spots(unit)
            w_q[slot, :head_dim, :] = q_ref[unit_rows, cols]
            w_do[slot, head_dim:, :] = do_buf[unit_rows, cols]
            kv = kv_ref[rows, :]
            scores = dot(kv, w_q[slot])
            row_ix = offset + key_chunk - TAIL + lax.broadcasted_iota(jnp.int32, (TAIL, q_block), 0)
            tail = jnp.where(row_ix < count_ref[pl.ds(owner, 1), :q_block], scores[key_chunk - TAIL:, :], NEG_FILL)
            scores = jnp.concatenate([scores[:key_chunk - TAIL, :], tail], axis=0)
            prob = jnp.exp2(scores * factor - lse_buf[unit])
            p_buf[slot] = prob.astype(BF16)
            ds_buf[slot] = (prob * (dot(kv, w_do[slot]) - delta_buf[unit])).astype(BF16)

        def second_stage(step):
            group, owner, offset, rows, unit, slot = place_of(step)
            d_scores = ds_buf[slot]
            spot = pl.ds(pl.multiple_of(offset, key_chunk), key_chunk)
            dkv_acc[group, spot, :] += dot(d_scores, w_q[slot], NT) + dot(p_buf[slot], w_do[slot], NT)
            dq_acc[unit] += dot(kvt_ref[:head_dim, rows], d_scores)

        def exchange(step):
            held = jnp.logical_and(step >= HOLD_STEP, step < HOLD_STEP + 12)
            turn = (step - HOLD_STEP) // 4 + first_small
            phase = lax.rem(step, 4)

            @pl.when(jnp.logical_and(held, phase == 1))
            def sum_chip():
                chip_sum(turn)

            @pl.when(jnp.logical_and(held, phase == 2))
            def send_cross():
                cross_copy(turn).start()

            lap, beat = step // FINAL_STEPS - FINAL_LAG, lax.rem(step, FINAL_STEPS)

            @pl.when(jnp.logical_and(lap >= 0, beat == 0))
            def sum_group():
                group_sum(lap)

            @pl.when(jnp.logical_and(lap >= 0, beat == 1))
            def send_back():
                for k in range(done):
                    @pl.when(lap == k)
                    def start_piece(k=k):
                        start_out(k)

            @pl.when(step == 3)
            def small_pieces():
                for index in range(first_small, total - 1):
                    mate_copy(index).start()

            @pl.when(step == per_group + 1)
            def first_group():
                dkv_copies[0].start()

            @pl.when(step == 2 * per_group + 1)
            def second_group():
                dkv_copies[0].wait_recv()
                dkv_sum[...] = dkv_acc[1] + dkv_in[0]

            @pl.when(step == 2 * per_group + 2)
            def send_second():
                dkv_copies[1].start()

            @pl.when(step == 3 * per_group + 1)
            def third_group():
                dkv_copies[2].start()

        done = (steps - 1) // FINAL_STEPS - FINAL_LAG + 1
        assert (steps - 1) % FINAL_STEPS >= 1 and 0 < done < total - 2 and HOLD_STEP > 2 * per_group + 2 and HOLD_STEP % 4 == 0

        first_stage(0)

        def body(step, carry):
            exchange(step)
            second_stage(step - 1)
            first_stage(step)
            return carry

        lax.fori_loop(1, steps, body, 0)
        second_stage(steps - 1)

        def gather_dq(unit, carry):
            head, rows, cols = unit_spots(unit)
            dq_all[rows, cols] = (dq_acc[unit] * scale).astype(BF16)
            return carry

        lax.fori_loop(0, units, gather_dq, 0)
        last = total - 1
        local[last] = dot(dq_all[...], hid_ref[...]).T
        dkv_copies[2].wait_recv()
        dkv_copies[1].wait_recv()
        dkv = dkv_acc[3] + dkv_in[2] + dkv_in[1]
        lane = lax.broadcasted_iota(jnp.int32, dkv.shape, 1)
        dkv = jnp.where(lane < head_dim, dkv * scale, dkv).astype(BF16)
        mate_copy(last).start()
        kv_local[...] = dot(dkv, hid_ref[...], TN)
        dx_acc[...] += dot(dkv, jnp.concatenate([w_kt_ref[...], w_vt_ref[...]], axis=0))
        kv_to_mate.start()
        chip_sum(last)
        kv_to_mate.wait_recv()
        kv_own[0] = kv_local[pl.ds(pl.multiple_of(side * kv_half, kv_half), kv_half), :] + kv_in[0]
        for peer in (mate, cross, other):
            halo_copy(me, peer).wait_recv()
        slot_hot = jnp.where(lax.broadcasted_iota(jnp.int32, (part_rows, 4 * halo_pair), 0) == slot_ref[...], 1.0, 0.0).astype(BF16)
        dx_acc[...] += dot(slot_hot, halo_in[...].reshape(4 * halo_pair, width))
        cross_copy(last).start()
        kv_to_cross.start()
        dx_ref[...] = (dx_acc[...] + dot(dq_all[...], w_q_ref[...].T, TN)).astype(BF16)
        for index in range(done, total):
            group_sum(index)
            if index == done:
                row_copies[1].start()
            else:
                start_out(index - 1)
        kv_to_cross.wait_recv()
        kv_own[1] = kv_own[0] + kv_in[1]
        start_out(last)
        kv_keep.start()
        kv_back(side).start()
        for copy in dkv_copies:
            copy.wait_send()

    pl.run_scoped(
        attention_phase,
        pltpu.VMEM((2, 2 * head_dim, q_block), BF16),
        pltpu.VMEM((2, 2 * head_dim, q_block), BF16),
        pltpu.VMEM((units, 1, q_block), F32),
        pltpu.VMEM((units, 1, q_block), F32),
        pltpu.VMEM((2, key_chunk, q_block), BF16),
        pltpu.VMEM((2, key_chunk, q_block), BF16),
        pltpu.VMEM((units, head_dim, q_block), F32),
        pltpu.VMEM((width, part_rows), BF16),
        pltpu.VMEM((4, part_rows, 2 * head_dim), F32),
    )
    for copy in [kv_to_mate, kv_to_cross, kv_back(side)] + [halo_copy(peer, me) for peer in (mate, cross, other)]:
        copy.wait_send()
    for copy in row_copies:
        copy.wait()
    kv_keep.wait()
    kv_back(1 - side).wait_recv()
    for index in range(total):
        mate_copy(index).wait_send()
        cross_copy(index).wait_send()
        keep_copy(index).wait()
        back_copy(index, side).wait_send()
        back_copy(index, 1 - side).wait_recv()


def backward(counts, o_t, lse, slots, x_feat, w_o, pre_act, y_cot, w_up, w_down, q_t, kv, kv_t, hidden_in, agg_msg, adjacency_t, w_msg, w_self, w_q, w_k_t, w_v_t):
    width, rows = q_t.shape
    keys = kv.shape[0]
    head_dim = kv.shape[1] // 2
    heads = width // head_dim
    nodes = keys // rows
    q_block, key_chunk = 512, 512
    half = width // 2
    shapes = [w_up.shape, w_down.shape] + [(width, width)] * 4
    total = sum(r * c // (width * width) for r, c in shapes)
    halo_pair = slots.shape[1] // nodes
    later = (q_t, kv, kv_t, hidden_in, agg_msg, adjacency_t, w_msg, w_self, w_q, w_k_t, w_v_t)
    vmem = pl.BlockSpec(memory_space=pltpu.VMEM)
    anywhere = pl.BlockSpec(memory_space=pl.ANY)
    dma = pltpu.SemaphoreType.DMA
    return pl.pallas_call(
        functools.partial(backward_kernel, head_dim, q_block, key_chunk, rows),
        out_shape=[jax.ShapeDtypeStruct((rows, width), BF16)] * 2 + [jax.ShapeDtypeStruct(shape, F32) for shape in shapes] + [jax.ShapeDtypeStruct((2 * head_dim, width), F32)],
        in_specs=[vmem] * 3 + [anywhere] * 18,
        out_specs=[anywhere] * 9,
        scratch_shapes=[pltpu.VMEM(a.shape, a.dtype) for a in later] + [
            pltpu.VMEM((rows, width), BF16),
            pltpu.VMEM((rows, width), BF16),
            pltpu.VMEM((width, rows), BF16),
            pltpu.VMEM((rows, width), BF16),
            pltpu.VMEM((width, width), BF16),
            pltpu.VMEM((width, rows), BF16),
            pltpu.VMEM((rows, width), BF16),
            pltpu.VMEM((rows, width), BF16),
            pltpu.VMEM((rows, width), F32),
            pltpu.VMEM((3, rows, 2 * head_dim), F32),
            pltpu.VMEM((rows, 2 * head_dim), F32),
            pltpu.VMEM((total, width, width), F32),
            pltpu.VMEM((total, half, width), F32),
            pltpu.VMEM((total, half, width), F32),
            pltpu.VMEM((2 * head_dim, width), F32),
            pltpu.VMEM((2, head_dim, width), F32),
            pltpu.VMEM((2, head_dim, width), F32),
            pltpu.VMEM((nodes, halo_pair, width), BF16),
            pltpu.VMEM((nodes, halo_pair, width), BF16),
            dma((7,)), dma((len(later),)), dma((total,)), dma((3, total)), dma((3, total)), dma((3,)), dma((3,)), dma, dma((3,)), dma((3,)), dma((nodes,)), dma((nodes,)), dma((2,)),
        ],
        compiler_params=pltpu.CompilerParams(vmem_limit_bytes=67043328, collective_id=1, has_side_effects=True),
        cost_estimate=pl.CostEstimate(flops=10 * heads * rows * keys * head_dim, bytes_accessed=40 << 20, transcendentals=heads * rows * keys),
        name='backward',
    )(counts, lse, slots, o_t, x_feat, w_o, pre_act, y_cot, w_up, w_down, *later)


def finish_kernel(plan, *refs):
    inputs = plan[-1][0] + 1
    sources, rest = refs[:inputs], refs[inputs:]
    outputs = plan[-1][1] + 1
    targets, rest = rest[:outputs], rest[outputs:]
    buffers, in_sem, out_sem = rest[:-2], rest[-2], rest[-1]
    gets = [pltpu.make_async_copy(sources[i].at[pl.ds(src, n), :], buf, in_sem.at[k]) for k, ((i, j, src, dst, n), buf) in enumerate(zip(plan, buffers))]
    puts = [pltpu.make_async_copy(buf, targets[j].at[pl.ds(dst, n), :], out_sem.at[k]) for k, ((i, j, src, dst, n), buf) in enumerate(zip(plan, buffers))]
    for copy in gets:
        copy.start()
    for get, put in zip(gets, puts):
        get.wait()
        put.start()
    for copy in puts:
        copy.wait()


def finish(*arrays):
    plan, shapes = [], []
    for i, a in enumerate(arrays):
        last = i == len(arrays) - 1
        step = a.shape[0] // 2 if last else min(a.shape[0], (1 << 20) // (a.shape[1] * a.dtype.itemsize))
        for start in range(0, a.shape[0], step):
            j = i + (start // step if last else 0)
            plan.append((i, j, start, 0 if last else start, step))
        shapes += [jax.ShapeDtypeStruct((step, a.shape[1]), a.dtype)] * 2 if last else [jax.ShapeDtypeStruct(a.shape, a.dtype)]
    anywhere = pl.BlockSpec(memory_space=pl.ANY)
    return pl.pallas_call(
        functools.partial(finish_kernel, plan),
        out_shape=shapes,
        in_specs=[anywhere] * len(arrays),
        out_specs=[anywhere] * len(shapes),
        scratch_shapes=[pltpu.VMEM((n, arrays[i].shape[1]), arrays[i].dtype) for i, j, src, dst, n in plan] + [pltpu.SemaphoreType.DMA((len(plan),))] * 2,
        compiler_params=pltpu.CompilerParams(vmem_limit_bytes=67043328),
        cost_estimate=pl.CostEstimate(flops=1 << 20, bytes_accessed=30 << 20, transcendentals=0),
        name='finish',
    )(*arrays)


def solution(mesh):
    nodes = mesh.shape['nodes']
    row_spec = P(('graphs', 'nodes'), None)
    flat_spec = P(('graphs', 'nodes'))
    halo_spec = P(('graphs', 'nodes'), None, None)
    grad_spec = P('graphs', None)

    def device_step(x_feat, valid, halo_slot, edge_src, edge_dst, edge_mask, bal_perm, pos_enc, y_cot, w_msg, w_self, w_q, w_k, w_v, w_o, w_up, w_down):
        head_dim = w_k.shape[1]
        mixed_t, lse, slots, counts, q_t, kv, kv_t, hidden_in, agg_msg, pre_act, adjacency_t = front(bal_perm[None, :], valid[None, :], halo_slot.reshape(nodes, -1), x_feat, pos_enc, edge_src, edge_dst, edge_mask, w_q, w_k.T, w_v.T, w_msg, w_self)
        results = backward(counts, mixed_t, lse, slots, x_feat, w_o, pre_act, y_cot, w_up, w_down, q_t, kv, kv_t, hidden_in, agg_msg, adjacency_t, w_msg, w_self, w_q, w_k.T, w_v.T)
        y_out, dx_feat, grad_up, grad_down, grad_self, grad_msg, grad_o, grad_q, grad_k, grad_v = finish(*results)
        return (y_out, dx_feat, grad_msg, grad_self, grad_q, grad_k.T, grad_v.T, grad_o, grad_up, grad_down)

    return jax.shard_map(device_step, mesh=mesh, in_specs=(row_spec, flat_spec, halo_spec, row_spec, row_spec, row_spec, flat_spec, row_spec, row_spec) + (P(),) * 8, out_specs=(row_spec, row_spec) + (grad_spec,) * 8, check_vma=False)
```

```python
import functools
import math

import jax
import jax.numpy as jnp
from jax import lax
from jax.experimental import pallas as pl
from jax.experimental.pallas import tpu as pltpu
from jax.sharding import PartitionSpec as P

NEG_FILL = -1e30
LOG2E = math.log2(math.e)
TAIL = 32
F32 = jnp.float32
BF16 = jnp.bfloat16
NN = (((1,), (0,)), ((), ()))
NT = (((1,), (1,)), ((), ()))
TN = (((0,), (0,)), ((), ()))
TT = (((0,), (1,)), ((), ()))


def dot(a, b, dims=NN):
    return lax.dot_general(a, b, dims, preferred_element_type=F32)


def remote(src, dst, send, recv, peer):
    return pltpu.make_async_remote_copy(src_ref=src, dst_ref=dst, send_sem=send, recv_sem=recv, device_id={'nodes': peer}, device_id_type=pl.DeviceIdType.MESH)


def neighbours():
    me = lax.axis_index('nodes')
    chip, side = me // 2, lax.rem(me, 2)
    return me, chip, side, chip * 2 + 1 - side, (1 - chip) * 2 + side, (1 - chip) * 2 + 1 - side


def meet(peers):
    barrier = pltpu.get_barrier_semaphore()
    for peer in peers:
        pl.semaphore_signal(barrier, inc=1, device_id={'nodes': peer}, device_id_type=pl.DeviceIdType.MESH)
    pl.semaphore_wait(barrier, len(peers))


CHUNKS, EDGE_STEP, POS_PIECES, KV_PIECES = 4, 512, 4, 2


def front_kernel(head_dim, perm_ref, valid_ref, halo_ref, x_hbm, pos_hbm, src_hbm, dst_hbm, on_hbm, w_q_hbm, w_kt_hbm, w_vt_hbm, w_msg_hbm, w_self_hbm, *rest):
    (out_ref, lse_ref, slot_ref, count_ref), rest = rest[:4], rest[4:]
    saved, rest = rest[:7], rest[7:]
    kept, rest = rest[:7], rest[7:]
    q_ref, kv_ref, kvt_ref, hid_ref, agg_ref, pre_ref, adj_ref = kept
    loaded, rest = rest[:10], rest[10:]
    x_ref, pos_ref, src_ref, dst_ref, on_ref, w_q_ref, w_kt_ref, w_vt_ref, w_msg_ref, w_self_ref = loaded
    w_unit, s_even, s_odd, stat, meta_ref, meta_all, pos_all, pos_acc, counts_acc, edge_acc, halo_out, halo_in, kv_all, load_sem, save_sem, meta_send, meta_recv, pos_send, pos_recv, halo_send, halo_recv, kv_send, kv_recv = rest
    rows_dev, width = x_ref.shape
    table_rows = adj_ref.shape[0]
    half = rows_dev // 2
    nodes = meta_all.shape[0]
    halo_pair = halo_in.shape[1]
    me, chip, side, mate, cross, other = neighbours()
    peers = (mate, cross, other)
    loads = [pltpu.make_async_copy(src, dst, load_sem.at[i]) for i, (src, dst) in enumerate(zip((x_hbm, pos_hbm, src_hbm, dst_hbm, on_hbm, w_q_hbm, w_kt_hbm, w_vt_hbm, w_msg_hbm, w_self_hbm), loaded))]
    saves = [pltpu.make_async_copy(src, dst, save_sem.at[i]) for i, (src, dst) in enumerate(zip(kept, saved))]
    for copy in loads:
        copy.start()
    lanes = nodes * halo_pair
    assert (nodes + 1) * lanes <= rows_dev
    meta_ref[0:1, :] = perm_ref[...]
    mine = lax.broadcasted_iota(jnp.int32, (1, lanes), 1) // halo_pair == me
    for owner in range(nodes):
        meta_ref[1:2, owner * lanes:(owner + 1) * lanes] = jnp.where(mine, jnp.concatenate([halo_ref[owner:owner + 1, :]] * nodes, axis=1), -1)
    held = jnp.sum(valid_ref[...].astype(F32), axis=1, keepdims=True).astype(jnp.int32)
    meta_ref[1:2, nodes * lanes:] = jnp.broadcast_to(held, (1, rows_dev - nodes * lanes))
    meet(peers)

    meta_copies = [remote(meta_ref, meta_all.at[me], meta_send.at[i], meta_recv.at[me], peer) for i, peer in enumerate(peers)]
    piece = rows_dev // POS_PIECES

    def pos_rows(index):
        return pl.ds(index * piece, piece)

    pos_to_cross = [remote(pos_ref.at[pos_rows(k), :], pos_all.at[me, pos_rows(k), :], pos_send.at[0, k], pos_recv.at[0, k], cross) for k in range(POS_PIECES)]
    pos_to_mate = [remote(pos_ref.at[pos_rows(k), :], pos_all.at[me, pos_rows(k), :], pos_send.at[1, k], pos_recv.at[1, k], mate) for k in range(POS_PIECES)]
    pos_relay = [remote(pos_all.at[cross, pos_rows(k), :], pos_all.at[cross, pos_rows(k), :], pos_send.at[2, k], pos_recv.at[2, k], mate) for k in range(POS_PIECES)]
    for copy in meta_copies:
        copy.start()
    loads[1].wait()
    for copy in pos_to_cross + pos_to_mate:
        copy.start()
    meta_all[me] = meta_ref[...]
    for copy in loads[:1] + loads[2:]:
        copy.wait()

    def relay_pos(k):
        pos_to_cross[k].wait_recv()
        pos_relay[k].start()

    def place_pos(owner, source, first):
        perm = meta_all[owner, 0:1, :] - me * rows_dev
        size = 256

        def body(index, carry):
            rows = pl.ds(pl.multiple_of(index * size, size), size)
            hot = jnp.where(index * size + lax.broadcasted_iota(jnp.int32, (size, rows_dev), 0) == perm, 1.0, 0.0).astype(BF16)
            part = dot(hot, source[...])
            pos_acc[rows, :] = part if first else pos_acc[rows, :] + part
            return carry

        lax.fori_loop(0, rows_dev // size, body, 0)

    edges = src_ref.shape[1]
    steps = edges // (CHUNKS * EDGE_STEP)
    assert CHUNKS * EDGE_STEP * steps == edges and EDGE_STEP * steps < 4096

    def edge_block(index):
        cols = pl.ds(pl.multiple_of(index * EDGE_STEP, EDGE_STEP), EDGE_STEP)
        src, dst, on = src_ref[:, cols], dst_ref[:, cols], on_ref[:, cols]
        upper = dst >= half
        place = jnp.where(upper, dst - half, dst)
        weight = jnp.where(on > 0, jnp.where(upper, 4096.0, 1.0), 0.0)
        src_hot = jnp.where(lax.broadcasted_iota(jnp.int32, (table_rows, EDGE_STEP), 0) == src, 1.0, 0.0).astype(BF16)
        dst_hot = jnp.where(lax.broadcasted_iota(jnp.int32, (half, EDGE_STEP), 0) == place, weight, 0.0).astype(BF16)
        return dot(src_hot, dst_hot, NT)

    def count_chunk(chunk):
        edge_acc[...] = jnp.zeros_like(edge_acc)

        def body(step, carry):
            edge_acc[...] += edge_block(chunk * steps + step)
            return carry

        lax.fori_loop(0, steps, body, 0)
        total = edge_acc[...]
        high = jnp.floor(total * (1.0 / 4096.0))
        low = total - high * 4096.0
        if chunk == 0:
            counts_acc[:, :half] = low
            counts_acc[:, half:] = high
        elif chunk < CHUNKS - 1:
            counts_acc[:, :half] += low
            counts_acc[:, half:] += high
        else:
            adj_ref[:, :half] = (counts_acc[:, :half] + low).astype(BF16)
            adj_ref[:, half:] = (counts_acc[:, half:] + high).astype(BF16)

    def halo_copy(peer, owner):
        return remote(halo_out.at[peer], halo_in.at[owner], halo_send.at[peer], halo_recv.at[owner], peer)

    count_chunk(0)
    for peer in peers:
        remote(meta_ref, meta_all.at[peer], meta_send.at[0], meta_recv.at[peer], peer).wait_recv()
    slots = jnp.full((1, lanes), -1, jnp.int32)
    for node in range(nodes):
        for owner in range(nodes):
            slots = jnp.maximum(slots, jnp.where(me == owner, meta_all[node, 1:2, owner * lanes:(owner + 1) * lanes], -1))
    slot_ref[...] = slots
    slot_hot = jnp.where(lax.broadcasted_iota(jnp.int32, (rows_dev, nodes * halo_pair), 0) == slots, 1.0, 0.0).astype(BF16)
    halo_out[...] = dot(slot_hot, x_ref[...], TN).astype(BF16).reshape(halo_out.shape)
    relay_pos(0)
    place_pos(me, pos_ref, True)
    for peer in peers:
        halo_copy(peer, me).start()
    halo_in[me] = halo_out[me]
    for node in range(nodes):
        count_ref[node:node + 1, :] = meta_all[node, 1:2, nodes * lanes:]
    count_chunk(1)
    relay_pos(1)
    for copy in pos_to_mate:
        copy.wait_recv()
    place_pos(mate, pos_all.at[mate], False)
    count_chunk(2)
    relay_pos(2)
    count_chunk(3)
    relay_pos(3)
    place_pos(cross, pos_all.at[cross], False)
    for copy in pos_relay:
        copy.wait_recv()
    place_pos(other, pos_all.at[other], False)

    hid_ref[...] = (x_ref[...].astype(F32) + pos_acc[...]).astype(BF16)
    kv_all[me] = dot(hid_ref[...], jnp.concatenate([w_kt_ref[...], w_vt_ref[...]], axis=0), NT).astype(BF16)
    q_ref[...] = dot(w_q_ref[...].T, hid_ref[...], NT).astype(BF16)
    kv_piece = rows_dev // KV_PIECES

    def kv_copy(owner, k, kind, peer):
        rows = pl.ds(k * kv_piece, kv_piece)
        return remote(kv_all.at[owner, rows, :], kv_all.at[owner, rows, :], kv_send.at[kind, k], kv_recv.at[kind, k], peer)

    kv_to_cross = [kv_copy(me, k, 0, cross) for k in range(KV_PIECES)]
    kv_to_mate = [kv_copy(me, k, 1, mate) for k in range(KV_PIECES)]
    kv_relay = [kv_copy(cross, k, 2, mate) for k in range(KV_PIECES)]
    for copy in kv_to_cross + kv_to_mate:
        copy.start()
    size = kv_all.shape[2]
    eye = jnp.where(lax.broadcasted_iota(jnp.int32, (size, size), 0) == lax.broadcasted_iota(jnp.int32, (size, size), 1), 1.0, 0.0).astype(BF16)

    def keep_kv(owner):
        rows = pl.ds(pl.multiple_of(owner * rows_dev, rows_dev), rows_dev)
        kv_ref[rows, :] = kv_all[owner]
        kvt_ref[:, rows] = dot(eye, kv_all[owner], NT).astype(BF16)

    for peer in peers:
        halo_copy(me, peer).wait_recv()
    agg = dot(adj_ref[:rows_dev, :], x_ref[...], TN) + dot(adj_ref[rows_dev:, :], halo_in[...].reshape(nodes * halo_pair, width), TN)
    agg_ref[...] = agg.astype(BF16)
    keep_kv(me)
    kv_to_cross[0].wait_recv()
    kv_relay[0].start()
    pre_ref[...] = dot(agg_ref[...], w_msg_ref[...]) + dot(x_ref[...], w_self_ref[...])
    for k in range(1, KV_PIECES):
        kv_to_cross[k].wait_recv()
        kv_relay[k].start()
    for copy in kv_to_mate:
        copy.wait_recv()
    keep_kv(mate)
    keep_kv(cross)
    for copy in kv_relay:
        copy.wait_recv()
    keep_kv(other)
    for copy in saves:
        copy.start()
    attention_forward(head_dim, rows_dev, count_ref, q_ref, kv_ref, kvt_ref, out_ref, lse_ref, w_unit, s_even, s_odd, stat)
    for copy in saves:
        copy.wait()
    for copy in meta_copies + pos_to_cross + pos_to_mate + pos_relay + [halo_copy(peer, me) for peer in peers] + kv_to_cross + kv_to_mate + kv_relay:
        copy.wait_send()


def front(perm, valid, halo_slot, x_feat, pos_enc, edge_src, edge_dst, edge_mask, w_q, w_k_t, w_v_t, w_msg, w_self):
    rows, width = x_feat.shape
    nodes, halo_pair = halo_slot.shape
    head_dim = w_k_t.shape[0]
    pair = 2 * head_dim
    heads = width // head_dim
    keys = nodes * rows
    table_rows = rows + nodes * halo_pair
    vmem = pl.BlockSpec(memory_space=pltpu.VMEM)
    anywhere = pl.BlockSpec(memory_space=pl.ANY)
    dma = pltpu.SemaphoreType.DMA
    small = [((width, rows), BF16), ((heads, rows), F32), ((1, nodes * halo_pair), jnp.int32), ((nodes, rows - nodes * nodes * halo_pair), jnp.int32)]
    saved = [((width, rows), BF16), ((keys, pair), BF16), ((pair, keys), BF16), ((rows, width), BF16), ((rows, width), BF16), ((rows, width), F32), ((table_rows, rows), BF16)]
    inputs = (x_feat, pos_enc, edge_src, edge_dst, edge_mask, w_q, w_k_t, w_v_t, w_msg, w_self)
    return pl.pallas_call(
        functools.partial(front_kernel, head_dim),
        out_shape=[jax.ShapeDtypeStruct(shape, dtype) for shape, dtype in small + saved],
        in_specs=[vmem] * 3 + [anywhere] * len(inputs),
        out_specs=[vmem] * len(small) + [anywhere] * len(saved),
        scratch_shapes=[pltpu.VMEM(shape, dtype) for shape, dtype in saved] + [pltpu.VMEM(a.shape, a.dtype) for a in inputs] + [
            pltpu.VMEM((pair, Q_BLOCK), BF16),
            pltpu.VMEM((keys, Q_BLOCK), F32),
            pltpu.VMEM((keys, Q_BLOCK), F32),
            pltpu.VMEM((8, Q_BLOCK), F32),
            pltpu.VMEM((2, rows), jnp.int32),
            pltpu.VMEM((nodes, 2, rows), jnp.int32),
            pltpu.VMEM((nodes, rows, width), BF16),
            pltpu.VMEM((rows, width), F32),
            pltpu.VMEM((table_rows, rows), F32),
            pltpu.VMEM((table_rows, rows // 2), F32),
            pltpu.VMEM((nodes, halo_pair, width), BF16),
            pltpu.VMEM((nodes, halo_pair, width), BF16),
            pltpu.VMEM((nodes, rows, pair), BF16),
            dma((len(inputs),)), dma((len(saved),)), dma((3,)), dma((nodes,)), dma((3, POS_PIECES)), dma((3, POS_PIECES)), dma((nodes,)), dma((nodes,)), dma((3, KV_PIECES)), dma((3, KV_PIECES)),
        ],
        compiler_params=pltpu.CompilerParams(vmem_limit_bytes=60 << 20, collective_id=2, has_side_effects=True),
        cost_estimate=pl.CostEstimate(flops=24 << 30, bytes_accessed=20 << 20, transcendentals=heads * rows * keys),
        name='front',
    )(perm, valid, halo_slot, *inputs)


def mask_tail(scores, chunk, key_chunk, part_rows, count_ref):
    start = chunk * key_chunk
    part = start // part_rows
    first = start - part * part_rows + key_chunk - TAIL
    row_ix = first + lax.broadcasted_iota(jnp.int32, (TAIL, scores.shape[1]), 0)
    tail = jnp.where(row_ix < count_ref[pl.ds(part, 1), :scores.shape[1]], scores[key_chunk - TAIL:, :], NEG_FILL)
    return jnp.concatenate([scores[:key_chunk - TAIL, :], tail], axis=0)


Q_BLOCK, KEY_CHUNK, UNROLL = 256, 1024, 2


def attention_forward(head_dim, part_rows, count_ref, q_ref, kv_ref, kvt_ref, out_ref, lse_ref, w_q, s_even, s_odd, stat):
    heads = q_ref.shape[0] // head_dim
    blocks = q_ref.shape[1] // Q_BLOCK
    units = heads * blocks
    chunks = kv_ref.shape[0] // KEY_CHUNK
    factor = head_dim ** -0.5 * LOG2E
    groups = KEY_CHUNK // 8

    def load_weights(unit):
        head, block = unit // blocks, lax.rem(unit, blocks)
        w_q[:head_dim, :] = q_ref[pl.ds(pl.multiple_of(head * head_dim, head_dim), head_dim), pl.ds(pl.multiple_of(block * Q_BLOCK, Q_BLOCK), Q_BLOCK)]

    def score_stage(buffer, chunk, run_max):
        rows = pl.ds(pl.multiple_of(chunk * KEY_CHUNK, KEY_CHUNK), KEY_CHUNK)
        scores = mask_tail(dot(kv_ref[rows, :], w_q[...]), chunk, KEY_CHUNK, part_rows, count_ref)
        buffer[rows, :] = scores
        return jnp.maximum(run_max, jnp.max(scores.reshape(groups, 8, Q_BLOCK), axis=0))

    w_q[head_dim:, :] = jnp.zeros((w_q.shape[0] - head_dim, Q_BLOCK), BF16)
    floor = jnp.full((8, Q_BLOCK), -jnp.inf, F32)
    load_weights(0)
    stat[...] = lax.fori_loop(0, chunks, lambda chunk, run_max: score_stage(s_even, chunk, run_max), floor)

    def one_unit(unit, held, free):
        load_weights(jnp.minimum(unit + 1, units - 1))
        top = jnp.max(stat[...], axis=0, keepdims=True) * factor

        def chunk_body(index, state):
            run_max, run_sum, weighted = state
            for k in range(UNROLL):
                chunk = index * UNROLL + k
                run_max = score_stage(free, chunk, run_max)
                cols = pl.ds(pl.multiple_of(chunk * KEY_CHUNK, KEY_CHUNK), KEY_CHUNK)
                prob = jnp.exp2(held[cols, :] * factor - top)
                run_sum = run_sum + jnp.sum(prob.reshape(groups, 8, Q_BLOCK), axis=0)
                weighted = weighted + dot(kvt_ref[head_dim:2 * head_dim, cols], prob.astype(BF16))
            return run_max, run_sum, weighted

        run_max, run_sum, weighted = lax.fori_loop(0, chunks // UNROLL, chunk_body, (floor, jnp.zeros((8, Q_BLOCK), F32), jnp.zeros((head_dim, Q_BLOCK), F32)))
        stat[...] = run_max
        total = jnp.sum(run_sum, axis=0, keepdims=True)
        head, block = unit // blocks, lax.rem(unit, blocks)
        cols = pl.ds(pl.multiple_of(block * Q_BLOCK, Q_BLOCK), Q_BLOCK)
        out_ref[pl.ds(pl.multiple_of(head * head_dim, head_dim), head_dim), cols] = (weighted / total).astype(BF16)
        lse_ref[pl.ds(head, 1), cols] = top + jnp.log2(total)

    def unit_pair(pair, carry):
        one_unit(2 * pair, s_even, s_odd)
        one_unit(2 * pair + 1, s_odd, s_even)
        return carry

    lax.fori_loop(0, units // 2, unit_pair, 0)


FINAL_STEPS, FINAL_LAG = 14, 1
HOLD_STEP = 68
ROW_BLOCK = 256
GELU_A, GELU_B = math.sqrt(2.0 / math.pi), 0.044715


def backward_kernel(head_dim, q_block, key_chunk, part_rows, count_ref, lse_ref, slot_ref, o_hbm, x_hbm, w_o_hbm, pre_hbm, cot_hbm, up_hbm, down_hbm, *rest):
    later, rest = rest[:11], rest[11:]
    row_outs, rest = rest[:2], rest[2:]
    sum_refs, kv_sum_ref, rest = rest[:6], rest[6], rest[7:]
    held, rest = rest[:11], rest[11:]
    (y_ref, dx_ref, o_ref, x_ref, w_o_ref), rest = rest[:5], rest[5:]
    row_copies = [pltpu.make_async_copy(src, dst, rest[-1].at[i]) for i, (src, dst) in enumerate(zip((y_ref, dx_ref), row_outs))]
    rest = rest[:-1]
    q_ref, kv_ref, kvt_ref, hid_ref, agg_ref, adj_ref, w_msg_ref, w_self_ref, w_q_ref, w_kt_ref, w_vt_ref = held
    do_buf, dz_buf, dpre_buf, dx_acc, dkv_in, dkv_sum, local, from_mate, from_cross, kv_local, kv_own, kv_in, halo_out, halo_in, load_sem, held_sem, keep_sem, send_sem, recv_sem, dkv_send, dkv_recv, kv_sem, kv_send, kv_recv, halo_send, halo_recv = rest
    heads = q_ref.shape[0] // head_dim
    blocks = q_ref.shape[1] // q_block
    units = heads * blocks
    chunks = kv_ref.shape[0] // key_chunk
    steps = units * chunks
    per_group = steps // 4
    halves = part_rows // key_chunk
    scale = head_dim ** -0.5
    factor = scale * LOG2E
    total, width = local.shape[0], local.shape[1]
    half_rows = width // 2
    ffn_chunks = up_hbm.shape[1] // width
    first_small = 2 * ffn_chunks
    me, chip, side, mate, cross, other = neighbours()

    def block(index, half):
        if index >= first_small:
            return sum_refs[2 + index - first_small].at[pl.ds(half * half_rows, half_rows), :]
        chunk = index // 2
        if index % 2 == 0:
            return sum_refs[1].at[pl.ds(chunk * width + half * half_rows, half_rows), :]
        return sum_refs[0].at[pl.ds(half * half_rows, half_rows), pl.ds(chunk * width, width)]

    def part(index, half):
        return local.at[index, pl.ds(half * half_rows, half_rows), :]

    def to_peer(src, dst, kind, index, peer):
        return remote(src, dst, send_sem.at[kind, index], recv_sem.at[kind, index], peer)

    def mate_copy(index):
        return to_peer(part(index, 1 - side), from_mate.at[index], 0, index, mate)

    def cross_copy(index):
        return to_peer(part(index, side), from_cross.at[index], 1, index, cross)

    def back_copy(index, half):
        return to_peer(from_mate.at[index], block(index, half), 2, index, mate)

    def keep_copy(index):
        return pltpu.make_async_copy(from_mate.at[index], block(index, side), keep_sem.at[index])

    my_half = pl.ds(pl.multiple_of(side * half_rows, half_rows), half_rows)

    def chip_sum(index):
        mate_copy(index).wait_recv()
        local[index, my_half, :] = local[index, my_half, :] + from_mate[index]

    def group_sum(index):
        cross_copy(index).wait_recv()
        from_mate[index] = local[index, my_half, :] + from_cross[index]

    def start_out(index):
        keep_copy(index).start()
        back_copy(index, side).start()

    kv_half = kv_local.shape[0] // 2

    def kv_rows(half):
        return pl.ds(half * kv_half, kv_half)

    kv_to_mate = remote(kv_local.at[kv_rows(1 - side), :], kv_in.at[0], kv_send.at[0], kv_recv.at[0], mate)
    kv_to_cross = remote(kv_own.at[0], kv_in.at[1], kv_send.at[1], kv_recv.at[1], cross)
    kv_keep = pltpu.make_async_copy(kv_own.at[1], kv_sum_ref.at[kv_rows(side), :], kv_sem)

    def kv_back(half):
        return remote(kv_own.at[1], kv_sum_ref.at[kv_rows(half), :], kv_send.at[2], kv_recv.at[2], mate)

    halo_pair = halo_out.shape[1]

    def halo_copy(peer, owner):
        return remote(halo_out.at[peer], halo_in.at[owner], halo_send.at[peer], halo_recv.at[owner], peer)

    held_loads = [pltpu.make_async_copy(src, dst, held_sem.at[i]) for i, (src, dst) in enumerate(zip(later, held))]

    def ffn_phase(w_up, w_down, g_buf, z_buf, y_acc, act, d_act):
        loads = [pltpu.make_async_copy(src, dst, load_sem.at[i]) for i, (src, dst) in enumerate(((o_hbm, o_ref), (w_o_hbm, w_o_ref), (x_hbm, x_ref), (pre_hbm, dx_acc), (cot_hbm, g_buf), (up_hbm, w_up), (down_hbm, w_down)))]
        for copy in loads:
            copy.start()
        meet((mate, cross, other))
        loads[0].wait()
        loads[1].wait()
        y_acc[...] = dot(o_ref[...], w_o_ref[...], TN)
        loads[2].wait()
        loads[3].wait()
        pre = dx_acc[...]
        x_wide = x_ref[...].astype(F32)
        z_mid = (x_wide + jnp.maximum(pre, 0.0) + x_wide + y_acc[...].astype(BF16).astype(F32)).astype(BF16)
        dpre_buf[...] = jnp.where(pre > 0, 1.0, 0.0).astype(BF16)
        z_buf[...] = z_mid
        loads[4].wait()
        keep = lax.broadcasted_iota(jnp.int32, (part_rows, width), 0) < count_ref[pl.ds(me, 1), :width]
        g_wide = jnp.where(keep, g_buf[...].astype(F32), 0.0)
        g_buf[...] = g_wide.astype(BF16)
        dx_acc[...] = g_wide
        y_acc[...] = z_mid.astype(F32)
        loads[5].wait()
        loads[6].wait()

        def ffn_chunk(chunk, carry):
            cols = pl.ds(pl.multiple_of(chunk * width, width), width)

            def act_block(index, inner):
                rows = pl.ds(pl.multiple_of(index * ROW_BLOCK, ROW_BLOCK), ROW_BLOCK)
                h_pre = dot(z_buf[rows, :], w_up[:, cols])
                bend = jnp.tanh(h_pre * (GELU_A + GELU_A * GELU_B * (h_pre * h_pre)))
                act[rows, :] = (h_pre * (0.5 + 0.5 * bend)).astype(BF16)
                return inner

            def row_block(index, inner):
                rows = pl.ds(pl.multiple_of(index * ROW_BLOCK, ROW_BLOCK), ROW_BLOCK)
                h_pre = dot(z_buf[rows, :], w_up[:, cols])
                square = h_pre * h_pre
                bend = jnp.tanh(h_pre * (GELU_A + GELU_A * GELU_B * square))
                slope = 0.5 + 0.5 * bend + (0.5 * h_pre) * (1.0 - bend * bend) * (GELU_A + 3.0 * GELU_A * GELU_B * square)
                d_hidden = dot(g_buf[rows, :], w_down[cols, :], NT).astype(BF16)
                d_act[rows, :] = (d_hidden.astype(F32) * slope).astype(BF16)
                y_acc[rows, :] += dot(act[rows, :], w_down[cols, :])
                dx_acc[rows, :] += dot(d_act[rows, :], w_up[:, cols], NT)
                return inner

            lax.fori_loop(0, part_rows // ROW_BLOCK, act_block, 0)
            local[2 * chunk] = dot(act[...], g_buf[...], TN)

            @pl.when(chunk == 0)
            def load_later():
                for copy in held_loads:
                    copy.start()

            @pl.when(chunk > 0)
            def sum_previous():
                chip_sum(2 * chunk - 1)

            row_block(0, 0)
            mate_copy(2 * chunk).start()

            @pl.when(chunk > 0)
            def send_previous():
                cross_copy(2 * chunk - 1).start()

            row_block(1, 0)
            chip_sum(2 * chunk)
            row_block(2, 0)
            cross_copy(2 * chunk).start()
            lax.fori_loop(3, part_rows // ROW_BLOCK, row_block, 0)
            local[2 * chunk + 1] = dot(z_buf[...], d_act[...], TN)
            mate_copy(2 * chunk + 1).start()
            return carry

        lax.fori_loop(0, ffn_chunks, ffn_chunk, 0)
        y_ref[...] = jnp.where(keep, y_acc[...], 0.0).astype(BF16)

    pl.run_scoped(ffn_phase, pltpu.VMEM(up_hbm.shape, BF16), pltpu.VMEM(down_hbm.shape, BF16), pltpu.VMEM(x_ref.shape, BF16), pltpu.VMEM(x_ref.shape, BF16), pltpu.VMEM(x_ref.shape, F32), pltpu.VMEM(x_ref.shape, BF16), pltpu.VMEM(x_ref.shape, BF16))
    row_copies[0].start()
    for copy in held_loads:
        copy.wait()
    d_z = dx_acc[...].astype(BF16)
    dz_buf[...] = d_z
    dpre_buf[...] = jnp.where(dpre_buf[...] > 0, d_z, jnp.zeros_like(d_z))
    chip_sum(first_small - 1)
    do_buf[...] = dot(w_o_ref[...], dz_buf[...], NT).astype(BF16)
    cross_copy(first_small - 1).start()

    local[first_small] = dot(x_ref[...], dpre_buf[...], TN)
    local[first_small + 1] = dot(agg_ref[...], dpre_buf[...], TN)
    local[first_small + 2] = dot(o_ref[...], dz_buf[...])

    def attention_phase(w_q_even, w_q_odd, w_do_even, w_do_odd, p_even, p_odd, ds_even, ds_odd, lse_buf, delta_buf, dq_acc, dq_all, dkv_acc):
        buffers = ((w_q_even, w_do_even, p_even, ds_even), (w_q_odd, w_do_odd, p_odd, ds_odd))
        dkv_copies = [remote(src, dkv_in.at[i], dkv_send.at[i], dkv_recv.at[i], peer) for i, (src, peer) in enumerate(((dkv_acc.at[0], mate), (dkv_sum, cross), (dkv_acc.at[2], mate)))]

        def unit_spots(unit):
            head, place = unit // blocks, lax.rem(unit, blocks)
            return head, pl.ds(pl.multiple_of(head * head_dim, head_dim), head_dim), pl.ds(pl.multiple_of(place * q_block, q_block), q_block)

        def prepare(unit, carry):
            head, rows, cols = unit_spots(unit)
            delta_buf[unit] = jnp.sum(do_buf[rows, cols].astype(F32) * o_ref[rows, cols].astype(F32), axis=0, keepdims=True)
            lse_buf[unit] = lse_ref[pl.ds(head, 1), cols]
            dq_acc[unit] = jnp.zeros((head_dim, q_block), F32)
            return carry

        lax.fori_loop(0, units, prepare, 0)
        for w_q, w_do, p_buf, ds_buf in buffers:
            w_q[head_dim:, :] = jnp.zeros((head_dim, q_block), BF16)
            w_do[:head_dim, :] = jnp.zeros((head_dim, q_block), BF16)
        dkv_acc[...] = jnp.zeros_like(dkv_acc)

        def place_of(step):
            group = step // per_group
            chunk = step // units
            owner = lax.rem(chip + 1 - group // 2, 2) * 2 + lax.rem(side + 1 - lax.rem(group, 2), 2)
            offset = lax.rem(chunk, halves) * key_chunk
            rows = pl.ds(pl.multiple_of(owner * part_rows + offset, key_chunk), key_chunk)
            return group, owner, offset, rows, lax.rem(step, units)

        def first_stage(step, parity):
            w_q, w_do, p_buf, ds_buf = buffers[parity]
            group, owner, offset, rows, unit = place_of(step)
            head, unit_rows, cols = unit_spots(unit)
            w_q[:head_dim, :] = q_ref[unit_rows, cols]
            w_do[head_dim:, :] = do_buf[unit_rows, cols]
            kv = kv_ref[rows, :]
            scores = dot(kv, w_q[...])
            row_ix = offset + key_chunk - TAIL + lax.broadcasted_iota(jnp.int32, (TAIL, q_block), 0)
            tail = jnp.where(row_ix < count_ref[pl.ds(owner, 1), :q_block], scores[key_chunk - TAIL:, :], NEG_FILL)
            scores = jnp.concatenate([scores[:key_chunk - TAIL, :], tail], axis=0)
            prob = jnp.exp2(scores * factor - lse_buf[unit])
            p_buf[...] = prob.astype(BF16)
            ds_buf[...] = (prob * (dot(kv, w_do[...]) - delta_buf[unit])).astype(BF16)

        def second_stage(step, parity):
            w_q, w_do, p_buf, ds_buf = buffers[parity]
            group, owner, offset, rows, unit = place_of(step)
            d_scores = ds_buf[...]
            spot = pl.ds(pl.multiple_of(offset, key_chunk), key_chunk)
            dkv_acc[group, spot, :] += dot(d_scores, w_q[...], NT) + dot(p_buf[...], w_do[...], NT)
            dq_acc[unit] += dot(kvt_ref[:head_dim, rows], d_scores)

        def exchange(step):
            held = jnp.logical_and(step >= HOLD_STEP, step < HOLD_STEP + 12)
            turn = (step - HOLD_STEP) // 4 + first_small
            phase = lax.rem(step, 4)

            @pl.when(jnp.logical_and(held, phase == 1))
            def sum_chip():
                chip_sum(turn)

            @pl.when(jnp.logical_and(held, phase == 2))
            def send_cross():
                cross_copy(turn).start()

            lap, beat = step // FINAL_STEPS - FINAL_LAG, lax.rem(step, FINAL_STEPS)

            @pl.when(jnp.logical_and(lap >= 0, beat == 0))
            def sum_group():
                group_sum(lap)

            @pl.when(jnp.logical_and(lap >= 0, beat == 1))
            def send_back():
                for k in range(done):
                    @pl.when(lap == k)
                    def start_piece(k=k):
                        start_out(k)

            @pl.when(step == 3)
            def small_pieces():
                for index in range(first_small, total - 1):
                    mate_copy(index).start()

            @pl.when(step == per_group + 1)
            def first_group():
                dkv_copies[0].start()

            @pl.when(step == 2 * per_group + 1)
            def second_group():
                dkv_copies[0].wait_recv()
                dkv_sum[...] = dkv_acc[1] + dkv_in[0]

            @pl.when(step == 2 * per_group + 2)
            def send_second():
                dkv_copies[1].start()

            @pl.when(step == 3 * per_group + 1)
            def third_group():
                dkv_copies[2].start()

        done = (steps - 1) // FINAL_STEPS - FINAL_LAG + 1
        assert (steps - 1) % FINAL_STEPS >= 1 and 0 < done < total - 2 and HOLD_STEP > 2 * per_group + 2 and HOLD_STEP % 4 == 0

        first_stage(0, 0)

        def body(pair, carry):
            for parity in (1, 0):
                step = 2 * pair + 2 - parity
                exchange(step)
                second_stage(step - 1, 1 - parity)
                first_stage(step, parity)
            return carry

        assert steps % 2 == 0
        lax.fori_loop(0, steps // 2 - 1, body, 0)
        exchange(steps - 1)
        first_stage(steps - 1, 1)
        second_stage(steps - 2, 0)
        second_stage(steps - 1, 1)

        def gather_dq(unit, carry):
            head, rows, cols = unit_spots(unit)
            dq_all[rows, cols] = (dq_acc[unit] * scale).astype(BF16)
            return carry

        lax.fori_loop(0, units, gather_dq, 0)
        last = total - 1
        local[last] = dot(dq_all[...], hid_ref[...]).T
        mate_copy(last).start()
        dkv_copies[2].wait_recv()
        dkv_copies[1].wait_recv()
        dkv = dkv_acc[3] + dkv_in[2] + dkv_in[1]
        lane = lax.broadcasted_iota(jnp.int32, dkv.shape, 1)
        dkv = jnp.where(lane < head_dim, dkv * scale, dkv).astype(BF16)
        kv_local[...] = dot(dkv, hid_ref[...], TN)
        d_agg = dot(dpre_buf[...], w_msg_ref[...], NT).astype(BF16)
        halo_out[...] = dot(adj_ref[part_rows:, :], d_agg).astype(BF16).reshape(halo_out.shape)
        kv_to_mate.start()
        chip_sum(last)
        dx_acc[...] = 2.0 * dz_buf[...].astype(F32) + dot(dpre_buf[...], w_self_ref[...], NT)
        for peer in (mate, cross, other):
            halo_copy(peer, me).start()
        halo_in[me] = halo_out[me]
        cross_copy(last).start()
        kv_to_mate.wait_recv()
        kv_own[0] = kv_local[pl.ds(pl.multiple_of(side * kv_half, kv_half), kv_half), :] + kv_in[0]
        dx_acc[...] += dot(adj_ref[:part_rows, :], d_agg)
        kv_to_cross.start()
        dx_acc[...] += dot(dkv, jnp.concatenate([w_kt_ref[...], w_vt_ref[...]], axis=0))
        for peer in (mate, cross, other):
            halo_copy(me, peer).wait_recv()
        slot_hot = jnp.where(lax.broadcasted_iota(jnp.int32, (part_rows, 4 * halo_pair), 0) == slot_ref[...], 1.0, 0.0).astype(BF16)
        dx_acc[...] += dot(slot_hot, halo_in[...].reshape(4 * halo_pair, width))
        dx_ref[...] = (dx_acc[...] + dot(dq_all[...], w_q_ref[...].T, TN)).astype(BF16)
        for index in range(done, total):
            group_sum(index)
            if index == done:
                row_copies[1].start()
            else:
                start_out(index - 1)
        kv_to_cross.wait_recv()
        kv_own[1] = kv_own[0] + kv_in[1]
        start_out(last)
        kv_keep.start()
        kv_back(side).start()
        for copy in dkv_copies:
            copy.wait_send()

    pl.run_scoped(
        attention_phase,
        *[pltpu.VMEM((2 * head_dim, q_block), BF16)] * 4,
        *[pltpu.VMEM((key_chunk, q_block), BF16)] * 4,
        pltpu.VMEM((units, 1, q_block), F32),
        pltpu.VMEM((units, 1, q_block), F32),
        pltpu.VMEM((units, head_dim, q_block), F32),
        pltpu.VMEM((width, part_rows), BF16),
        pltpu.VMEM((4, part_rows, 2 * head_dim), F32),
    )
    for copy in [kv_to_mate, kv_to_cross, kv_back(side)] + [halo_copy(peer, me) for peer in (mate, cross, other)]:
        copy.wait_send()
    for copy in row_copies:
        copy.wait()
    kv_keep.wait()
    kv_back(1 - side).wait_recv()
    for index in range(total):
        mate_copy(index).wait_send()
        cross_copy(index).wait_send()
        keep_copy(index).wait()
        back_copy(index, side).wait_send()
        back_copy(index, 1 - side).wait_recv()


def backward(counts, o_t, lse, slots, x_feat, w_o, pre_act, y_cot, w_up, w_down, q_t, kv, kv_t, hidden_in, agg_msg, adjacency_t, w_msg, w_self, w_q, w_k_t, w_v_t):
    width, rows = q_t.shape
    keys = kv.shape[0]
    head_dim = kv.shape[1] // 2
    heads = width // head_dim
    nodes = keys // rows
    q_block, key_chunk = 512, 512
    half = width // 2
    shapes = [w_up.shape, w_down.shape] + [(width, width)] * 4
    total = sum(r * c // (width * width) for r, c in shapes)
    halo_pair = slots.shape[1] // nodes
    later = (q_t, kv, kv_t, hidden_in, agg_msg, adjacency_t, w_msg, w_self, w_q, w_k_t, w_v_t)
    vmem = pl.BlockSpec(memory_space=pltpu.VMEM)
    anywhere = pl.BlockSpec(memory_space=pl.ANY)
    dma = pltpu.SemaphoreType.DMA
    return pl.pallas_call(
        functools.partial(backward_kernel, head_dim, q_block, key_chunk, rows),
        out_shape=[jax.ShapeDtypeStruct((rows, width), BF16)] * 2 + [jax.ShapeDtypeStruct(shape, F32) for shape in shapes] + [jax.ShapeDtypeStruct((2 * head_dim, width), F32)],
        in_specs=[vmem] * 3 + [anywhere] * 18,
        out_specs=[anywhere] * 9,
        scratch_shapes=[pltpu.VMEM(a.shape, a.dtype) for a in later] + [
            pltpu.VMEM((rows, width), BF16),
            pltpu.VMEM((rows, width), BF16),
            pltpu.VMEM((width, rows), BF16),
            pltpu.VMEM((rows, width), BF16),
            pltpu.VMEM((width, width), BF16),
            pltpu.VMEM((width, rows), BF16),
            pltpu.VMEM((rows, width), BF16),
            pltpu.VMEM((rows, width), BF16),
            pltpu.VMEM((rows, width), F32),
            pltpu.VMEM((3, rows, 2 * head_dim), F32),
            pltpu.VMEM((rows, 2 * head_dim), F32),
            pltpu.VMEM((total, width, width), F32),
            pltpu.VMEM((total, half, width), F32),
            pltpu.VMEM((total, half, width), F32),
            pltpu.VMEM((2 * head_dim, width), F32),
            pltpu.VMEM((2, head_dim, width), F32),
            pltpu.VMEM((2, head_dim, width), F32),
            pltpu.VMEM((nodes, halo_pair, width), BF16),
            pltpu.VMEM((nodes, halo_pair, width), BF16),
            dma((7,)), dma((len(later),)), dma((total,)), dma((3, total)), dma((3, total)), dma((3,)), dma((3,)), dma, dma((3,)), dma((3,)), dma((nodes,)), dma((nodes,)), dma((2,)),
        ],
        compiler_params=pltpu.CompilerParams(vmem_limit_bytes=67043328, collective_id=1, has_side_effects=True),
        cost_estimate=pl.CostEstimate(flops=10 * heads * rows * keys * head_dim, bytes_accessed=40 << 20, transcendentals=heads * rows * keys),
        name='backward',
    )(counts, lse, slots, o_t, x_feat, w_o, pre_act, y_cot, w_up, w_down, *later)


def finish_kernel(plan, *refs):
    inputs = plan[-1][0] + 1
    sources, rest = refs[:inputs], refs[inputs:]
    outputs = plan[-1][1] + 1
    targets, rest = rest[:outputs], rest[outputs:]
    buffers, in_sem, out_sem = rest[:-2], rest[-2], rest[-1]
    gets = [pltpu.make_async_copy(sources[i].at[pl.ds(src, n), :], buf, in_sem.at[k]) for k, ((i, j, src, dst, n), buf) in enumerate(zip(plan, buffers))]
    puts = [pltpu.make_async_copy(buf, targets[j].at[pl.ds(dst, n), :], out_sem.at[k]) for k, ((i, j, src, dst, n), buf) in enumerate(zip(plan, buffers))]
    for copy in gets:
        copy.start()
    for get, put in zip(gets, puts):
        get.wait()
        put.start()
    for copy in puts:
        copy.wait()


def finish(*arrays):
    plan, shapes = [], []
    for i, a in enumerate(arrays):
        last = i == len(arrays) - 1
        step = a.shape[0] // 2 if last else min(a.shape[0], (1 << 20) // (a.shape[1] * a.dtype.itemsize))
        for start in range(0, a.shape[0], step):
            j = i + (start // step if last else 0)
            plan.append((i, j, start, 0 if last else start, step))
        shapes += [jax.ShapeDtypeStruct((step, a.shape[1]), a.dtype)] * 2 if last else [jax.ShapeDtypeStruct(a.shape, a.dtype)]
    anywhere = pl.BlockSpec(memory_space=pl.ANY)
    return pl.pallas_call(
        functools.partial(finish_kernel, plan),
        out_shape=shapes,
        in_specs=[anywhere] * len(arrays),
        out_specs=[anywhere] * len(shapes),
        scratch_shapes=[pltpu.VMEM((n, arrays[i].shape[1]), arrays[i].dtype) for i, j, src, dst, n in plan] + [pltpu.SemaphoreType.DMA((len(plan),))] * 2,
        compiler_params=pltpu.CompilerParams(vmem_limit_bytes=67043328),
        cost_estimate=pl.CostEstimate(flops=1 << 20, bytes_accessed=30 << 20, transcendentals=0),
        name='finish',
    )(*arrays)


def solution(mesh):
    nodes = mesh.shape['nodes']
    row_spec = P(('graphs', 'nodes'), None)
    flat_spec = P(('graphs', 'nodes'))
    halo_spec = P(('graphs', 'nodes'), None, None)
    grad_spec = P('graphs', None)

    def device_step(x_feat, valid, halo_slot, edge_src, edge_dst, edge_mask, bal_perm, pos_enc, y_cot, w_msg, w_self, w_q, w_k, w_v, w_o, w_up, w_down):
        head_dim = w_k.shape[1]
        mixed_t, lse, slots, counts, q_t, kv, kv_t, hidden_in, agg_msg, pre_act, adjacency_t = front(bal_perm[None, :], valid[None, :], halo_slot.reshape(nodes, -1), x_feat, pos_enc, edge_src, edge_dst, edge_mask, w_q, w_k.T, w_v.T, w_msg, w_self)
        results = backward(counts, mixed_t, lse, slots, x_feat, w_o, pre_act, y_cot, w_up, w_down, q_t, kv, kv_t, hidden_in, agg_msg, adjacency_t, w_msg, w_self, w_q, w_k.T, w_v.T)
        y_out, dx_feat, grad_up, grad_down, grad_self, grad_msg, grad_o, grad_q, grad_k, grad_v = finish(*results)
        return (y_out, dx_feat, grad_msg, grad_self, grad_q, grad_k.T, grad_v.T, grad_o, grad_up, grad_down)

    return jax.shard_map(device_step, mesh=mesh, in_specs=(row_spec, flat_spec, halo_spec, row_spec, row_spec, row_spec, flat_spec, row_spec, row_spec) + (P(),) * 8, out_specs=(row_spec, row_spec) + (grad_spec,) * 8, check_vma=False)
```

```python
import functools
import math

import jax
import jax.numpy as jnp
from jax import lax
from jax.experimental import pallas as pl
from jax.experimental.pallas import tpu as pltpu
from jax.sharding import PartitionSpec as P

NEG_FILL = -1e30
LOG2E = math.log2(math.e)
TAIL = 32
F32 = jnp.float32
BF16 = jnp.bfloat16
NN = (((1,), (0,)), ((), ()))
NT = (((1,), (1,)), ((), ()))
TN = (((0,), (0,)), ((), ()))
TT = (((0,), (1,)), ((), ()))


def dot(a, b, dims=NN):
    return lax.dot_general(a, b, dims, preferred_element_type=F32)


def remote(src, dst, send, recv, peer):
    return pltpu.make_async_remote_copy(src_ref=src, dst_ref=dst, send_sem=send, recv_sem=recv, device_id={'nodes': peer}, device_id_type=pl.DeviceIdType.MESH)


def neighbours():
    me = lax.axis_index('nodes')
    chip, side = me // 2, lax.rem(me, 2)
    return me, chip, side, chip * 2 + 1 - side, (1 - chip) * 2 + side, (1 - chip) * 2 + 1 - side


def meet(peers):
    barrier = pltpu.get_barrier_semaphore()
    for peer in peers:
        pl.semaphore_signal(barrier, inc=1, device_id={'nodes': peer}, device_id_type=pl.DeviceIdType.MESH)
    pl.semaphore_wait(barrier, len(peers))


CHUNKS, EDGE_STEP, POS_PIECES, KV_PIECES = 4, 512, 4, 2


def front_kernel(head_dim, perm_ref, valid_ref, halo_ref, x_hbm, pos_hbm, src_hbm, dst_hbm, on_hbm, w_q_hbm, w_kt_hbm, w_vt_hbm, w_msg_hbm, w_self_hbm, *rest):
    (out_ref, lse_ref, slot_ref, count_ref), rest = rest[:4], rest[4:]
    saved, rest = rest[:7], rest[7:]
    kept, rest = rest[:7], rest[7:]
    q_ref, kv_ref, kvt_ref, hid_ref, agg_ref, pre_ref, adj_ref = kept
    loaded, rest = rest[:10], rest[10:]
    x_ref, pos_ref, src_ref, dst_ref, on_ref, w_q_ref, w_kt_ref, w_vt_ref, w_msg_ref, w_self_ref = loaded
    w_unit, s_even, s_odd, stat, meta_ref, meta_all, pos_all, pos_acc, counts_acc, edge_acc, halo_out, halo_in, kv_all, load_sem, save_sem, meta_send, meta_recv, pos_send, pos_recv, halo_send, halo_recv, kv_send, kv_recv = rest
    rows_dev, width = x_ref.shape
    table_rows = adj_ref.shape[0]
    half = rows_dev // 2
    nodes = meta_all.shape[0]
    halo_pair = halo_in.shape[1]
    me, chip, side, mate, cross, other = neighbours()
    peers = (mate, cross, other)
    loads = [pltpu.make_async_copy(src, dst, load_sem.at[i]) for i, (src, dst) in enumerate(zip((x_hbm, pos_hbm, src_hbm, dst_hbm, on_hbm, w_q_hbm, w_kt_hbm, w_vt_hbm, w_msg_hbm, w_self_hbm), loaded))]
    saves = [pltpu.make_async_copy(src, dst, save_sem.at[i]) for i, (src, dst) in enumerate(zip(kept, saved))]
    for copy in loads:
        copy.start()
    lanes = nodes * halo_pair
    assert (nodes + 1) * lanes <= rows_dev
    meta_ref[0:1, :] = perm_ref[...]
    mine = lax.broadcasted_iota(jnp.int32, (1, lanes), 1) // halo_pair == me
    for owner in range(nodes):
        meta_ref[1:2, owner * lanes:(owner + 1) * lanes] = jnp.where(mine, jnp.concatenate([halo_ref[owner:owner + 1, :]] * nodes, axis=1), -1)
    held = jnp.sum(valid_ref[...].astype(F32), axis=1, keepdims=True).astype(jnp.int32)
    meta_ref[1:2, nodes * lanes:] = jnp.broadcast_to(held, (1, rows_dev - nodes * lanes))
    meet(peers)

    meta_copies = [remote(meta_ref, meta_all.at[me], meta_send.at[i], meta_recv.at[me], peer) for i, peer in enumerate(peers)]
    piece = rows_dev // POS_PIECES

    def pos_rows(index):
        return pl.ds(index * piece, piece)

    pos_to_cross = [remote(pos_ref.at[pos_rows(k), :], pos_all.at[me, pos_rows(k), :], pos_send.at[0, k], pos_recv.at[0, k], cross) for k in range(POS_PIECES)]
    pos_to_mate = [remote(pos_ref.at[pos_rows(k), :], pos_all.at[me, pos_rows(k), :], pos_send.at[1, k], pos_recv.at[1, k], mate) for k in range(POS_PIECES)]
    pos_relay = [remote(pos_all.at[cross, pos_rows(k), :], pos_all.at[cross, pos_rows(k), :], pos_send.at[2, k], pos_recv.at[2, k], mate) for k in range(POS_PIECES)]
    for copy in meta_copies:
        copy.start()
    loads[1].wait()
    for copy in pos_to_cross + pos_to_mate:
        copy.start()
    meta_all[me] = meta_ref[...]
    for copy in loads[:1] + loads[2:]:
        copy.wait()

    def relay_pos(k):
        pos_to_cross[k].wait_recv()
        pos_relay[k].start()

    def place_pos(owner, source, first):
        perm = meta_all[owner, 0:1, :] - me * rows_dev
        size = 256

        def body(index, carry):
            rows = pl.ds(pl.multiple_of(index * size, size), size)
            hot = jnp.where(index * size + lax.broadcasted_iota(jnp.int32, (size, rows_dev), 0) == perm, 1.0, 0.0).astype(BF16)
            part = dot(hot, source[...])
            pos_acc[rows, :] = part if first else pos_acc[rows, :] + part
            return carry

        lax.fori_loop(0, rows_dev // size, body, 0)

    edges = src_ref.shape[1]
    steps = edges // (CHUNKS * EDGE_STEP)
    assert CHUNKS * EDGE_STEP * steps == edges and EDGE_STEP * steps < 4096

    def edge_block(index):
        cols = pl.ds(pl.multiple_of(index * EDGE_STEP, EDGE_STEP), EDGE_STEP)
        src, dst, on = src_ref[:, cols], dst_ref[:, cols], on_ref[:, cols]
        upper = dst >= half
        place = jnp.where(upper, dst - half, dst)
        weight = jnp.where(on > 0, jnp.where(upper, 4096.0, 1.0), 0.0)
        src_hot = jnp.where(lax.broadcasted_iota(jnp.int32, (table_rows, EDGE_STEP), 0) == src, 1.0, 0.0).astype(BF16)
        dst_hot = jnp.where(lax.broadcasted_iota(jnp.int32, (half, EDGE_STEP), 0) == place, weight, 0.0).astype(BF16)
        return dot(src_hot, dst_hot, NT)

    def count_chunk(chunk):
        edge_acc[...] = jnp.zeros_like(edge_acc)

        def body(step, carry):
            edge_acc[...] += edge_block(chunk * steps + step)
            return carry

        lax.fori_loop(0, steps, body, 0)
        total = edge_acc[...]
        high = jnp.floor(total * (1.0 / 4096.0))
        low = total - high * 4096.0
        if chunk == 0:
            counts_acc[:, :half] = low
            counts_acc[:, half:] = high
        elif chunk < CHUNKS - 1:
            counts_acc[:, :half] += low
            counts_acc[:, half:] += high
        else:
            adj_ref[:, :half] = (counts_acc[:, :half] + low).astype(BF16)
            adj_ref[:, half:] = (counts_acc[:, half:] + high).astype(BF16)

    def halo_copy(peer, owner):
        return remote(halo_out.at[peer], halo_in.at[owner], halo_send.at[peer], halo_recv.at[owner], peer)

    count_chunk(0)
    for peer in peers:
        remote(meta_ref, meta_all.at[peer], meta_send.at[0], meta_recv.at[peer], peer).wait_recv()
    slots = jnp.full((1, lanes), -1, jnp.int32)
    for node in range(nodes):
        for owner in range(nodes):
            slots = jnp.maximum(slots, jnp.where(me == owner, meta_all[node, 1:2, owner * lanes:(owner + 1) * lanes], -1))
    slot_ref[...] = slots
    slot_hot = jnp.where(lax.broadcasted_iota(jnp.int32, (rows_dev, nodes * halo_pair), 0) == slots, 1.0, 0.0).astype(BF16)
    halo_out[...] = dot(slot_hot, x_ref[...], TN).astype(BF16).reshape(halo_out.shape)
    relay_pos(0)
    place_pos(me, pos_ref, True)
    for peer in peers:
        halo_copy(peer, me).start()
    halo_in[me] = halo_out[me]
    for node in range(nodes):
        count_ref[node:node + 1, :] = meta_all[node, 1:2, nodes * lanes:]
    count_chunk(1)
    relay_pos(1)
    for copy in pos_to_mate:
        copy.wait_recv()
    place_pos(mate, pos_all.at[mate], False)
    count_chunk(2)
    relay_pos(2)
    count_chunk(3)
    relay_pos(3)
    place_pos(cross, pos_all.at[cross], False)
    for copy in pos_relay:
        copy.wait_recv()
    place_pos(other, pos_all.at[other], False)

    hid_ref[...] = (x_ref[...].astype(F32) + pos_acc[...]).astype(BF16)
    kv_all[me] = dot(hid_ref[...], jnp.concatenate([w_kt_ref[...], w_vt_ref[...]], axis=0), NT).astype(BF16)
    kv_piece = rows_dev // KV_PIECES

    def kv_copy(owner, k, kind, peer):
        rows = pl.ds(k * kv_piece, kv_piece)
        return remote(kv_all.at[owner, rows, :], kv_all.at[owner, rows, :], kv_send.at[kind, k], kv_recv.at[kind, k], peer)

    kv_to_cross = [kv_copy(me, k, 0, cross) for k in range(KV_PIECES)]
    kv_to_mate = [kv_copy(me, k, 1, mate) for k in range(KV_PIECES)]
    kv_relay = [kv_copy(cross, k, 2, mate) for k in range(KV_PIECES)]
    size = kv_all.shape[2]
    eye = jnp.where(lax.broadcasted_iota(jnp.int32, (size, size), 0) == lax.broadcasted_iota(jnp.int32, (size, size), 1), 1.0, 0.0).astype(BF16)

    def keep_kv(owner):
        rows = pl.ds(pl.multiple_of(owner * rows_dev, rows_dev), rows_dev)
        kv_ref[rows, :] = kv_all[owner]
        kvt_ref[:, rows] = dot(eye, kv_all[owner], NT).astype(BF16)

    keep_kv(me)
    for copy in kv_to_cross + kv_to_mate:
        copy.start()
    q_ref[...] = dot(w_q_ref[...].T, hid_ref[...], NT).astype(BF16)
    for peer in peers:
        halo_copy(me, peer).wait_recv()
    agg = dot(adj_ref[:rows_dev, :], x_ref[...], TN) + dot(adj_ref[rows_dev:, :], halo_in[...].reshape(nodes * halo_pair, width), TN)
    agg_ref[...] = agg.astype(BF16)
    kv_to_cross[0].wait_recv()
    kv_relay[0].start()
    pre_ref[...] = dot(agg_ref[...], w_msg_ref[...]) + dot(x_ref[...], w_self_ref[...])
    for k in range(1, KV_PIECES):
        kv_to_cross[k].wait_recv()
        kv_relay[k].start()
    for copy in kv_to_mate:
        copy.wait_recv()
    keep_kv(mate)
    keep_kv(cross)
    for copy in kv_relay:
        copy.wait_recv()
    keep_kv(other)
    for copy in saves:
        copy.start()
    attention_forward(head_dim, rows_dev, count_ref, q_ref, kv_ref, kvt_ref, out_ref, lse_ref, w_unit, s_even, s_odd, stat)
    for copy in saves:
        copy.wait()
    for copy in meta_copies + pos_to_cross + pos_to_mate + pos_relay + [halo_copy(peer, me) for peer in peers] + kv_to_cross + kv_to_mate + kv_relay:
        copy.wait_send()


def front(perm, valid, halo_slot, x_feat, pos_enc, edge_src, edge_dst, edge_mask, w_q, w_k_t, w_v_t, w_msg, w_self):
    rows, width = x_feat.shape
    nodes, halo_pair = halo_slot.shape
    head_dim = w_k_t.shape[0]
    pair = 2 * head_dim
    heads = width // head_dim
    keys = nodes * rows
    table_rows = rows + nodes * halo_pair
    vmem = pl.BlockSpec(memory_space=pltpu.VMEM)
    anywhere = pl.BlockSpec(memory_space=pl.ANY)
    dma = pltpu.SemaphoreType.DMA
    small = [((width, rows), BF16), ((heads, rows), F32), ((1, nodes * halo_pair), jnp.int32), ((nodes, rows - nodes * nodes * halo_pair), jnp.int32)]
    saved = [((width, rows), BF16), ((keys, pair), BF16), ((pair, keys), BF16), ((rows, width), BF16), ((rows, width), BF16), ((rows, width), F32), ((table_rows, rows), BF16)]
    inputs = (x_feat, pos_enc, edge_src, edge_dst, edge_mask, w_q, w_k_t, w_v_t, w_msg, w_self)
    return pl.pallas_call(
        functools.partial(front_kernel, head_dim),
        out_shape=[jax.ShapeDtypeStruct(shape, dtype) for shape, dtype in small + saved],
        in_specs=[vmem] * 3 + [anywhere] * len(inputs),
        out_specs=[vmem] * len(small) + [anywhere] * len(saved),
        scratch_shapes=[pltpu.VMEM(shape, dtype) for shape, dtype in saved] + [pltpu.VMEM(a.shape, a.dtype) for a in inputs] + [
            pltpu.VMEM((pair, Q_BLOCK), BF16),
            pltpu.VMEM((keys, Q_BLOCK), F32),
            pltpu.VMEM((keys, Q_BLOCK), F32),
            pltpu.VMEM((8, Q_BLOCK), F32),
            pltpu.VMEM((2, rows), jnp.int32),
            pltpu.VMEM((nodes, 2, rows), jnp.int32),
            pltpu.VMEM((nodes, rows, width), BF16),
            pltpu.VMEM((rows, width), F32),
            pltpu.VMEM((table_rows, rows), F32),
            pltpu.VMEM((table_rows, rows // 2), F32),
            pltpu.VMEM((nodes, halo_pair, width), BF16),
            pltpu.VMEM((nodes, halo_pair, width), BF16),
            pltpu.VMEM((nodes, rows, pair), BF16),
            dma((len(inputs),)), dma((len(saved),)), dma((3,)), dma((nodes,)), dma((3, POS_PIECES)), dma((3, POS_PIECES)), dma((nodes,)), dma((nodes,)), dma((3, KV_PIECES)), dma((3, KV_PIECES)),
        ],
        compiler_params=pltpu.CompilerParams(vmem_limit_bytes=60 << 20, collective_id=2, has_side_effects=True),
        cost_estimate=pl.CostEstimate(flops=24 << 30, bytes_accessed=20 << 20, transcendentals=heads * rows * keys),
        name='front',
    )(perm, valid, halo_slot, *inputs)


def mask_tail(scores, chunk, key_chunk, part_rows, count_ref):
    start = chunk * key_chunk
    part = start // part_rows
    first = start - part * part_rows + key_chunk - TAIL
    row_ix = first + lax.broadcasted_iota(jnp.int32, (TAIL, scores.shape[1]), 0)
    tail = jnp.where(row_ix < count_ref[pl.ds(part, 1), :scores.shape[1]], scores[key_chunk - TAIL:, :], NEG_FILL)
    return jnp.concatenate([scores[:key_chunk - TAIL, :], tail], axis=0)


Q_BLOCK, KEY_CHUNK, UNROLL = 256, 1024, 2


def attention_forward(head_dim, part_rows, count_ref, q_ref, kv_ref, kvt_ref, out_ref, lse_ref, w_q, s_even, s_odd, stat):
    heads = q_ref.shape[0] // head_dim
    blocks = q_ref.shape[1] // Q_BLOCK
    units = heads * blocks
    chunks = kv_ref.shape[0] // KEY_CHUNK
    factor = head_dim ** -0.5 * LOG2E
    groups = KEY_CHUNK // 8

    def load_weights(unit):
        head, block = unit // blocks, lax.rem(unit, blocks)
        w_q[:head_dim, :] = q_ref[pl.ds(pl.multiple_of(head * head_dim, head_dim), head_dim), pl.ds(pl.multiple_of(block * Q_BLOCK, Q_BLOCK), Q_BLOCK)]

    def score_stage(buffer, chunk, run_max):
        rows = pl.ds(pl.multiple_of(chunk * KEY_CHUNK, KEY_CHUNK), KEY_CHUNK)
        scores = mask_tail(dot(kv_ref[rows, :], w_q[...]), chunk, KEY_CHUNK, part_rows, count_ref)
        buffer[rows, :] = scores
        return jnp.maximum(run_max, jnp.max(scores.reshape(groups, 8, Q_BLOCK), axis=0))

    w_q[head_dim:, :] = jnp.zeros((w_q.shape[0] - head_dim, Q_BLOCK), BF16)
    floor = jnp.full((8, Q_BLOCK), -jnp.inf, F32)
    load_weights(0)
    stat[...] = lax.fori_loop(0, chunks, lambda chunk, run_max: score_stage(s_even, chunk, run_max), floor)

    def one_unit(unit, held, free):
        load_weights(jnp.minimum(unit + 1, units - 1))
        top = jnp.max(stat[...], axis=0, keepdims=True) * factor

        def chunk_body(index, state):
            run_max, run_sum, weighted = state
            for k in range(UNROLL):
                chunk = index * UNROLL + k
                run_max = score_stage(free, chunk, run_max)
                cols = pl.ds(pl.multiple_of(chunk * KEY_CHUNK, KEY_CHUNK), KEY_CHUNK)
                prob = jnp.exp2(held[cols, :] * factor - top)
                run_sum = run_sum + jnp.sum(prob.reshape(groups, 8, Q_BLOCK), axis=0)
                weighted = weighted + dot(kvt_ref[head_dim:2 * head_dim, cols], prob.astype(BF16))
            return run_max, run_sum, weighted

        run_max, run_sum, weighted = lax.fori_loop(0, chunks // UNROLL, chunk_body, (floor, jnp.zeros((8, Q_BLOCK), F32), jnp.zeros((head_dim, Q_BLOCK), F32)))
        stat[...] = run_max
        total = jnp.sum(run_sum, axis=0, keepdims=True)
        head, block = unit // blocks, lax.rem(unit, blocks)
        cols = pl.ds(pl.multiple_of(block * Q_BLOCK, Q_BLOCK), Q_BLOCK)
        out_ref[pl.ds(pl.multiple_of(head * head_dim, head_dim), head_dim), cols] = (weighted / total).astype(BF16)
        lse_ref[pl.ds(head, 1), cols] = top + jnp.log2(total)

    def unit_pair(pair, carry):
        one_unit(2 * pair, s_even, s_odd)
        one_unit(2 * pair + 1, s_odd, s_even)
        return carry

    lax.fori_loop(0, units // 2, unit_pair, 0)


FINAL_STEPS, FINAL_LAG = 14, 1
HOLD_STEP = 68
ROW_BLOCK = 256
GELU_A, GELU_B = math.sqrt(2.0 / math.pi), 0.044715


def backward_kernel(head_dim, q_block, key_chunk, part_rows, count_ref, lse_ref, slot_ref, o_hbm, x_hbm, w_o_hbm, pre_hbm, cot_hbm, up_hbm, down_hbm, *rest):
    later, rest = rest[:11], rest[11:]
    row_outs, rest = rest[:2], rest[2:]
    sum_refs, kv_sum_ref, rest = rest[:6], rest[6], rest[7:]
    held, rest = rest[:11], rest[11:]
    (y_ref, dx_ref, o_ref, x_ref, w_o_ref), rest = rest[:5], rest[5:]
    row_copies = [pltpu.make_async_copy(src, dst, rest[-1].at[i]) for i, (src, dst) in enumerate(zip((y_ref, dx_ref), row_outs))]
    rest = rest[:-1]
    q_ref, kv_ref, kvt_ref, hid_ref, agg_ref, adj_ref, w_msg_ref, w_self_ref, w_q_ref, w_kt_ref, w_vt_ref = held
    do_buf, dz_buf, dpre_buf, dx_acc, dkv_in, dkv_sum, local, from_mate, from_cross, kv_local, kv_own, kv_in, halo_out, halo_in, load_sem, held_sem, keep_sem, send_sem, recv_sem, dkv_send, dkv_recv, kv_sem, kv_send, kv_recv, halo_send, halo_recv = rest
    heads = q_ref.shape[0] // head_dim
    blocks = q_ref.shape[1] // q_block
    units = heads * blocks
    chunks = kv_ref.shape[0] // key_chunk
    steps = units * chunks
    per_group = steps // 4
    halves = part_rows // key_chunk
    scale = head_dim ** -0.5
    factor = scale * LOG2E
    total, width = local.shape[0], local.shape[1]
    half_rows = width // 2
    ffn_chunks = up_hbm.shape[1] // width
    first_small = 2 * ffn_chunks
    me, chip, side, mate, cross, other = neighbours()

    def block(index, half):
        if index >= first_small:
            return sum_refs[2 + index - first_small].at[pl.ds(half * half_rows, half_rows), :]
        chunk = index // 2
        if index % 2 == 0:
            return sum_refs[1].at[pl.ds(chunk * width + half * half_rows, half_rows), :]
        return sum_refs[0].at[pl.ds(half * half_rows, half_rows), pl.ds(chunk * width, width)]

    def part(index, half):
        return local.at[index, pl.ds(half * half_rows, half_rows), :]

    def to_peer(src, dst, kind, index, peer):
        return remote(src, dst, send_sem.at[kind, index], recv_sem.at[kind, index], peer)

    def mate_copy(index):
        return to_peer(part(index, 1 - side), from_mate.at[index], 0, index, mate)

    def cross_copy(index):
        return to_peer(part(index, side), from_cross.at[index], 1, index, cross)

    def back_copy(index, half):
        return to_peer(from_mate.at[index], block(index, half), 2, index, mate)

    def keep_copy(index):
        return pltpu.make_async_copy(from_mate.at[index], block(index, side), keep_sem.at[index])

    my_half = pl.ds(pl.multiple_of(side * half_rows, half_rows), half_rows)

    def chip_sum(index):
        mate_copy(index).wait_recv()
        local[index, my_half, :] = local[index, my_half, :] + from_mate[index]

    def group_sum(index):
        cross_copy(index).wait_recv()
        from_mate[index] = local[index, my_half, :] + from_cross[index]

    def start_out(index):
        keep_copy(index).start()
        back_copy(index, side).start()

    kv_half = kv_local.shape[0] // 2

    def kv_rows(half):
        return pl.ds(half * kv_half, kv_half)

    kv_to_mate = remote(kv_local.at[kv_rows(1 - side), :], kv_in.at[0], kv_send.at[0], kv_recv.at[0], mate)
    kv_to_cross = remote(kv_own.at[0], kv_in.at[1], kv_send.at[1], kv_recv.at[1], cross)
    kv_keep = pltpu.make_async_copy(kv_own.at[1], kv_sum_ref.at[kv_rows(side), :], kv_sem)

    def kv_back(half):
        return remote(kv_own.at[1], kv_sum_ref.at[kv_rows(half), :], kv_send.at[2], kv_recv.at[2], mate)

    halo_pair = halo_out.shape[1]

    def halo_copy(peer, owner):
        return remote(halo_out.at[peer], halo_in.at[owner], halo_send.at[peer], halo_recv.at[owner], peer)

    held_loads = [pltpu.make_async_copy(src, dst, held_sem.at[i]) for i, (src, dst) in enumerate(zip(later, held))]

    def ffn_phase(w_up, w_down, g_buf, z_buf, y_acc, act, d_act):
        loads = [pltpu.make_async_copy(src, dst, load_sem.at[i]) for i, (src, dst) in enumerate(((o_hbm, o_ref), (w_o_hbm, w_o_ref), (x_hbm, x_ref), (pre_hbm, dx_acc), (cot_hbm, g_buf), (up_hbm, w_up), (down_hbm, w_down)))]
        for copy in loads:
            copy.start()
        meet((mate, cross, other))
        loads[0].wait()
        loads[1].wait()
        y_acc[...] = dot(o_ref[...], w_o_ref[...], TN)
        loads[2].wait()
        loads[3].wait()
        pre = dx_acc[...]
        x_wide = x_ref[...].astype(F32)
        z_mid = (x_wide + jnp.maximum(pre, 0.0) + x_wide + y_acc[...].astype(BF16).astype(F32)).astype(BF16)
        dpre_buf[...] = jnp.where(pre > 0, 1.0, 0.0).astype(BF16)
        z_buf[...] = z_mid
        loads[4].wait()
        keep = lax.broadcasted_iota(jnp.int32, (part_rows, width), 0) < count_ref[pl.ds(me, 1), :width]
        g_wide = jnp.where(keep, g_buf[...].astype(F32), 0.0)
        g_buf[...] = g_wide.astype(BF16)
        dx_acc[...] = g_wide
        y_acc[...] = z_mid.astype(F32)
        loads[5].wait()
        loads[6].wait()

        def ffn_chunk(chunk, carry):
            cols = pl.ds(pl.multiple_of(chunk * width, width), width)

            def act_block(index, inner):
                rows = pl.ds(pl.multiple_of(index * ROW_BLOCK, ROW_BLOCK), ROW_BLOCK)
                h_pre = dot(z_buf[rows, :], w_up[:, cols])
                bend = jnp.tanh(h_pre * (GELU_A + GELU_A * GELU_B * (h_pre * h_pre)))
                act[rows, :] = (h_pre * (0.5 + 0.5 * bend)).astype(BF16)
                return inner

            def row_block(index, inner):
                rows = pl.ds(pl.multiple_of(index * ROW_BLOCK, ROW_BLOCK), ROW_BLOCK)
                h_pre = dot(z_buf[rows, :], w_up[:, cols])
                square = h_pre * h_pre
                bend = jnp.tanh(h_pre * (GELU_A + GELU_A * GELU_B * square))
                slope = 0.5 + 0.5 * bend + (0.5 * h_pre) * (1.0 - bend * bend) * (GELU_A + 3.0 * GELU_A * GELU_B * square)
                d_hidden = dot(g_buf[rows, :], w_down[cols, :], NT).astype(BF16)
                d_act[rows, :] = (d_hidden.astype(F32) * slope).astype(BF16)
                y_acc[rows, :] += dot(act[rows, :], w_down[cols, :])
                dx_acc[rows, :] += dot(d_act[rows, :], w_up[:, cols], NT)
                return inner

            lax.fori_loop(0, part_rows // ROW_BLOCK, act_block, 0)
            local[2 * chunk] = dot(act[...], g_buf[...], TN)

            @pl.when(chunk == 0)
            def load_later():
                for copy in held_loads:
                    copy.start()

            @pl.when(chunk > 0)
            def sum_previous():
                chip_sum(2 * chunk - 1)

            row_block(0, 0)
            mate_copy(2 * chunk).start()

            @pl.when(chunk > 0)
            def send_previous():
                cross_copy(2 * chunk - 1).start()

            row_block(1, 0)
            chip_sum(2 * chunk)
            row_block(2, 0)
            cross_copy(2 * chunk).start()
            lax.fori_loop(3, part_rows // ROW_BLOCK, row_block, 0)
            local[2 * chunk + 1] = dot(z_buf[...], d_act[...], TN)
            mate_copy(2 * chunk + 1).start()
            return carry

        lax.fori_loop(0, ffn_chunks, ffn_chunk, 0)
        y_ref[...] = jnp.where(keep, y_acc[...], 0.0).astype(BF16)

    pl.run_scoped(ffn_phase, pltpu.VMEM(up_hbm.shape, BF16), pltpu.VMEM(down_hbm.shape, BF16), pltpu.VMEM(x_ref.shape, BF16), pltpu.VMEM(x_ref.shape, BF16), pltpu.VMEM(x_ref.shape, F32), pltpu.VMEM(x_ref.shape, BF16), pltpu.VMEM(x_ref.shape, BF16))
    row_copies[0].start()
    for copy in held_loads:
        copy.wait()
    d_z = dx_acc[...].astype(BF16)
    dz_buf[...] = d_z
    dpre_buf[...] = jnp.where(dpre_buf[...] > 0, d_z, jnp.zeros_like(d_z))
    chip_sum(first_small - 1)
    do_buf[...] = dot(w_o_ref[...], dz_buf[...], NT).astype(BF16)
    cross_copy(first_small - 1).start()

    local[first_small] = dot(x_ref[...], dpre_buf[...], TN)
    local[first_small + 1] = dot(agg_ref[...], dpre_buf[...], TN)
    local[first_small + 2] = dot(o_ref[...], dz_buf[...])

    def attention_phase(w_q_even, w_q_odd, w_do_even, w_do_odd, p_even, p_odd, ds_even, ds_odd, lse_buf, delta_buf, dq_acc, dq_all, dkv_acc):
        buffers = ((w_q_even, w_do_even, p_even, ds_even), (w_q_odd, w_do_odd, p_odd, ds_odd))
        dkv_copies = [remote(src, dkv_in.at[i], dkv_send.at[i], dkv_recv.at[i], peer) for i, (src, peer) in enumerate(((dkv_acc.at[0], mate), (dkv_sum, cross), (dkv_acc.at[2], mate)))]

        def unit_spots(unit):
            head, place = unit // blocks, lax.rem(unit, blocks)
            return head, pl.ds(pl.multiple_of(head * head_dim, head_dim), head_dim), pl.ds(pl.multiple_of(place * q_block, q_block), q_block)

        def prepare(unit, carry):
            head, rows, cols = unit_spots(unit)
            delta_buf[unit] = jnp.sum(do_buf[rows, cols].astype(F32) * o_ref[rows, cols].astype(F32), axis=0, keepdims=True)
            lse_buf[unit] = lse_ref[pl.ds(head, 1), cols]
            dq_acc[unit] = jnp.zeros((head_dim, q_block), F32)
            return carry

        lax.fori_loop(0, units, prepare, 0)
        for w_q, w_do, p_buf, ds_buf in buffers:
            w_q[head_dim:, :] = jnp.zeros((head_dim, q_block), BF16)
            w_do[:head_dim, :] = jnp.zeros((head_dim, q_block), BF16)
        dkv_acc[...] = jnp.zeros_like(dkv_acc)

        def place_of(step):
            group = step // per_group
            chunk = step // units
            owner = lax.rem(chip + 1 - group // 2, 2) * 2 + lax.rem(side + 1 - lax.rem(group, 2), 2)
            offset = lax.rem(chunk, halves) * key_chunk
            rows = pl.ds(pl.multiple_of(owner * part_rows + offset, key_chunk), key_chunk)
            return group, owner, offset, rows, lax.rem(step, units)

        def first_stage(step, parity):
            w_q, w_do, p_buf, ds_buf = buffers[parity]
            group, owner, offset, rows, unit = place_of(step)
            head, unit_rows, cols = unit_spots(unit)
            w_q[:head_dim, :] = q_ref[unit_rows, cols]
            w_do[head_dim:, :] = do_buf[unit_rows, cols]
            kv = kv_ref[rows, :]
            scores = dot(kv, w_q[...])
            row_ix = offset + key_chunk - TAIL + lax.broadcasted_iota(jnp.int32, (TAIL, q_block), 0)
            tail = jnp.where(row_ix < count_ref[pl.ds(owner, 1), :q_block], scores[key_chunk - TAIL:, :], NEG_FILL)
            scores = jnp.concatenate([scores[:key_chunk - TAIL, :], tail], axis=0)
            prob = jnp.exp2(scores * factor - lse_buf[unit])
            p_buf[...] = prob.astype(BF16)
            ds_buf[...] = (prob * (dot(kv, w_do[...]) - delta_buf[unit])).astype(BF16)

        def second_stage(step, parity):
            w_q, w_do, p_buf, ds_buf = buffers[parity]
            group, owner, offset, rows, unit = place_of(step)
            d_scores = ds_buf[...]
            spot = pl.ds(pl.multiple_of(offset, key_chunk), key_chunk)
            dkv_acc[group, spot, :] += dot(d_scores, w_q[...], NT) + dot(p_buf[...], w_do[...], NT)
            dq_acc[unit] += dot(kvt_ref[:head_dim, rows], d_scores)

        def exchange(step):
            held = jnp.logical_and(step >= HOLD_STEP, step < HOLD_STEP + 12)
            turn = (step - HOLD_STEP) // 4 + first_small
            phase = lax.rem(step, 4)

            @pl.when(jnp.logical_and(held, phase == 1))
            def sum_chip():
                chip_sum(turn)

            @pl.when(jnp.logical_and(held, phase == 2))
            def send_cross():
                cross_copy(turn).start()

            lap, beat = step // FINAL_STEPS - FINAL_LAG, lax.rem(step, FINAL_STEPS)

            @pl.when(jnp.logical_and(lap >= 0, beat == 0))
            def sum_group():
                group_sum(lap)

            @pl.when(jnp.logical_and(lap >= 0, beat == 1))
            def send_back():
                for k in range(done):
                    @pl.when(lap == k)
                    def start_piece(k=k):
                        start_out(k)

            @pl.when(step == 3)
            def small_pieces():
                for index in range(first_small, total - 1):
                    mate_copy(index).start()

            @pl.when(step == per_group + 1)
            def first_group():
                dkv_copies[0].start()

            @pl.when(step == 2 * per_group + 1)
            def second_group():
                dkv_copies[0].wait_recv()
                dkv_sum[...] = dkv_acc[1] + dkv_in[0]

            @pl.when(step == 2 * per_group + 2)
            def send_second():
                dkv_copies[1].start()

            @pl.when(step == 3 * per_group + 1)
            def third_group():
                dkv_copies[2].start()

        done = (steps - 1) // FINAL_STEPS - FINAL_LAG + 1
        assert (steps - 1) % FINAL_STEPS >= 1 and 0 < done < total - 2 and HOLD_STEP > 2 * per_group + 2 and HOLD_STEP % 4 == 0

        first_stage(0, 0)

        def body(pair, carry):
            for parity in (1, 0):
                step = 2 * pair + 2 - parity
                exchange(step)
                second_stage(step - 1, 1 - parity)
                first_stage(step, parity)
            return carry

        assert steps % 2 == 0
        lax.fori_loop(0, steps // 2 - 1, body, 0)
        exchange(steps - 1)
        first_stage(steps - 1, 1)
        second_stage(steps - 2, 0)
        second_stage(steps - 1, 1)

        def gather_dq(unit, carry):
            head, rows, cols = unit_spots(unit)
            dq_all[rows, cols] = (dq_acc[unit] * scale).astype(BF16)
            return carry

        lax.fori_loop(0, units, gather_dq, 0)
        last = total - 1
        local[last] = dot(dq_all[...], hid_ref[...]).T
        mate_copy(last).start()
        dkv_copies[2].wait_recv()
        dkv_copies[1].wait_recv()
        dkv = dkv_acc[3] + dkv_in[2] + dkv_in[1]
        lane = lax.broadcasted_iota(jnp.int32, dkv.shape, 1)
        dkv = jnp.where(lane < head_dim, dkv * scale, dkv).astype(BF16)
        kv_local[...] = dot(dkv, hid_ref[...], TN)
        d_agg = dot(dpre_buf[...], w_msg_ref[...], NT).astype(BF16)
        halo_out[...] = dot(adj_ref[part_rows:, :], d_agg).astype(BF16).reshape(halo_out.shape)
        kv_to_mate.start()
        chip_sum(last)
        dx_acc[...] = 2.0 * dz_buf[...].astype(F32) + dot(dpre_buf[...], w_self_ref[...], NT)
        for peer in (mate, cross, other):
            halo_copy(peer, me).start()
        halo_in[me] = halo_out[me]
        cross_copy(last).start()
        kv_to_mate.wait_recv()
        kv_own[0] = kv_local[pl.ds(pl.multiple_of(side * kv_half, kv_half), kv_half), :] + kv_in[0]
        dx_acc[...] += dot(adj_ref[:part_rows, :], d_agg)
        kv_to_cross.start()
        dx_acc[...] += dot(dkv, jnp.concatenate([w_kt_ref[...], w_vt_ref[...]], axis=0))
        for peer in (mate, cross, other):
            halo_copy(me, peer).wait_recv()
        slot_hot = jnp.where(lax.broadcasted_iota(jnp.int32, (part_rows, 4 * halo_pair), 0) == slot_ref[...], 1.0, 0.0).astype(BF16)
        dx_acc[...] += dot(slot_hot, halo_in[...].reshape(4 * halo_pair, width))
        dx_ref[...] = (dx_acc[...] + dot(dq_all[...], w_q_ref[...].T, TN)).astype(BF16)
        for index in range(done, total):
            group_sum(index)
            if index == done:
                row_copies[1].start()
            else:
                start_out(index - 1)
        kv_to_cross.wait_recv()
        kv_own[1] = kv_own[0] + kv_in[1]
        start_out(last)
        kv_keep.start()
        kv_back(side).start()
        for copy in dkv_copies:
            copy.wait_send()

    pl.run_scoped(
        attention_phase,
        *[pltpu.VMEM((2 * head_dim, q_block), BF16)] * 4,
        *[pltpu.VMEM((key_chunk, q_block), BF16)] * 4,
        pltpu.VMEM((units, 1, q_block), F32),
        pltpu.VMEM((units, 1, q_block), F32),
        pltpu.VMEM((units, head_dim, q_block), F32),
        pltpu.VMEM((width, part_rows), BF16),
        pltpu.VMEM((4, part_rows, 2 * head_dim), F32),
    )
    for copy in [kv_to_mate, kv_to_cross, kv_back(side)] + [halo_copy(peer, me) for peer in (mate, cross, other)]:
        copy.wait_send()
    for copy in row_copies:
        copy.wait()
    kv_keep.wait()
    kv_back(1 - side).wait_recv()
    for index in range(total):
        mate_copy(index).wait_send()
        cross_copy(index).wait_send()
        keep_copy(index).wait()
        back_copy(index, side).wait_send()
        back_copy(index, 1 - side).wait_recv()


def backward(counts, o_t, lse, slots, x_feat, w_o, pre_act, y_cot, w_up, w_down, q_t, kv, kv_t, hidden_in, agg_msg, adjacency_t, w_msg, w_self, w_q, w_k_t, w_v_t):
    width, rows = q_t.shape
    keys = kv.shape[0]
    head_dim = kv.shape[1] // 2
    heads = width // head_dim
    nodes = keys // rows
    q_block, key_chunk = 512, 512
    half = width // 2
    shapes = [w_up.shape, w_down.shape] + [(width, width)] * 4
    total = sum(r * c // (width * width) for r, c in shapes)
    halo_pair = slots.shape[1] // nodes
    later = (q_t, kv, kv_t, hidden_in, agg_msg, adjacency_t, w_msg, w_self, w_q, w_k_t, w_v_t)
    vmem = pl.BlockSpec(memory_space=pltpu.VMEM)
    anywhere = pl.BlockSpec(memory_space=pl.ANY)
    dma = pltpu.SemaphoreType.DMA
    return pl.pallas_call(
        functools.partial(backward_kernel, head_dim, q_block, key_chunk, rows),
        out_shape=[jax.ShapeDtypeStruct((rows, width), BF16)] * 2 + [jax.ShapeDtypeStruct(shape, F32) for shape in shapes] + [jax.ShapeDtypeStruct((2 * head_dim, width), F32)],
        in_specs=[vmem] * 3 + [anywhere] * 18,
        out_specs=[anywhere] * 9,
        scratch_shapes=[pltpu.VMEM(a.shape, a.dtype) for a in later] + [
            pltpu.VMEM((rows, width), BF16),
            pltpu.VMEM((rows, width), BF16),
            pltpu.VMEM((width, rows), BF16),
            pltpu.VMEM((rows, width), BF16),
            pltpu.VMEM((width, width), BF16),
            pltpu.VMEM((width, rows), BF16),
            pltpu.VMEM((rows, width), BF16),
            pltpu.VMEM((rows, width), BF16),
            pltpu.VMEM((rows, width), F32),
            pltpu.VMEM((3, rows, 2 * head_dim), F32),
            pltpu.VMEM((rows, 2 * head_dim), F32),
            pltpu.VMEM((total, width, width), F32),
            pltpu.VMEM((total, half, width), F32),
            pltpu.VMEM((total, half, width), F32),
            pltpu.VMEM((2 * head_dim, width), F32),
            pltpu.VMEM((2, head_dim, width), F32),
            pltpu.VMEM((2, head_dim, width), F32),
            pltpu.VMEM((nodes, halo_pair, width), BF16),
            pltpu.VMEM((nodes, halo_pair, width), BF16),
            dma((7,)), dma((len(later),)), dma((total,)), dma((3, total)), dma((3, total)), dma((3,)), dma((3,)), dma, dma((3,)), dma((3,)), dma((nodes,)), dma((nodes,)), dma((2,)),
        ],
        compiler_params=pltpu.CompilerParams(vmem_limit_bytes=67043328, collective_id=1, has_side_effects=True),
        cost_estimate=pl.CostEstimate(flops=10 * heads * rows * keys * head_dim, bytes_accessed=40 << 20, transcendentals=heads * rows * keys),
        name='backward',
    )(counts, lse, slots, o_t, x_feat, w_o, pre_act, y_cot, w_up, w_down, *later)


def finish_kernel(plan, *refs):
    inputs = plan[-1][0] + 1
    sources, rest = refs[:inputs], refs[inputs:]
    outputs = plan[-1][1] + 1
    targets, rest = rest[:outputs], rest[outputs:]
    buffers, in_sem, out_sem = rest[:-2], rest[-2], rest[-1]
    gets = [pltpu.make_async_copy(sources[i].at[pl.ds(src, n), :], buf, in_sem.at[k]) for k, ((i, j, src, dst, n), buf) in enumerate(zip(plan, buffers))]
    puts = [pltpu.make_async_copy(buf, targets[j].at[pl.ds(dst, n), :], out_sem.at[k]) for k, ((i, j, src, dst, n), buf) in enumerate(zip(plan, buffers))]
    for copy in gets:
        copy.start()
    for get, put in zip(gets, puts):
        get.wait()
        put.start()
    for copy in puts:
        copy.wait()


def finish(*arrays):
    plan, shapes = [], []
    for i, a in enumerate(arrays):
        last = i == len(arrays) - 1
        step = a.shape[0] // 2 if last else min(a.shape[0], (1 << 20) // (a.shape[1] * a.dtype.itemsize))
        for start in range(0, a.shape[0], step):
            j = i + (start // step if last else 0)
            plan.append((i, j, start, 0 if last else start, step))
        shapes += [jax.ShapeDtypeStruct((step, a.shape[1]), a.dtype)] * 2 if last else [jax.ShapeDtypeStruct(a.shape, a.dtype)]
    anywhere = pl.BlockSpec(memory_space=pl.ANY)
    return pl.pallas_call(
        functools.partial(finish_kernel, plan),
        out_shape=shapes,
        in_specs=[anywhere] * len(arrays),
        out_specs=[anywhere] * len(shapes),
        scratch_shapes=[pltpu.VMEM((n, arrays[i].shape[1]), arrays[i].dtype) for i, j, src, dst, n in plan] + [pltpu.SemaphoreType.DMA((len(plan),))] * 2,
        compiler_params=pltpu.CompilerParams(vmem_limit_bytes=67043328),
        cost_estimate=pl.CostEstimate(flops=1 << 20, bytes_accessed=30 << 20, transcendentals=0),
        name='finish',
    )(*arrays)


def solution(mesh):
    nodes = mesh.shape['nodes']
    row_spec = P(('graphs', 'nodes'), None)
    flat_spec = P(('graphs', 'nodes'))
    halo_spec = P(('graphs', 'nodes'), None, None)
    grad_spec = P('graphs', None)

    def device_step(x_feat, valid, halo_slot, edge_src, edge_dst, edge_mask, bal_perm, pos_enc, y_cot, w_msg, w_self, w_q, w_k, w_v, w_o, w_up, w_down):
        head_dim = w_k.shape[1]
        mixed_t, lse, slots, counts, q_t, kv, kv_t, hidden_in, agg_msg, pre_act, adjacency_t = front(bal_perm[None, :], valid[None, :], halo_slot.reshape(nodes, -1), x_feat, pos_enc, edge_src, edge_dst, edge_mask, w_q, w_k.T, w_v.T, w_msg, w_self)
        results = backward(counts, mixed_t, lse, slots, x_feat, w_o, pre_act, y_cot, w_up, w_down, q_t, kv, kv_t, hidden_in, agg_msg, adjacency_t, w_msg, w_self, w_q, w_k.T, w_v.T)
        y_out, dx_feat, grad_up, grad_down, grad_self, grad_msg, grad_o, grad_q, grad_k, grad_v = finish(*results)
        return (y_out, dx_feat, grad_msg, grad_self, grad_q, grad_k.T, grad_v.T, grad_o, grad_up, grad_down)

    return jax.shard_map(device_step, mesh=mesh, in_specs=(row_spec, flat_spec, halo_spec, row_spec, row_spec, row_spec, flat_spec, row_spec, row_spec) + (P(),) * 8, out_specs=(row_spec, row_spec) + (grad_spec,) * 8, check_vma=False)
```
